256 devices in a mesh: groups: 2 (over z), dev: 128 (over x, y, core).
Axes of the slice: x: 8, y: 8, z: 2, core: 2. Of those that a mesh axis runs over, the one named last changes fastest.
The devices are a block of a 8x8x16 slice.
Arguments:
- tokens: bfloat16 [1024, 6144], P(('groups', 'dev')), parts along dimension 0, may hold values from -6 to 6
- queries: bfloat16 [1024, 6144], P(('groups', 'dev')), parts along dimension 0, may hold values from -250 to 250
- token_kv: bfloat16 [1024, 2048], P(('groups', 'dev')), parts along dimension 0, may hold values from -6 to 6
- kv_cache: bfloat16 [1024, 64, 2048], P(('groups', 'dev')), parts along dimension 0, may hold values from -6.5 to 6.5, as said below
- context_lengths: int32 [1024], P(('groups', 'dev')), parts along dimension 0, may hold values from 2 to 64
- fresh_kv: bfloat16 [16384, 2048], P(('groups', 'dev')), parts along dimension 0, may hold values from -6 to 6
- block_counts: int32 [256], P('groups'), parts along dimension 0, may hold values from 0 to 8, as said below
- expert_ids: int32 [1024, 2], P(('groups', 'dev')), parts along dimension 0, may hold values from 0 to 3, all different within a row; in each aligned block of 4 rows (0 to 3, 4 to 7, ...) at most 3 rows name the same one
- route_weights: float32 [1024, 2], P(('groups', 'dev')), parts along dimension 0, may hold values from 0.25 to 1
- norm_gain: float32 [6144], replicated, may hold values from 0.1 to 1.9
- w_gate: bfloat16 [6144, 32768], P(None, 'dev'), may hold values from -0.078125 to 0.078125
- w_up: bfloat16 [6144, 32768], P(None, 'dev'), may hold values from -0.078125 to 0.078125
- w_down: bfloat16 [32768, 6144], P('dev'), may hold values from -0.0625 to 0.0625
Outputs:
- layer_out: bfloat16 [1024, 6144], P(('groups', 'dev')), parts along dimension 0
The draws below stay inside these ranges and needn't reach their ends.
There are 2 independent parts, one for each index of `groups`. The reference program is written for one: setup_inputs(seed, part) draws one part's arguments, and reference() takes and returns one part's arrays. A program takes and returns all parts, laid end to end along the dimension named above; an argument that names none is the same for every part. Nothing has to cross between parts.
Inputs may be any that keep to these rules, and one draw needn't show every extreme that they name: `kv_cache`: each request's cached keys and values; the table of arrays gives their range. `block_counts`: the counts sum to 512; for every device d > 0 the exclusive prefix sum before it lies between d * 4 + 1 and (d + 1) * 4; the first device takes 2 * 4 blocks. `expert_ids`: among the rows of one device no expert is named more than 3 times, and in some devices one expert is named exactly 3 times.
All inputs are finite; a program needn't handle non-finite values.
Results may differ from the reference program's by a relative error of at most 0.008.
Values may be sent and summed in bfloat16 or wider, within the bound.
No kernel may reach another device: no remote copies, remote signals or barrier semaphores. Data moves between devices by JAX's collectives and lax.ppermute only.
A program may use at most 128 MiB of HBM per device.

```python
import math
import jax
import jax.numpy as jnp
import numpy as np
from jax import lax

D = 6144
QH = 48
KVH = 8
HD = 128
EXPERTS = 4
FF = 8192
REQ_DEV = 4
CTX = 64
BLOCK = 16
BLK_DEV = 4
MOST = 3
TOK = 512
FRESH = 8192


def cache_and_queries(key):
    base = jax.random.fold_in(key, 11)
    k_cache = jax.random.fold_in(base, 0)
    k_query = jax.random.fold_in(base, 2)
    width = 2 * KVH * HD
    cache = jnp.clip(jax.random.normal(k_cache, (TOK, CTX, width), jnp.float32), -6.0, 6.0)
    queries = jax.random.normal(k_query, (TOK, QH * HD), jnp.float32)
    queries = jnp.clip(queries, -250.0, 250.0)
    return (cache, queries)


def draw_kv_cache(key, part):
    cache, queries = cache_and_queries(key)
    return cache.astype(jnp.bfloat16)


def draw_queries(key, part):
    cache, queries = cache_and_queries(key)
    return queries.astype(jnp.bfloat16)


def draw_block_counts(key, part):
    devices = TOK // REQ_DEV
    carried = jax.random.randint(jax.random.fold_in(key, 23), (devices,), 1, BLK_DEV + 1)
    places = jnp.arange(devices, dtype=jnp.int32)
    carried = jnp.where(places == 0, BLK_DEV, carried)
    carried = jnp.where(places == devices - 1, 0, carried)
    before = jnp.concatenate([jnp.zeros((1,), jnp.int32), carried[:-1]], 0)
    return (BLK_DEV + carried - before).astype(jnp.int32)


def plant(values, stream_key, low, high):
    place = [jax.random.randint(jax.random.fold_in(stream_key, axis), (), 0, length) for axis, length in enumerate(values.shape)]
    widest = values.shape.index(max(values.shape))
    neighbour = place[:widest] + [(place[widest] + 1) % values.shape[widest]] + place[widest + 1:]
    return values.at[tuple(place)].set(low).at[tuple(neighbour)].set(high)


def steps_of(key, shape, cuts, least, largest):
    loudness, own = 1.0, jax.random.fold_in(key, 6)
    for dim, parts in cuts:
        draws = jnp.exp(jax.random.uniform(jax.random.fold_in(own, dim), (parts,), jnp.float32, least / len(cuts), largest / len(cuts)))
        loudness = loudness * jnp.repeat(draws, shape[dim] // parts).reshape([-1 if axis == dim else 1 for axis in range(len(shape))])
    return loudness


def deal_out(key, own, number, rows, number_of, top, most, skew):
    sequence = jax.random.permutation(key, number_of)
    packed, common = load_shares(number_of, rows * top, most, skew, True), load_shares(number_of, rows * top, most, skew, False)
    places = jnp.arange(number_of)

    def named(lengths, rotation):
        used = int((lengths > 0).sum())
        fixed = max(1, used // 4)
        passed = fixed + (places - fixed + rotation * (used - fixed)) % max(1, number_of - fixed)
        return jnp.zeros((number_of,), jnp.int32).at[sequence[jnp.where(places < fixed, places, passed)]].set(jnp.asarray(lengths, jnp.int32))

    lengths = jnp.where(number % 4 == 0, named(packed, number // 4), named(common, number - number // 4 - 1))
    mixed = jax.random.permutation(jax.random.fold_in(own, 3), number_of)
    source_of, taker = mixed[0:number_of // 2 * 2:2], mixed[1:number_of // 2 * 2:2]
    slack = jnp.minimum(lengths[source_of] - 1, most - lengths[taker]) // 2
    slack = jnp.where((source_of == sequence[0]) | (taker == sequence[0]) | (lengths[taker] == 0), 0, jnp.maximum(slack, 0))
    passed = jax.random.randint(jax.random.fold_in(own, 4), (number_of // 2,), 0, 1 << 20) % (slack + 1)
    lengths = lengths.at[source_of].add(-passed).at[taker].add(passed)
    members = jnp.searchsorted(jnp.cumsum(lengths), jnp.arange(rows * top), side="right").astype(jnp.int32)
    table = members.reshape(top, rows).T
    table = table[jax.random.permutation(jax.random.fold_in(own, 1), rows)]
    rotation = jax.random.randint(jax.random.fold_in(own, 2), (rows, 1), 0, top)
    return jnp.take_along_axis(table, (jnp.arange(top)[None, :] + rotation) % top, axis=1)


def load_shares(amount, total, bound, lean, full):
    portions = [(1 << 20) // math.isqrt(rank ** lean) + 1 for rank in range(1, amount + 1)]
    largest = bound if full else min(bound, max(-(-total // amount), total * portions[0] // sum(portions)))
    least = 1 if total - largest >= amount - 1 else 0
    counts, rest = [largest] + [least] * (amount - 1), total - largest - least * (amount - 1)
    while rest > 0:
        free = [i for i in range(1, amount) if counts[i] < largest] or [i for i in range(1, amount) if counts[i] < bound]
        pool, left = sum([portions[i] for i in free]), rest
        for i in free:
            addition = min(bound - counts[i], max(1, left * portions[i] // pool), rest)
            counts[i] = counts[i] + addition
            rest = rest - addition
    return np.array(counts)


def bell_draw(rng, shape, scale, reach, cuts=(), held_as=jnp.bfloat16):
    loudness = steps_of(rng, shape, cuts, -0.22, 0.18) if cuts else 1.0
    drawn = jax.random.normal(rng, shape, jnp.float32) * scale * loudness
    return jnp.minimum(jnp.maximum(drawn, -reach), reach).astype(held_as)


def setup_inputs(seed: int = 0, part: int = 0) -> dict:
    splits = jax.random.split(jax.random.key(seed), 14)
    part_splits = jax.random.split(jax.random.fold_in(splits[13], part), 14)
    tokens = bell_draw(part_splits[0], (TOK, D), 1.0, 6.0, ((0, 128),))
    queries = draw_queries(jax.random.fold_in(jax.random.fold_in(splits[13], part), 71), part)
    token_kv = bell_draw(part_splits[2], (TOK, 2 * KVH * HD), 1.0, 6.0, ((0, 128),))
    kv_cache = draw_kv_cache(jax.random.fold_in(jax.random.fold_in(splits[13], part), 71), part)
    context_lengths = plant(jax.random.randint(part_splits[4], (TOK,), 2, CTX + 1), jax.random.fold_in(part_splits[4], 1), 2, CTX).astype(jnp.int32)
    fresh_kv = bell_draw(part_splits[5], (FRESH, 2 * KVH * HD), 1.0, 6.0, ((0, 128),))
    block_counts = draw_block_counts(jax.random.fold_in(jax.random.fold_in(splits[13], part), 71), part)
    expert_ids_keys = jax.random.split(jax.random.fold_in(part_splits[7], 1), TOK // REQ_DEV)
    expert_ids_turns = jax.random.permutation(jax.random.fold_in(part_splits[7], 3), TOK // REQ_DEV)
    expert_ids = jax.vmap(lambda own, number: deal_out(jax.random.fold_in(part_splits[7], 2), own, number, REQ_DEV, EXPERTS, 2, MOST, 2))(expert_ids_keys, expert_ids_turns).reshape((TOK, 2))
    route_weights = jnp.clip(jnp.exp(math.log(1.0) - 1.3862944 * jax.random.uniform(part_splits[8], (TOK, 2), jnp.float32) ** steps_of(part_splits[8], (TOK, 2), ((0, 128),), -0.2, 0.2)), 0.25, 1.0)
    norm_gain = jnp.clip(1.0 + 0.18 * jax.random.normal(splits[9], (D,), jnp.float32), 0.1, 1.9)
    w_gate = bell_draw(splits[10], (D, EXPERTS * FF), D ** -0.5, 0.078125, ((1, 128),))
    w_up = bell_draw(splits[11], (D, EXPERTS * FF), D ** -0.5, 0.078125, ((1, 128),))
    w_down = bell_draw(splits[12], (EXPERTS * FF, D), FF ** -0.5, 0.0625, ((0, 128),))
    return {"tokens": tokens, "queries": queries, "token_kv": token_kv, "kv_cache": kv_cache, "context_lengths": context_lengths, "fresh_kv": fresh_kv, "block_counts": block_counts, "expert_ids": expert_ids, "route_weights": route_weights, "norm_gain": norm_gain, "w_gate": w_gate, "w_up": w_up, "w_down": w_down}


EPS = 1e-05
NEG = -1e+30

def attend(query, cache, lens, own, window, first, last):
    reqs = query.shape[0]
    length = cache.shape[1]
    group = QH // KVH
    half = KVH * HD
    scale = 1.0 / math.sqrt(HD)
    q_all = query.astype(jnp.float32).reshape(reqs, KVH, group, HD)
    keys_c = cache[:, :, :half].astype(jnp.float32).reshape(reqs, length, KVH, HD)
    vals_c = cache[:, :, half:].astype(jnp.float32).reshape(reqs, length, KVH, HD)
    keys_w = window[:, :half].astype(jnp.float32).reshape(-1, KVH, HD)
    vals_w = window[:, half:].astype(jnp.float32).reshape(-1, KVH, HD)
    keys_o = own[:, :half].astype(jnp.float32).reshape(reqs, KVH, HD)
    vals_o = own[:, half:].astype(jnp.float32).reshape(reqs, KVH, HD)
    s_cache = jnp.einsum('rkgh,rpkh->rkgp', q_all, keys_c) * scale
    places = jnp.arange(length, dtype=jnp.int32)
    s_cache = jnp.where(places[None, None, None, :] < lens[:, None, None, None], s_cache, NEG)
    s_win = jnp.einsum('rkgh,pkh->rkgp', q_all, keys_w) * scale
    rows = jnp.arange(window.shape[0], dtype=jnp.int32)
    live = (rows >= first) & (rows < last)
    leader = jnp.arange(reqs, dtype=jnp.int32) == 0
    usable = leader[:, None] & live[None, :]
    s_win = jnp.where(usable[:, None, None, :], s_win, NEG)
    s_own = jnp.einsum('rkgh,rkh->rkg', q_all, keys_o) * scale
    top = jnp.maximum(jnp.maximum(lax.optimization_barrier(jnp.max(s_cache, -1)), lax.optimization_barrier(jnp.max(s_win, -1))), s_own)
    e_cache = jnp.exp(s_cache - top[..., None])
    e_win = jnp.exp(s_win - top[..., None])
    e_own = jnp.exp(s_own - top)
    total = lax.optimization_barrier(jnp.sum(e_cache, -1)) + lax.optimization_barrier(jnp.sum(e_win, -1)) + e_own
    p_cache = (e_cache / total[..., None]).astype(jnp.bfloat16).astype(jnp.float32)
    p_win = (e_win / total[..., None]).astype(jnp.bfloat16).astype(jnp.float32)
    p_own = (e_own / total).astype(jnp.bfloat16).astype(jnp.float32)
    mixed = jnp.einsum('rkgp,rpkh->rkgh', p_cache, vals_c)
    mixed = mixed + jnp.einsum('rkgp,pkh->rkgh', p_win, vals_w)
    mixed = mixed + p_own[..., None] * vals_o[:, :, None, :]
    return mixed.reshape(reqs, QH * HD)

def reference(tokens, queries, token_kv, kv_cache, context_lengths, fresh_kv, block_counts, expert_ids, route_weights, norm_gain, w_gate, w_up, w_down):
    devices = TOK // REQ_DEV
    width = 2 * KVH * HD
    span = BLK_DEV * BLOCK
    fresh = fresh_kv.reshape(devices, span, width)
    following = jnp.concatenate([fresh[1:], jnp.zeros((1, span, width), fresh.dtype)], 0)
    windows = jnp.concatenate([fresh, following], 1)
    offsets = jnp.cumsum(block_counts) - block_counts
    starts = (offsets - jnp.arange(devices, dtype=jnp.int32) * BLK_DEV).astype(jnp.int32)
    ends = (starts + block_counts).astype(jnp.int32)

    def one_device(pieces):
        q_dev, c_dev, l_dev, o_dev, w_dev, s_dev, e_dev = pieces
        return attend(q_dev, c_dev, l_dev, o_dev, w_dev, s_dev * BLOCK, e_dev * BLOCK)
    attn = lax.map(one_device, (queries.reshape(devices, REQ_DEV, QH * HD), kv_cache.reshape(devices, REQ_DEV, CTX, width), context_lengths.reshape(devices, REQ_DEV), token_kv.reshape(devices, REQ_DEV, width), windows, starts, ends)).reshape(TOK, D)
    hidden_state = tokens.astype(jnp.float32) + attn
    spread = lax.optimization_barrier(jnp.mean(hidden_state * hidden_state, -1, keepdims=True))
    normed = (hidden_state * lax.rsqrt(spread + EPS) * norm_gain).astype(jnp.bfloat16)
    labels = jnp.arange(EXPERTS, dtype=jnp.int32)
    coef = lax.optimization_barrier(jnp.sum(route_weights[:, :, None] * (expert_ids[:, :, None] == labels[None, None, :]).astype(jnp.float32), 1))
    shards = devices // EXPERTS
    units = FF // shards
    gates = w_gate.reshape(D, EXPERTS, FF).transpose(1, 0, 2)
    ups = w_up.reshape(D, EXPERTS, FF).transpose(1, 0, 2)
    downs = w_down.reshape(EXPERTS, shards, units, D)

    def one_expert(pieces):
        gate_e, up_e, down_e, coef_e = pieces
        gate_v = jnp.dot(normed, gate_e, preferred_element_type=jnp.float32)
        up_v = jnp.dot(normed, up_e, preferred_element_type=jnp.float32)
        act = (jax.nn.silu(gate_v) * up_v).astype(jnp.bfloat16)
        act_parts = act.reshape(TOK, shards, units).transpose(1, 0, 2)

        def add_shard(total, piece):
            act_s, down_s = piece
            part = jnp.dot(act_s, down_s, preferred_element_type=jnp.float32).astype(jnp.bfloat16)
            part = lax.optimization_barrier(part)
            return (total + part.astype(jnp.float32), None)
        summed, unused = lax.scan(add_shard, jnp.zeros((TOK, D), jnp.float32), (act_parts, down_e))
        return coef_e[:, None] * summed
    contrib = lax.map(one_expert, (gates, ups, downs, coef.T))
    moe = lax.optimization_barrier(jnp.sum(contrib, 0))
    return (hidden_state + moe).astype(jnp.bfloat16)
```

```python
import math

import jax
import jax.numpy as jnp
from jax import lax
from jax.sharding import Mesh
from jax.sharding import PartitionSpec as P

QH = 48
KVH = 8
HD = 128
EXPERTS = 4
BLOCK = 16
MOST = 3
DEV = ("dev_0", "dev_1", "dev_2")
GROUPS_DEV = ("groups", "dev_0", "dev_1", "dev_2")


EPS = 1e-05
NEG = -1e30


def passed_along(value, axis, steps):
    count = lax.axis_size(axis)
    leading, last = (max(0, -steps), min(count, count - steps))
    return lax.ppermute(value, axis, [(source, source + steps) for source in range(leading, last)])


def shifted(value, axis, steps):
    count = lax.axis_size(axis)
    return lax.ppermute(value, axis, [(place, (place + steps) % count) for place in range(count)])


def gathered_both_ways(own, axis):
    far = lax.axis_size(axis) // 2
    blocks = {0: own}
    for step in range(1, far):
        blocks[-step] = shifted(blocks[1 - step], axis, 1)
        blocks[step] = shifted(blocks[step - 1], axis, -1)
    half = own.shape[1] // 2
    left = shifted(blocks[1 - far][:, :half], axis, 1)
    right = shifted(blocks[far - 1][:, half:], axis, -1)
    blocks[far] = jnp.concatenate([left, right], 1)
    return blocks


def added(*terms):
    total = terms[0].astype(jnp.float32)
    for term in terms[1:]:
        total = total + term.astype(jnp.float32)
    return total


def scattered_both_ways(mine, theirs, axis):
    far = lax.axis_size(axis) // 2
    half = mine[0].shape[1] // 2
    last = added(mine[far], theirs[far]).astype(jnp.bfloat16)
    up = shifted(last[:, :half], axis, 1)
    down = shifted(last[:, half:], axis, -1)
    for step in range(far - 1, 0, -1):
        above = added(mine[step], theirs[step])
        below = added(mine[-step], theirs[-step])
        if step == far - 1:
            above = jnp.concatenate([above[:, :half] + up.astype(jnp.float32), above[:, half:]], 1)
            below = jnp.concatenate([below[:, :half], below[:, half:] + down.astype(jnp.float32)], 1)
        else:
            above = above + up.astype(jnp.float32)
            below = below + down.astype(jnp.float32)
        up = shifted(above.astype(jnp.bfloat16), axis, 1)
        down = shifted(below.astype(jnp.bfloat16), axis, -1)
    return added(mine[0], theirs[0], up, down)


def attend(query, cache, lens, own, window, first, last):
    reqs = query.shape[0]
    length = cache.shape[1]
    group = QH // KVH
    half = KVH * HD
    scale = 1.0 / math.sqrt(HD)
    q_all = query.reshape(reqs, KVH, group, HD)
    keys_c = cache[:, :, :half].reshape(reqs, length, KVH, HD)
    vals_c = cache[:, :, half:].reshape(reqs, length, KVH, HD)
    keys_w = window[:, :half].reshape(-1, KVH, HD)
    vals_w = window[:, half:].reshape(-1, KVH, HD)
    keys_o = own[:, :half].reshape(reqs, KVH, HD)
    vals_o = own[:, half:].astype(jnp.float32).reshape(reqs, KVH, HD)
    s_cache = (
        jnp.einsum("rkgh,rpkh->rkgp", q_all, keys_c, preferred_element_type=jnp.float32) * scale
    )
    places = jnp.arange(length, dtype=jnp.int32)
    s_cache = jnp.where(places[None, None, None, :] < lens[:, None, None, None], s_cache, NEG)
    s_win = jnp.einsum("rkgh,pkh->rkgp", q_all, keys_w, preferred_element_type=jnp.float32) * scale
    rows = jnp.arange(window.shape[0], dtype=jnp.int32)
    live = (rows >= first) & (rows < last)
    leader = jnp.arange(reqs, dtype=jnp.int32) == 0
    usable = leader[:, None] & live[None, :]
    s_win = jnp.where(usable[:, None, None, :], s_win, NEG)
    s_own = jnp.einsum("rkgh,rkh->rkg", q_all, keys_o, preferred_element_type=jnp.float32) * scale
    top = jnp.maximum(jnp.maximum(jnp.max(s_cache, -1), jnp.max(s_win, -1)), s_own)
    e_cache = jnp.exp(s_cache - top[..., None])
    e_win = jnp.exp(s_win - top[..., None])
    e_own = jnp.exp(s_own - top)
    total = jnp.sum(e_cache, -1) + jnp.sum(e_win, -1) + e_own
    p_cache = (e_cache / total[..., None]).astype(jnp.bfloat16)
    p_win = (e_win / total[..., None]).astype(jnp.bfloat16)
    p_own = (e_own / total).astype(jnp.bfloat16).astype(jnp.float32)
    mixed = jnp.einsum("rkgp,rpkh->rkgh", p_cache, vals_c, preferred_element_type=jnp.float32)
    mixed = mixed + jnp.einsum("rkgp,pkh->rkgh", p_win, vals_w, preferred_element_type=jnp.float32)
    mixed = mixed + p_own[..., None] * vals_o[:, :, None, :]
    return mixed.reshape(reqs, QH * HD)


def per_device(
    tokens,
    queries,
    token_kv,
    kv_cache,
    context_lengths,
    fresh_kv,
    block_counts,
    expert_ids,
    route_weights,
    norm_gain,
    w_gate,
    w_up,
    w_down,
):
    me = lax.axis_index(DEV)
    reqs = tokens.shape[0]
    width = tokens.shape[1]
    span = fresh_kv.shape[0]
    following = passed_along(fresh_kv, DEV, -1)
    window = jnp.concatenate([fresh_kv, following], 0)
    offsets = jnp.cumsum(block_counts) - block_counts
    mine = lax.dynamic_index_in_dim(offsets, me, 0, keepdims=False)
    taken = lax.dynamic_index_in_dim(block_counts, me, 0, keepdims=False)
    first = (mine - me * (span // BLOCK)) * BLOCK
    last = first + taken * BLOCK
    attn = attend(queries, kv_cache, context_lengths, token_kv, window, first, last)
    hidden_state = tokens.astype(jnp.float32) + attn
    spread = jnp.mean(hidden_state * hidden_state, -1, keepdims=True)
    normed = (hidden_state * lax.rsqrt(spread + EPS) * norm_gain).astype(jnp.bfloat16)
    labels = jnp.arange(EXPERTS, dtype=jnp.int32)
    flat_ids = expert_ids.reshape(-1)
    picks = (flat_ids[:, None] == labels[None, :]).astype(jnp.int32)
    slots = jnp.sum((jnp.cumsum(picks, 0) - picks) * picks, 1).reshape(reqs, 2)
    rows_x = lax.axis_size("dev_0")
    per_expert = rows_x // EXPERTS
    expert_of = jnp.arange(rows_x, dtype=jnp.int32) // per_expert
    slot_ids = jnp.arange(MOST, dtype=jnp.int32)
    named = (expert_ids[None, None, :, :] == expert_of[:, None, None, None]) & (
        slots[None, None, :, :] == slot_ids[None, :, None, None]
    )
    taking = jnp.sum(named.astype(jnp.float32), 3)
    weights = jnp.sum(named.astype(jnp.float32) * route_weights[None, None, :, :], 3)
    leaving = jnp.einsum(
        "xmt,td->xmd", taking.astype(jnp.bfloat16), normed, preferred_element_type=jnp.float32
    ).astype(jnp.bfloat16)
    came = lax.all_to_all(leaving, "dev_0", 0, 0, tiled=True)
    own_block = came.reshape(rows_x * MOST, width)
    blocks = gathered_both_ways(own_block, "dev_1")
    order = sorted(blocks)
    other = {place: shifted(blocks[place], "dev_2", 1) for place in order}
    rows = jnp.concatenate([blocks[k] for k in order] + [other[k] for k in order], 0)
    gate_v = jnp.dot(rows, w_gate, preferred_element_type=jnp.float32)
    up_v = jnp.dot(rows, w_up, preferred_element_type=jnp.float32)
    act = (jax.nn.silu(gate_v) * up_v).astype(jnp.bfloat16)
    part = jnp.dot(act, w_down, preferred_element_type=jnp.float32).astype(jnp.bfloat16)
    each = rows_x * MOST
    here = each * len(order)
    back = shifted(part[here:], "dev_2", 1)
    mine = {k: part[i * each : (i + 1) * each] for i, k in enumerate(order)}
    theirs = {k: back[i * each : (i + 1) * each] for i, k in enumerate(order)}
    summed = scattered_both_ways(mine, theirs, "dev_1").astype(jnp.bfloat16)
    home = lax.all_to_all(summed.reshape(rows_x, MOST, width), "dev_0", 0, 0, tiled=True)
    moe = jnp.einsum(
        "xmt,xmd->td", weights, home.astype(jnp.float32), precision=lax.Precision.HIGHEST
    )
    return (hidden_state + moe).astype(jnp.bfloat16)


def solution(mesh):
    split = Mesh(
        mesh.devices.reshape(mesh.shape["groups"], 8, 8, 2), ("groups", "dev_0", "dev_1", "dev_2")
    )
    return jax.shard_map(
        per_device,
        mesh=split,
        in_specs=(
            P(GROUPS_DEV, None),
            P(GROUPS_DEV, None),
            P(GROUPS_DEV, None),
            P(GROUPS_DEV, None, None),
            P(GROUPS_DEV),
            P(GROUPS_DEV, None),
            P("groups"),
            P(GROUPS_DEV, None),
            P(GROUPS_DEV, None),
            P(),
            P(None, DEV),
            P(None, DEV),
            P(DEV, None),
        ),
        out_specs=P(GROUPS_DEV, None),
        check_vma=False,
    )
```

```python
import math

import jax
import jax.numpy as jnp
from jax import lax
from jax.experimental import pallas as pl
from jax.experimental.pallas import tpu as pltpu
from jax.sharding import Mesh
from jax.sharding import PartitionSpec as P


QH = 48
KVH = 8
HD = 128
EXPERTS = 4
BLOCK = 16
MOST = 3
DEV = ("dev_0", "dev_1", "dev_2")
GROUPS_DEV = ("groups", "dev_0", "dev_1", "dev_2")


EPS = 1e-05
NEG = -1e30

PIECES = 16
CUT_K = 8
CUT_N = 4


def passed_along(value, axis, steps):
    count = lax.axis_size(axis)
    leading, last = (max(0, -steps), min(count, count - steps))
    return lax.ppermute(value, axis, [(source, source + steps) for source in range(leading, last)])


def shifted(value, axis, steps):
    count = lax.axis_size(axis)
    return lax.ppermute(value, axis, [(place, (place + steps) % count) for place in range(count)])


def swapped(value):
    return shifted(value, "dev_2", 1)


def passed_on(value):
    chips, cores = lax.axis_size("dev_1"), lax.axis_size("dev_2")
    pairs = []
    for chip in range(chips):
        for core in range(cores):
            pairs.append((chip * cores + core, (chip + 1 - 2 * core) % chips * cores + core))
    return lax.ppermute(value, ("dev_1", "dev_2"), pairs)


def added(*terms):
    total = terms[0].astype(jnp.float32)
    for term in terms[1:]:
        total = total + term.astype(jnp.float32)
    return total


def gathered(own):
    other = swapped(own)
    far = lax.axis_size("dev_1") // 2
    came, theirs = {}, {}
    block = {0: own, 1: other}
    for step in range(1, far + 1):
        for part in (0, 1) if step < far else (0,):
            block[part] = passed_on(block[part])
            came[step, part] = block[part]
        for part in (0, 1) if step < far else (0,):
            theirs[step, part] = swapped(came[step, part])
    return own, other, came, theirs


def chain_order(far):
    return [(far - i, 0) for i in range(far)], [(far - i, 1) for i in range(1, far)]


def scattered(far, each, own, other, kept, sent):
    got = [swapped(sent[part]) for part in (0, 1)]
    moving = {}
    for step in range(far, 0, -1):
        for part in (0, 1) if step < far else (0,):
            at = (far - part - step) * each
            terms = [x[at : at + each] for x in (kept[part], got[part])]
            parcel = added(*terms, *moving.get(part, ())).astype(jnp.bfloat16)
            moving[part] = (passed_on(parcel),)
    leaving = added(other, *moving[0]).astype(jnp.bfloat16)
    return added(own, *moving[1], swapped(leaving)).astype(jnp.bfloat16)


def experts_kernel(*refs):
    pieces = refs[:PIECES]
    gate_hbm, up_hbm, down_hbm = refs[PIECES : PIECES + 3]
    outs = refs[PIECES + 3 : PIECES + 9]
    gate, up, down, sems = refs[PIECES + 9 :]
    depth = gate.shape[0] // CUT_K
    span = down.shape[1] // CUT_N
    copies = []
    for k in range(CUT_K):
        rows = pl.ds(k * depth, depth)
        copies.append(
            (
                pltpu.make_async_copy(gate_hbm.at[rows], gate.at[rows], sems.at[2 * k]),
                pltpu.make_async_copy(up_hbm.at[rows], up.at[rows], sems.at[2 * k + 1]),
            )
        )
    last = pltpu.make_async_copy(down_hbm, down, sems.at[2 * CUT_K])
    for pair in copies:
        pair[0].start()
        pair[1].start()
    last.start()
    gate_v = up_v = None
    for k in range(CUT_K):
        cols = pl.ds(k * depth, depth)
        x = jnp.concatenate([p[:, cols] for p in pieces], 0)
        copies[k][0].wait()
        copies[k][1].wait()
        g = jnp.dot(x, gate[cols, :], preferred_element_type=jnp.float32)
        u = jnp.dot(x, up[cols, :], preferred_element_type=jnp.float32)
        gate_v = g if gate_v is None else gate_v + g
        up_v = u if up_v is None else up_v + u
    act = (gate_v / (1.0 + jnp.exp(-gate_v)) * up_v).astype(jnp.bfloat16)
    last.wait()
    for n in range(CUT_N):
        cols = pl.ds(n * span, span)
        part = jnp.dot(act, down[:, cols], preferred_element_type=jnp.float32).astype(jnp.bfloat16)
        at = 0
        for out in outs:
            rows = out.shape[0]
            out[:, cols] = part[at : at + rows]
            at += rows


def experts(pieces, w_gate, w_up, w_down, sizes):
    width = w_gate.shape[0]
    hidden = w_gate.shape[1]
    vm = pl.BlockSpec(memory_space=pltpu.VMEM)
    anyspec = pl.BlockSpec(memory_space=pl.ANY)
    total = sum(sizes)
    return pl.pallas_call(
        experts_kernel,
        out_shape=[jax.ShapeDtypeStruct((s, width), jnp.bfloat16) for s in sizes],
        in_specs=[vm] * PIECES + [anyspec] * 3,
        out_specs=[vm] * len(sizes),
        scratch_shapes=[
            pltpu.VMEM((width, hidden), jnp.bfloat16),
            pltpu.VMEM((width, hidden), jnp.bfloat16),
            pltpu.VMEM((hidden, width), jnp.bfloat16),
            pltpu.SemaphoreType.DMA((2 * CUT_K + 1,)),
        ],
        compiler_params=pltpu.CompilerParams(vmem_limit_bytes=40 * 1024 * 1024),
        cost_estimate=pl.CostEstimate(flops=6 * total * width * hidden, bytes_accessed=6 * width * hidden, transcendentals=total * hidden),
        name="experts",
    )(*pieces, w_gate, w_up, w_down)


def attend(query, cache, lens, own, window, first, last):
    reqs = query.shape[0]
    length = cache.shape[1]
    group = QH // KVH
    half = KVH * HD
    scale = 1.0 / math.sqrt(HD)
    q_all = query.reshape(reqs, KVH, group, HD)
    keys_c = cache[:, :, :half].reshape(reqs, length, KVH, HD)
    vals_c = cache[:, :, half:].reshape(reqs, length, KVH, HD)
    keys_w = window[:, :half].reshape(-1, KVH, HD)
    vals_w = window[:, half:].reshape(-1, KVH, HD)
    keys_o = own[:, :half].reshape(reqs, KVH, HD)
    vals_o = own[:, half:].astype(jnp.float32).reshape(reqs, KVH, HD)
    s_cache = (
        jnp.einsum("rkgh,rpkh->rkgp", q_all, keys_c, preferred_element_type=jnp.float32) * scale
    )
    places = jnp.arange(length, dtype=jnp.int32)
    s_cache = jnp.where(places[None, None, None, :] < lens[:, None, None, None], s_cache, NEG)
    s_win = jnp.einsum("rkgh,pkh->rkgp", q_all, keys_w, preferred_element_type=jnp.float32) * scale
    rows = jnp.arange(window.shape[0], dtype=jnp.int32)
    live = (rows >= first) & (rows < last)
    leader = jnp.arange(reqs, dtype=jnp.int32) == 0
    usable = leader[:, None] & live[None, :]
    s_win = jnp.where(usable[:, None, None, :], s_win, NEG)
    s_own = jnp.einsum("rkgh,rkh->rkg", q_all, keys_o, preferred_element_type=jnp.float32) * scale
    top = jnp.maximum(jnp.maximum(jnp.max(s_cache, -1), jnp.max(s_win, -1)), s_own)
    e_cache = jnp.exp(s_cache - top[..., None])
    e_win = jnp.exp(s_win - top[..., None])
    e_own = jnp.exp(s_own - top)
    total = jnp.sum(e_cache, -1) + jnp.sum(e_win, -1) + e_own
    p_cache = (e_cache / total[..., None]).astype(jnp.bfloat16)
    p_win = (e_win / total[..., None]).astype(jnp.bfloat16)
    p_own = (e_own / total).astype(jnp.bfloat16).astype(jnp.float32)
    mixed = jnp.einsum("rkgp,rpkh->rkgh", p_cache, vals_c, preferred_element_type=jnp.float32)
    mixed = mixed + jnp.einsum("rkgp,pkh->rkgh", p_win, vals_w, preferred_element_type=jnp.float32)
    mixed = mixed + p_own[..., None] * vals_o[:, :, None, :]
    return mixed.reshape(reqs, QH * HD)


def layer(
    tokens,
    queries,
    token_kv,
    kv_cache,
    context_lengths,
    fresh_kv,
    block_counts,
    expert_ids,
    route_weights,
    norm_gain,
    w_gate,
    w_up,
    w_down,
):
    me = lax.axis_index(DEV)
    reqs = tokens.shape[0]
    width = tokens.shape[1]
    span = fresh_kv.shape[0]
    following = passed_along(fresh_kv, DEV, -1)
    window = jnp.concatenate([fresh_kv, following], 0)
    offsets = jnp.cumsum(block_counts) - block_counts
    mine = lax.dynamic_index_in_dim(offsets, me, 0, keepdims=False)
    taken = lax.dynamic_index_in_dim(block_counts, me, 0, keepdims=False)
    first = (mine - me * (span // BLOCK)) * BLOCK
    last = first + taken * BLOCK
    attn = attend(queries, kv_cache, context_lengths, token_kv, window, first, last)
    hidden_state = tokens.astype(jnp.float32) + attn
    spread = jnp.mean(hidden_state * hidden_state, -1, keepdims=True)
    normed = (hidden_state * lax.rsqrt(spread + EPS) * norm_gain).astype(jnp.bfloat16)
    labels = jnp.arange(EXPERTS, dtype=jnp.int32)
    flat_ids = expert_ids.reshape(-1)
    picks = (flat_ids[:, None] == labels[None, :]).astype(jnp.int32)
    slots = jnp.sum((jnp.cumsum(picks, 0) - picks) * picks, 1).reshape(reqs, 2)
    rows_x = lax.axis_size("dev_0")
    per_expert = rows_x // EXPERTS
    expert_of = jnp.arange(rows_x, dtype=jnp.int32) // per_expert
    slot_ids = jnp.arange(MOST, dtype=jnp.int32)
    named = (expert_ids[None, None, :, :] == expert_of[:, None, None, None]) & (
        slots[None, None, :, :] == slot_ids[None, :, None, None]
    )
    taking = jnp.sum(named.astype(jnp.float32), 3)
    weights = jnp.sum(named.astype(jnp.float32) * route_weights[None, None, :, :], 3)
    leaving = jnp.einsum(
        "xmt,td->xmd", taking.astype(jnp.bfloat16), normed, preferred_element_type=jnp.float32
    ).astype(jnp.bfloat16)
    came = lax.all_to_all(leaving, "dev_0", 0, 0, tiled=True)
    own_block = came.reshape(rows_x * MOST, width)
    own, other, came, theirs = gathered(own_block)
    far = lax.axis_size("dev_1") // 2
    chains = chain_order(far)
    each = rows_x * MOST
    pieces = [own, other]
    for group in (theirs, came):
        for chain in chains:
            pieces += [group[key] for key in chain]
    sizes = [each, each] + 2 * [len(chain) * each for chain in chains]
    home_own, home_other, kept_0, kept_1, sent_0, sent_1 = experts(pieces, w_gate, w_up, w_down, sizes)
    summed = scattered(far, each, home_own, home_other, (kept_0, kept_1), (sent_0, sent_1))
    home = lax.all_to_all(summed.reshape(rows_x, MOST, width), "dev_0", 0, 0, tiled=True)
    moe = jnp.einsum(
        "xmt,xmd->td", weights, home.astype(jnp.float32), precision=lax.Precision.HIGHEST
    )
    return (hidden_state + moe).astype(jnp.bfloat16)


def solution(mesh):
    split = Mesh(
        mesh.devices.reshape(mesh.shape["groups"], 8, 8, 2), ("groups", "dev_0", "dev_1", "dev_2")
    )
    return jax.shard_map(
        layer,
        mesh=split,
        in_specs=(
            P(GROUPS_DEV, None),
            P(GROUPS_DEV, None),
            P(GROUPS_DEV, None),
            P(GROUPS_DEV, None, None),
            P(GROUPS_DEV),
            P(GROUPS_DEV, None),
            P("groups"),
            P(GROUPS_DEV, None),
            P(GROUPS_DEV, None),
            P(),
            P(None, DEV),
            P(None, DEV),
            P(DEV, None),
        ),
        out_specs=P(GROUPS_DEV, None),
        check_vma=False,
    )
```

```python
import math

import jax
import jax.numpy as jnp
from jax import lax
from jax.experimental import pallas as pl
from jax.experimental.pallas import tpu as pltpu
from jax.sharding import Mesh
from jax.sharding import PartitionSpec as P


QH = 48
KVH = 8
HD = 128
EXPERTS = 4
BLOCK = 16
MOST = 3
DEV = ("dev_0", "dev_1", "dev_2")
GROUPS_DEV = ("groups", "dev_0", "dev_1", "dev_2")


EPS = 1e-05
NEG = -1e30

PIECES = 16
CUT_K = 8
CUT_N = 4


def passed_along(value, axis, steps):
    count = lax.axis_size(axis)
    leading, last = (max(0, -steps), min(count, count - steps))
    return lax.ppermute(value, axis, [(source, source + steps) for source in range(leading, last)])


def shifted(value, axis, steps):
    count = lax.axis_size(axis)
    return lax.ppermute(value, axis, [(place, (place + steps) % count) for place in range(count)])


def swapped(value):
    return shifted(value, "dev_2", 1)


def passed_on(value):
    chips, cores = lax.axis_size("dev_1"), lax.axis_size("dev_2")
    pairs = []
    for chip in range(chips):
        for core in range(cores):
            pairs.append((chip * cores + core, (chip + 1 - 2 * core) % chips * cores + core))
    return lax.ppermute(value, ("dev_1", "dev_2"), pairs)


def added(*terms):
    total = terms[0].astype(jnp.float32)
    for term in terms[1:]:
        total = total + term.astype(jnp.float32)
    return total


def gathered(own):
    other = swapped(own)
    far = lax.axis_size("dev_1") // 2
    came, theirs = {}, {}
    block = {0: own, 1: other}
    for step in range(1, far + 1):
        for part in (0, 1) if step < far else (0,):
            block[part] = passed_on(block[part])
            came[step, part] = block[part]
        for part in (0, 1) if step < far else (0,):
            theirs[step, part] = swapped(came[step, part])
    return own, other, came, theirs


def chain_order(far):
    return [(far - i, 0) for i in range(far)], [(far - i, 1) for i in range(1, far)]


def scattered(far, each, own, other, kept, sent):
    got = [swapped(sent[part]) for part in (0, 1)]
    moving = {}
    for step in range(far, 0, -1):
        for part in (0, 1) if step < far else (0,):
            at = (far - part - step) * each
            terms = [x[at : at + each] for x in (kept[part], got[part])]
            parcel = added(*terms, *moving.get(part, ())).astype(jnp.bfloat16)
            moving[part] = (passed_on(parcel),)
    leaving = added(other, *moving[0]).astype(jnp.bfloat16)
    return own, *moving[1], swapped(leaving)


def experts_kernel(*refs):
    pieces = refs[:PIECES]
    gate_hbm, up_hbm, down_hbm = refs[PIECES : PIECES + 3]
    outs = refs[PIECES + 3 : PIECES + 9]
    gate, up, down, sems = refs[PIECES + 9 :]
    depth = gate.shape[0] // CUT_K
    span = down.shape[1] // CUT_N
    copies = []
    for k in range(CUT_K):
        rows = pl.ds(k * depth, depth)
        copies.append(
            (
                pltpu.make_async_copy(gate_hbm.at[rows], gate.at[rows], sems.at[2 * k]),
                pltpu.make_async_copy(up_hbm.at[rows], up.at[rows], sems.at[2 * k + 1]),
            )
        )
    last = pltpu.make_async_copy(down_hbm, down, sems.at[2 * CUT_K])
    for pair in copies:
        pair[0].start()
        pair[1].start()
    last.start()
    gate_v = up_v = None
    for k in range(CUT_K):
        cols = pl.ds(k * depth, depth)
        x = jnp.concatenate([p[:, cols] for p in pieces], 0)
        copies[k][0].wait()
        copies[k][1].wait()
        g = jnp.dot(x, gate[cols, :], preferred_element_type=jnp.float32)
        u = jnp.dot(x, up[cols, :], preferred_element_type=jnp.float32)
        gate_v = g if gate_v is None else gate_v + g
        up_v = u if up_v is None else up_v + u
    act = (gate_v / (1.0 + jnp.exp(-gate_v)) * up_v).astype(jnp.bfloat16)
    last.wait()
    for n in range(CUT_N):
        cols = pl.ds(n * span, span)
        part = jnp.dot(act, down[:, cols], preferred_element_type=jnp.float32).astype(jnp.bfloat16)
        at = 0
        for out in outs:
            rows = out.shape[0]
            out[:, cols] = part[at : at + rows]
            at += rows


def experts(pieces, w_gate, w_up, w_down, sizes):
    width = w_gate.shape[0]
    hidden = w_gate.shape[1]
    vm = pl.BlockSpec(memory_space=pltpu.VMEM)
    anyspec = pl.BlockSpec(memory_space=pl.ANY)
    total = sum(sizes)
    return pl.pallas_call(
        experts_kernel,
        out_shape=[jax.ShapeDtypeStruct((s, width), jnp.bfloat16) for s in sizes],
        in_specs=[vm] * PIECES + [anyspec] * 3,
        out_specs=[vm] * len(sizes),
        scratch_shapes=[
            pltpu.VMEM((width, hidden), jnp.bfloat16),
            pltpu.VMEM((width, hidden), jnp.bfloat16),
            pltpu.VMEM((hidden, width), jnp.bfloat16),
            pltpu.SemaphoreType.DMA((2 * CUT_K + 1,)),
        ],
        compiler_params=pltpu.CompilerParams(vmem_limit_bytes=40 * 1024 * 1024),
        cost_estimate=pl.CostEstimate(flops=6 * total * width * hidden, bytes_accessed=6 * width * hidden, transcendentals=total * hidden),
        name="experts",
    )(*pieces, w_gate, w_up, w_down)


def slots_of(ids_ref, reqs, top):
    named = [ids_ref[k, t] for t in range(reqs) for k in range(top)]
    slots = []
    for i, one in enumerate(named):
        slot = jnp.int32(0)
        for earlier in named[:i]:
            slot = slot + (earlier == one).astype(jnp.int32)
        slots.append(slot)
    return named, slots


def attend_kernel(me_ref, *refs):
    next_ref = refs[0]
    far_refs, (hidden_ref, leaving_ref, turned, mixed, packed), near_refs = refs[1:10], refs[10:15], refs[15:24]
    copies = [pltpu.make_async_copy(f, n, refs[24].at[i]) for i, (f, n) in enumerate(zip(far_refs, near_refs))]
    for copy in copies:
        copy.start()
    lens_ref, ids_ref, counts_ref, query_ref, own_ref, cache_ref, fresh_ref, tokens_ref, gain_ref = near_refs
    reqs, width = tokens_ref.shape
    length = cache_ref.shape[1]
    span = fresh_ref.shape[0]
    group = QH // KVH
    rows = group * reqs
    half = KVH * HD
    scale = 1.0 / math.sqrt(HD)
    me = me_ref[0]
    f32 = jnp.float32
    for copy in copies:
        copy.wait()
    for h in range(QH):
        turned[h * reqs : (h + 1) * reqs, :] = query_ref[:, h * HD : (h + 1) * HD].astype(f32)
    counts = counts_ref[...].astype(f32)
    places = lax.broadcasted_iota(jnp.int32, counts.shape, 1)
    before = jnp.sum(jnp.where(places < me, counts, 0.0), 1, keepdims=True)
    taken = jnp.sum(jnp.where(places == me, counts, 0.0), 1, keepdims=True)
    first = (before - (me * (span // BLOCK)).astype(f32)) * BLOCK
    last = first + taken * BLOCK
    row_w = lax.broadcasted_iota(jnp.int32, (rows, 2 * span), 0) % reqs
    col_w = lax.broadcasted_iota(jnp.int32, (rows, 2 * span), 1).astype(f32)
    live_w = (row_w == 0) & (col_w >= first) & (col_w < last)
    row_c = lax.broadcasted_iota(jnp.int32, (rows, reqs * length), 0) % reqs
    col_c = lax.broadcasted_iota(jnp.int32, (rows, reqs * length), 1)
    live_c = (row_c < 0)
    for r in range(reqs):
        live_c = live_c | ((row_c == r) & (col_c >= r * length) & (col_c < r * length + lens_ref[r]))
    for g in range(KVH):
        k_at = slice(g * HD, (g + 1) * HD)
        v_at = slice(half + g * HD, half + (g + 1) * HD)
        q32 = turned[g * rows : (g + 1) * rows, :]
        q = q32.astype(jnp.bfloat16)
        contract = (((1,), (1,)), ((), ()))
        key_c = cache_ref[:, :, k_at].reshape(reqs * length, HD)
        key_w = jnp.concatenate([fresh_ref[:, k_at], next_ref[:, k_at]], 0)
        key_o = jnp.concatenate([own_ref[:, k_at].astype(f32)] * group, 0)
        val_o = jnp.concatenate([own_ref[:, v_at].astype(f32)] * group, 0)
        s_c = lax.dot_general(q, key_c, contract, preferred_element_type=f32) * scale
        s_w = lax.dot_general(q, key_w, contract, preferred_element_type=f32) * scale
        s_o = jnp.sum(q32 * key_o, 1, keepdims=True) * scale
        s_c = jnp.where(live_c, s_c, NEG)
        s_w = jnp.where(live_w, s_w, NEG)
        top = jnp.maximum(jnp.maximum(jnp.max(s_c, 1, keepdims=True), jnp.max(s_w, 1, keepdims=True)), s_o)
        e_c = jnp.exp(s_c - top)
        e_w = jnp.exp(s_w - top)
        e_o = jnp.exp(s_o - top)
        total = jnp.sum(e_c, 1, keepdims=True) + jnp.sum(e_w, 1, keepdims=True) + e_o
        over = 1.0 / total
        p_c = (e_c * over).astype(jnp.bfloat16)
        p_w = (e_w * over).astype(jnp.bfloat16)
        p_o = (e_o * over).astype(jnp.bfloat16).astype(f32)
        val_c = cache_ref[:, :, v_at].reshape(reqs * length, HD)
        val_w = jnp.concatenate([fresh_ref[:, v_at], next_ref[:, v_at]], 0)
        out = jnp.dot(p_c, val_c, preferred_element_type=f32) + jnp.dot(p_w, val_w, preferred_element_type=f32)
        mixed[g * rows : (g + 1) * rows, :] = out + p_o * val_o
    squares = jnp.zeros((reqs, HD), f32)
    for h in range(QH):
        cols = slice(h * HD, (h + 1) * HD)
        hidden = tokens_ref[:, cols].astype(f32) + mixed[h * reqs : (h + 1) * reqs, :]
        hidden_ref[:, cols] = hidden
        squares = squares + hidden * hidden
    norm = lax.rsqrt(jnp.sum(squares, 1, keepdims=True) / width + EPS)
    normed = (hidden_ref[...] * norm * gain_ref[...]).astype(jnp.bfloat16).astype(f32)
    named, slots = slots_of(ids_ref, reqs, ids_ref.shape[0])
    tall = leaving_ref.shape[0] // EXPERTS
    padded = MOST + 1
    cell = lax.broadcasted_iota(jnp.int32, (EXPERTS * padded, 1), 0)
    gone = jnp.zeros((EXPERTS * padded, width), f32)
    for t in range(reqs):
        takes = jnp.zeros((EXPERTS * padded, 1), f32)
        for k in range(ids_ref.shape[0]):
            i = t * ids_ref.shape[0] + k
            takes = takes + (cell == named[i] * padded + slots[i]).astype(f32)
        gone = gone + takes * normed[t : t + 1, :]
    for j in range(width // HD):
        packed[pl.ds(j, EXPERTS * padded, stride=width // HD), :] = gone[:, j * HD : (j + 1) * HD]
    cut = width // HD
    for x in range(leaving_ref.shape[0]):
        at = x // tall * padded * cut
        leaving_ref[x, :, :] = packed[at : at + MOST * cut, :].astype(jnp.bfloat16)


def attended(me, lens, ids, counts, query, own, cache, fresh, following, tokens, gain, places):
    reqs, width = tokens.shape
    sm = pl.BlockSpec(memory_space=pltpu.SMEM)
    vm = pl.BlockSpec(memory_space=pltpu.VMEM)
    far = (lens, ids, counts, query, own, cache, fresh, tokens, gain)
    far = [pltpu.with_memory_space_constraint(x, pltpu.HBM) for x in far]
    return pl.pallas_call(
        attend_kernel,
        out_shape=[jax.ShapeDtypeStruct((reqs, width), jnp.float32), jax.ShapeDtypeStruct((places, MOST * width // HD, HD), jnp.bfloat16)],
        in_specs=[sm, vm] + [pl.BlockSpec(memory_space=pltpu.HBM)] * len(far),
        out_specs=[vm, vm],
        scratch_shapes=[
            pltpu.VMEM((QH * reqs, HD), jnp.float32),
            pltpu.VMEM((QH * reqs, HD), jnp.float32),
            pltpu.VMEM((EXPERTS * (MOST + 1) * width // HD, HD), jnp.float32),
            *(pltpu.SMEM(x.shape, x.dtype) for x in far[:2]),
            *(pltpu.VMEM(x.shape, x.dtype) for x in far[2:]),
            pltpu.SemaphoreType.DMA((len(far),)),
        ],
        compiler_params=pltpu.CompilerParams(vmem_limit_bytes=16 * 1024 * 1024),
        cost_estimate=pl.CostEstimate(flops=8 * reqs * width * 392, bytes_accessed=2 * 1024 * 1024, transcendentals=0),
        name="attended",
    )(me, following, *far)


def unpack_kernel(came_ref, block_ref, spread):
    rows, width = block_ref.shape
    spread[...] = came_ref[...].astype(jnp.float32).reshape(spread.shape)
    for j in range(width // HD):
        block_ref[:, j * HD : (j + 1) * HD] = spread[pl.ds(j, rows, stride=width // HD), :].astype(jnp.bfloat16)


def unpacked(came):
    places, packed, lanes = came.shape
    vm = pl.BlockSpec(memory_space=pltpu.VMEM)
    return pl.pallas_call(
        unpack_kernel,
        out_shape=jax.ShapeDtypeStruct((places * MOST, packed // MOST * lanes), jnp.bfloat16),
        in_specs=[vm],
        out_specs=vm,
        scratch_shapes=[pltpu.VMEM((places * packed, lanes), jnp.float32)],
        compiler_params=pltpu.CompilerParams(vmem_limit_bytes=8 * 1024 * 1024),
        name="unpacked",
    )(came)


def pack_kernel(first_ref, second_ref, third_ref, packed_ref, spread):
    rows, width = first_ref.shape
    f32 = jnp.float32
    for j in range(width // HD):
        cols = slice(j * HD, (j + 1) * HD)
        total = first_ref[:, cols].astype(f32) + second_ref[:, cols].astype(f32) + third_ref[:, cols].astype(f32)
        spread[pl.ds(j, rows, stride=width // HD), :] = total
    packed_ref[...] = spread[...].astype(jnp.bfloat16).reshape(packed_ref.shape)


def packed_sum(first, second, third, places):
    rows, width = first.shape
    vm = pl.BlockSpec(memory_space=pltpu.VMEM)
    return pl.pallas_call(
        pack_kernel,
        out_shape=jax.ShapeDtypeStruct((places, rows // places * width // HD, HD), jnp.bfloat16),
        in_specs=[vm] * 3,
        out_specs=vm,
        scratch_shapes=[pltpu.VMEM((rows * width // HD, HD), jnp.float32)],
        compiler_params=pltpu.CompilerParams(vmem_limit_bytes=8 * 1024 * 1024),
        name="packed_sum",
    )(first, second, third)


def mix_kernel(ids_ref, weights_ref, home_ref, hidden_ref, out_ref, spread):
    reqs, width = hidden_ref.shape
    tall = home_ref.shape[0] // EXPERTS
    cut = width // HD
    f32 = jnp.float32
    named, slots = slots_of(ids_ref, reqs, ids_ref.shape[0])
    sums = [jnp.zeros((cut, HD), f32) for _ in range(reqs)]
    for e in range(EXPERTS):
        for m in range(MOST):
            at = slice(m * cut, (m + 1) * cut)
            cell = home_ref[e * tall, at, :].astype(f32)
            for x in range(1, tall):
                cell = cell + home_ref[e * tall + x, at, :].astype(f32)
            for t in range(reqs):
                weight = jnp.float32(0.0)
                for k in range(ids_ref.shape[0]):
                    i = t * ids_ref.shape[0] + k
                    here = (named[i] == e) & (slots[i] == m)
                    weight = weight + jnp.where(here, weights_ref[k, t], 0.0)
                sums[t] = sums[t] + weight * cell
    for t in range(reqs):
        spread[t * cut : (t + 1) * cut, :] = sums[t]
    for j in range(cut):
        cols = slice(j * HD, (j + 1) * HD)
        moe = spread[pl.ds(j, reqs, stride=cut), :]
        out_ref[:, cols] = (hidden_ref[:, cols] + moe).astype(jnp.bfloat16)


def mixed_in(ids, weights, home, hidden):
    reqs, width = hidden.shape
    sm = pl.BlockSpec(memory_space=pltpu.SMEM)
    vm = pl.BlockSpec(memory_space=pltpu.VMEM)
    return pl.pallas_call(
        mix_kernel,
        out_shape=jax.ShapeDtypeStruct((reqs, width), jnp.bfloat16),
        in_specs=[sm, sm, vm, vm],
        out_specs=vm,
        scratch_shapes=[pltpu.VMEM((reqs * width // HD, HD), jnp.float32)],
        compiler_params=pltpu.CompilerParams(vmem_limit_bytes=8 * 1024 * 1024),
        name="mixed_in",
    )(ids, weights, home, hidden)


def layer(
    tokens,
    queries,
    token_kv,
    kv_cache,
    context_lengths,
    fresh_kv,
    block_counts,
    expert_ids,
    route_weights,
    norm_gain,
    w_gate,
    w_up,
    w_down,
):
    me = lax.axis_index(DEV)
    following = passed_along(fresh_kv, DEV, -1)
    rows_x = lax.axis_size("dev_0")
    me = lax.axis_index(DEV).astype(jnp.int32)[None]
    hidden_state, leaving = attended(
        me,
        context_lengths,
        expert_ids.T,
        block_counts[None],
        queries,
        token_kv,
        kv_cache,
        fresh_kv,
        following,
        tokens,
        norm_gain[None],
        rows_x,
    )
    own_block = unpacked(lax.all_to_all(leaving, "dev_0", 0, 0, tiled=True))
    own, other, came, theirs = gathered(own_block)
    far = lax.axis_size("dev_1") // 2
    chains = chain_order(far)
    each = rows_x * MOST
    pieces = [own, other]
    for group in (theirs, came):
        for chain in chains:
            pieces += [group[key] for key in chain]
    sizes = [each, each] + 2 * [len(chain) * each for chain in chains]
    home_own, home_other, kept_0, kept_1, sent_0, sent_1 = experts(pieces, w_gate, w_up, w_down, sizes)
    last_terms = scattered(far, each, home_own, home_other, (kept_0, kept_1), (sent_0, sent_1))
    home = lax.all_to_all(packed_sum(*last_terms, rows_x), "dev_0", 0, 0, tiled=True)
    return mixed_in(expert_ids.T, route_weights.T, home, hidden_state)


def solution(mesh):
    split = Mesh(
        mesh.devices.reshape(mesh.shape["groups"], 8, 8, 2), ("groups", "dev_0", "dev_1", "dev_2")
    )
    return jax.shard_map(
        layer,
        mesh=split,
        in_specs=(
            P(GROUPS_DEV, None),
            P(GROUPS_DEV, None),
            P(GROUPS_DEV, None),
            P(GROUPS_DEV, None, None),
            P(GROUPS_DEV),
            P(GROUPS_DEV, None),
            P("groups"),
            P(GROUPS_DEV, None),
            P(GROUPS_DEV, None),
            P(),
            P(None, DEV),
            P(None, DEV),
            P(DEV, None),
        ),
        out_specs=P(GROUPS_DEV, None),
        check_vma=False,
    )
```

```python
import functools
import math

import jax
import jax.numpy as jnp
from jax import lax
from jax.experimental import pallas as pl
from jax.experimental.pallas import tpu as pltpu
from jax.sharding import Mesh
from jax.sharding import PartitionSpec as P


QH = 48
KVH = 8
HD = 128
EXPERTS = 4
BLOCK = 16
MOST = 3
DEV = ("dev_0", "dev_1", "dev_2")
GROUPS_DEV = ("groups", "dev_0", "dev_1", "dev_2")


EPS = 1e-05
NEG = -1e30

CUT_K = 8
CUT_N = 4


def passed_along(value, axis, steps):
    count = lax.axis_size(axis)
    leading, last = (max(0, -steps), min(count, count - steps))
    return lax.ppermute(value, axis, [(source, source + steps) for source in range(leading, last)])


def shifted(value, axis, steps):
    count = lax.axis_size(axis)
    return lax.ppermute(value, axis, [(place, (place + steps) % count) for place in range(count)])


def swapped(value):
    return shifted(value, "dev_2", 1)


def passed_on(value):
    chips, cores = lax.axis_size("dev_1"), lax.axis_size("dev_2")
    pairs = []
    for chip in range(chips):
        for core in range(cores):
            pairs.append((chip * cores + core, (chip + 1 - 2 * core) % chips * cores + core))
    return lax.ppermute(value, ("dev_1", "dev_2"), pairs)


def added(*terms):
    total = terms[0].astype(jnp.float32)
    for term in terms[1:]:
        total = total + term.astype(jnp.float32)
    return total


def gathered(own):
    other = swapped(own)
    far = lax.axis_size("dev_1") // 2
    came, theirs = {}, {}
    block = {0: own, 1: other}
    for step in range(1, far + 1):
        for part in (0, 1) if step < far else (0,):
            block[part] = passed_on(block[part])
            came[step, part] = block[part]
        for part in (0, 1) if step < far else (0,):
            theirs[step, part] = swapped(came[step, part])
    return other, came, theirs


def scattered(far, own, other, kept, got):
    moving = {}
    for step in range(far, 0, -1):
        for part in (0, 1) if step < far else (1,):
            terms = [kept[step, part], got[step, part]]
            parcel = added(*terms, *moving.get(part, ())).astype(jnp.bfloat16)
            moving[part] = (passed_on(parcel),)
    leaving = added(other, *moving[0]).astype(jnp.bfloat16)
    return own, *moving[1], swapped(leaving)


def multiplied(pieces, gate, up, down, outs, ready):
    depth = gate.shape[0] // CUT_K
    span = down.shape[1] // CUT_N
    gate_v = up_v = None
    for k in range(CUT_K):
        cols = pl.ds(k * depth, depth)
        x = jnp.concatenate([p[:, cols] for p in pieces], 0)
        ready(k)
        g = jnp.dot(x, gate[cols, :], preferred_element_type=jnp.float32)
        u = jnp.dot(x, up[cols, :], preferred_element_type=jnp.float32)
        gate_v = g if gate_v is None else gate_v + g
        up_v = u if up_v is None else up_v + u
    act = (gate_v / (1.0 + jnp.exp(-gate_v)) * up_v).astype(jnp.bfloat16)
    ready(CUT_K)
    for n in range(CUT_N):
        cols = pl.ds(n * span, span)
        part = jnp.dot(act, down[:, cols], preferred_element_type=jnp.float32).astype(jnp.bfloat16)
        at = 0
        for out in outs:
            rows = out.shape[0]
            out[:, cols] = part[at : at + rows]
            at += rows


def early_kernel(count, *refs):
    pieces, (gate_far, up_far, down_far) = refs[:count], refs[count : count + 3]
    outs, (gate, up, down, sems) = refs[count + 3 : -4], refs[-4:]
    depth = gate.shape[0] // CUT_K
    copies = []
    for k in range(CUT_K):
        rows = pl.ds(k * depth, depth)
        copies.append(
            (
                pltpu.make_async_copy(gate_far.at[rows], gate.at[rows], sems.at[2 * k]),
                pltpu.make_async_copy(up_far.at[rows], up.at[rows], sems.at[2 * k + 1]),
            )
        )
    copies.append((pltpu.make_async_copy(down_far, down, sems.at[2 * CUT_K]),))
    for group in copies:
        for copy in group:
            copy.start()

    def ready(k):
        for copy in copies[k]:
            copy.wait()

    multiplied(pieces, gate, up, down, outs, ready)


def late_kernel(count, *refs):
    multiplied(refs[:count], *refs[count : count + 3], refs[count + 3 :], lambda k: None)


def product_cost(rows, width, hidden):
    return pl.CostEstimate(flops=6 * rows * width * hidden, bytes_accessed=6 * width * hidden, transcendentals=rows * hidden)


def early_products(pieces, weights, sizes):
    width, hidden = weights[0].shape
    vm = pl.BlockSpec(memory_space=pltpu.VMEM)
    far = pl.BlockSpec(memory_space=pltpu.HBM)
    outs = [jax.ShapeDtypeStruct((s, width), jnp.bfloat16) for s in sizes]
    held = [pltpu.VMEM(w.shape, w.dtype) for w in weights]
    return pl.pallas_call(
        functools.partial(early_kernel, len(pieces)),
        out_shape=outs + held,
        in_specs=[vm] * len(pieces) + [far] * 3,
        out_specs=[vm] * (len(sizes) + 3),
        scratch_shapes=[pltpu.SemaphoreType.DMA((2 * CUT_K + 1,))],
        compiler_params=pltpu.CompilerParams(vmem_limit_bytes=24 * 1024 * 1024),
        cost_estimate=product_cost(sum(sizes), width, hidden),
        name="early",
    )(*pieces, *[pltpu.with_memory_space_constraint(w, pltpu.HBM) for w in weights])


def late_products(pieces, weights, sizes):
    width, hidden = weights[0].shape
    vm = pl.BlockSpec(memory_space=pltpu.VMEM)
    return pl.pallas_call(
        functools.partial(late_kernel, len(pieces)),
        out_shape=[jax.ShapeDtypeStruct((s, width), jnp.bfloat16) for s in sizes],
        in_specs=[vm] * (len(pieces) + 3),
        out_specs=[vm] * len(sizes),
        compiler_params=pltpu.CompilerParams(vmem_limit_bytes=24 * 1024 * 1024),
        cost_estimate=product_cost(sum(sizes), width, hidden),
        name="late",
    )(*pieces, *weights)


def slots_of(ids_ref, reqs, top):
    named = [ids_ref[k, t] for t in range(reqs) for k in range(top)]
    slots = []
    for i, one in enumerate(named):
        slot = jnp.int32(0)
        for earlier in named[:i]:
            slot = slot + (earlier == one).astype(jnp.int32)
        slots.append(slot)
    return named, slots


def attend_kernel(me_ref, *refs):
    next_ref = refs[0]
    far_refs, (hidden_ref, leaving_ref, turned, mixed, packed), near_refs = refs[1:10], refs[10:15], refs[15:24]
    copies = [pltpu.make_async_copy(f, n, refs[24].at[i]) for i, (f, n) in enumerate(zip(far_refs, near_refs))]
    for copy in copies:
        copy.start()
    lens_ref, ids_ref, counts_ref, query_ref, own_ref, cache_ref, fresh_ref, tokens_ref, gain_ref = near_refs
    reqs, width = tokens_ref.shape
    length = cache_ref.shape[1]
    span = fresh_ref.shape[0]
    group = QH // KVH
    rows = group * reqs
    half = KVH * HD
    scale = 1.0 / math.sqrt(HD)
    me = me_ref[0]
    f32 = jnp.float32
    for copy in copies:
        copy.wait()
    for h in range(QH):
        turned[h * reqs : (h + 1) * reqs, :] = query_ref[:, h * HD : (h + 1) * HD].astype(f32)
    counts = counts_ref[...].astype(f32)
    places = lax.broadcasted_iota(jnp.int32, counts.shape, 1)
    before = jnp.sum(jnp.where(places < me, counts, 0.0), 1, keepdims=True)
    taken = jnp.sum(jnp.where(places == me, counts, 0.0), 1, keepdims=True)
    first = (before - (me * (span // BLOCK)).astype(f32)) * BLOCK
    last = first + taken * BLOCK
    row_w = lax.broadcasted_iota(jnp.int32, (rows, 2 * span), 0) % reqs
    col_w = lax.broadcasted_iota(jnp.int32, (rows, 2 * span), 1).astype(f32)
    live_w = (row_w == 0) & (col_w >= first) & (col_w < last)
    row_c = lax.broadcasted_iota(jnp.int32, (rows, reqs * length), 0) % reqs
    col_c = lax.broadcasted_iota(jnp.int32, (rows, reqs * length), 1)
    live_c = (row_c < 0)
    for r in range(reqs):
        live_c = live_c | ((row_c == r) & (col_c >= r * length) & (col_c < r * length + lens_ref[r]))
    for g in range(KVH):
        k_at = slice(g * HD, (g + 1) * HD)
        v_at = slice(half + g * HD, half + (g + 1) * HD)
        q32 = turned[g * rows : (g + 1) * rows, :]
        q = q32.astype(jnp.bfloat16)
        contract = (((1,), (1,)), ((), ()))
        key_c = cache_ref[:, :, k_at].reshape(reqs * length, HD)
        key_w = jnp.concatenate([fresh_ref[:, k_at], next_ref[:, k_at]], 0)
        key_o = jnp.concatenate([own_ref[:, k_at].astype(f32)] * group, 0)
        val_o = jnp.concatenate([own_ref[:, v_at].astype(f32)] * group, 0)
        s_c = lax.dot_general(q, key_c, contract, preferred_element_type=f32) * scale
        s_w = lax.dot_general(q, key_w, contract, preferred_element_type=f32) * scale
        s_o = jnp.sum(q32 * key_o, 1, keepdims=True) * scale
        s_c = jnp.where(live_c, s_c, NEG)
        s_w = jnp.where(live_w, s_w, NEG)
        top = jnp.maximum(jnp.maximum(jnp.max(s_c, 1, keepdims=True), jnp.max(s_w, 1, keepdims=True)), s_o)
        e_c = jnp.exp(s_c - top)
        e_w = jnp.exp(s_w - top)
        e_o = jnp.exp(s_o - top)
        total = jnp.sum(e_c, 1, keepdims=True) + jnp.sum(e_w, 1, keepdims=True) + e_o
        over = 1.0 / total
        p_c = (e_c * over).astype(jnp.bfloat16)
        p_w = (e_w * over).astype(jnp.bfloat16)
        p_o = (e_o * over).astype(jnp.bfloat16).astype(f32)
        val_c = cache_ref[:, :, v_at].reshape(reqs * length, HD)
        val_w = jnp.concatenate([fresh_ref[:, v_at], next_ref[:, v_at]], 0)
        out = jnp.dot(p_c, val_c, preferred_element_type=f32) + jnp.dot(p_w, val_w, preferred_element_type=f32)
        mixed[g * rows : (g + 1) * rows, :] = out + p_o * val_o
    squares = jnp.zeros((reqs, HD), f32)
    for h in range(QH):
        cols = slice(h * HD, (h + 1) * HD)
        hidden = tokens_ref[:, cols].astype(f32) + mixed[h * reqs : (h + 1) * reqs, :]
        hidden_ref[:, cols] = hidden
        squares = squares + hidden * hidden
    norm = lax.rsqrt(jnp.sum(squares, 1, keepdims=True) / width + EPS)
    normed = (hidden_ref[...] * norm * gain_ref[...]).astype(jnp.bfloat16).astype(f32)
    named, slots = slots_of(ids_ref, reqs, ids_ref.shape[0])
    tall = leaving_ref.shape[0] // EXPERTS
    padded = MOST + 1
    cell = lax.broadcasted_iota(jnp.int32, (EXPERTS * padded, 1), 0)
    gone = jnp.zeros((EXPERTS * padded, width), f32)
    for t in range(reqs):
        takes = jnp.zeros((EXPERTS * padded, 1), f32)
        for k in range(ids_ref.shape[0]):
            i = t * ids_ref.shape[0] + k
            takes = takes + (cell == named[i] * padded + slots[i]).astype(f32)
        gone = gone + takes * normed[t : t + 1, :]
    for j in range(width // HD):
        packed[pl.ds(j, EXPERTS * padded, stride=width // HD), :] = gone[:, j * HD : (j + 1) * HD]
    cut = width // HD
    for x in range(leaving_ref.shape[0]):
        at = x // tall * padded * cut
        leaving_ref[x, :, :] = packed[at : at + MOST * cut, :].astype(jnp.bfloat16)


def attended(me, lens, ids, counts, query, own, cache, fresh, following, tokens, gain, places):
    reqs, width = tokens.shape
    sm = pl.BlockSpec(memory_space=pltpu.SMEM)
    vm = pl.BlockSpec(memory_space=pltpu.VMEM)
    far = (lens, ids, counts, query, own, cache, fresh, tokens, gain)
    far = [pltpu.with_memory_space_constraint(x, pltpu.HBM) for x in far]
    return pl.pallas_call(
        attend_kernel,
        out_shape=[jax.ShapeDtypeStruct((reqs, width), jnp.float32), jax.ShapeDtypeStruct((places, MOST * width // HD, HD), jnp.bfloat16)],
        in_specs=[sm, vm] + [pl.BlockSpec(memory_space=pltpu.HBM)] * len(far),
        out_specs=[vm, vm],
        scratch_shapes=[
            pltpu.VMEM((QH * reqs, HD), jnp.float32),
            pltpu.VMEM((QH * reqs, HD), jnp.float32),
            pltpu.VMEM((EXPERTS * (MOST + 1) * width // HD, HD), jnp.float32),
            *(pltpu.SMEM(x.shape, x.dtype) for x in far[:2]),
            *(pltpu.VMEM(x.shape, x.dtype) for x in far[2:]),
            pltpu.SemaphoreType.DMA((len(far),)),
        ],
        compiler_params=pltpu.CompilerParams(vmem_limit_bytes=16 * 1024 * 1024),
        cost_estimate=pl.CostEstimate(flops=8 * reqs * width * 392, bytes_accessed=2 * 1024 * 1024, transcendentals=0),
        name="attended",
    )(me, following, *far)


def unpack_kernel(came_ref, block_ref, spread):
    rows, width = block_ref.shape
    spread[...] = came_ref[...].astype(jnp.float32).reshape(spread.shape)
    for j in range(width // HD):
        block_ref[:, j * HD : (j + 1) * HD] = spread[pl.ds(j, rows, stride=width // HD), :].astype(jnp.bfloat16)


def unpacked(came):
    places, packed, lanes = came.shape
    vm = pl.BlockSpec(memory_space=pltpu.VMEM)
    return pl.pallas_call(
        unpack_kernel,
        out_shape=jax.ShapeDtypeStruct((places * MOST, packed // MOST * lanes), jnp.bfloat16),
        in_specs=[vm],
        out_specs=vm,
        scratch_shapes=[pltpu.VMEM((places * packed, lanes), jnp.float32)],
        compiler_params=pltpu.CompilerParams(vmem_limit_bytes=8 * 1024 * 1024),
        name="unpacked",
    )(came)


def pack_kernel(first_ref, second_ref, third_ref, packed_ref, spread):
    rows, width = first_ref.shape
    f32 = jnp.float32
    for j in range(width // HD):
        cols = slice(j * HD, (j + 1) * HD)
        total = first_ref[:, cols].astype(f32) + second_ref[:, cols].astype(f32) + third_ref[:, cols].astype(f32)
        spread[pl.ds(j, rows, stride=width // HD), :] = total
    packed_ref[...] = spread[...].astype(jnp.bfloat16).reshape(packed_ref.shape)


def packed_sum(first, second, third, places):
    rows, width = first.shape
    vm = pl.BlockSpec(memory_space=pltpu.VMEM)
    return pl.pallas_call(
        pack_kernel,
        out_shape=jax.ShapeDtypeStruct((places, rows // places * width // HD, HD), jnp.bfloat16),
        in_specs=[vm] * 3,
        out_specs=vm,
        scratch_shapes=[pltpu.VMEM((rows * width // HD, HD), jnp.float32)],
        compiler_params=pltpu.CompilerParams(vmem_limit_bytes=8 * 1024 * 1024),
        name="packed_sum",
    )(first, second, third)


def mix_kernel(ids_ref, weights_ref, home_ref, hidden_ref, out_ref, spread):
    reqs, width = hidden_ref.shape
    tall = home_ref.shape[0] // EXPERTS
    cut = width // HD
    f32 = jnp.float32
    named, slots = slots_of(ids_ref, reqs, ids_ref.shape[0])
    sums = [jnp.zeros((cut, HD), f32) for _ in range(reqs)]
    for e in range(EXPERTS):
        for m in range(MOST):
            at = slice(m * cut, (m + 1) * cut)
            cell = home_ref[e * tall, at, :].astype(f32)
            for x in range(1, tall):
                cell = cell + home_ref[e * tall + x, at, :].astype(f32)
            for t in range(reqs):
                weight = jnp.float32(0.0)
                for k in range(ids_ref.shape[0]):
                    i = t * ids_ref.shape[0] + k
                    here = (named[i] == e) & (slots[i] == m)
                    weight = weight + jnp.where(here, weights_ref[k, t], 0.0)
                sums[t] = sums[t] + weight * cell
    for t in range(reqs):
        spread[t * cut : (t + 1) * cut, :] = sums[t]
    for j in range(cut):
        cols = slice(j * HD, (j + 1) * HD)
        moe = spread[pl.ds(j, reqs, stride=cut), :]
        out_ref[:, cols] = (hidden_ref[:, cols] + moe).astype(jnp.bfloat16)


def mixed_in(ids, weights, home, hidden):
    reqs, width = hidden.shape
    sm = pl.BlockSpec(memory_space=pltpu.SMEM)
    vm = pl.BlockSpec(memory_space=pltpu.VMEM)
    return pl.pallas_call(
        mix_kernel,
        out_shape=jax.ShapeDtypeStruct((reqs, width), jnp.bfloat16),
        in_specs=[sm, sm, vm, vm],
        out_specs=vm,
        scratch_shapes=[pltpu.VMEM((reqs * width // HD, HD), jnp.float32)],
        compiler_params=pltpu.CompilerParams(vmem_limit_bytes=8 * 1024 * 1024),
        name="mixed_in",
    )(ids, weights, home, hidden)


def layer(
    tokens,
    queries,
    token_kv,
    kv_cache,
    context_lengths,
    fresh_kv,
    block_counts,
    expert_ids,
    route_weights,
    norm_gain,
    w_gate,
    w_up,
    w_down,
):
    me = lax.axis_index(DEV)
    following = passed_along(fresh_kv, DEV, -1)
    rows_x = lax.axis_size("dev_0")
    me = lax.axis_index(DEV).astype(jnp.int32)[None]
    hidden_state, leaving = attended(
        me,
        context_lengths,
        expert_ids.T,
        block_counts[None],
        queries,
        token_kv,
        kv_cache,
        fresh_kv,
        following,
        tokens,
        norm_gain[None],
        rows_x,
    )
    own_block = unpacked(lax.all_to_all(leaving, "dev_0", 0, 0, tiled=True))
    other, came, theirs = gathered(own_block)
    far = lax.axis_size("dev_1") // 2
    each = rows_x * MOST
    near = range(far - 2, 0, -1)
    pieces = [own_block, other]
    for group in (theirs, came):
        for part in (0, 1):
            pieces += [group[step, part] for step in near]
    home_own, home_other, *groups, gate, up, down = early_products(
        pieces, (w_gate, w_up, w_down), [each, each] + [len(near) * each] * 4
    )
    last = far - 1
    pieces = [
        came[far, 0],
        theirs[last, 1],
        theirs[last, 0],
        theirs[far, 0],
        came[last, 1],
        came[last, 0],
    ]
    kept, got = {}, {}
    sent = [swapped(groups[2 + part]) for part in (0, 1)]
    for part in (0, 1):
        for i, step in enumerate(near):
            kept[step, part] = groups[part][i * each : (i + 1) * each]
            got[step, part] = sent[part][i * each : (i + 1) * each]
    kept[far, 1], kept[last, 1], kept[last, 0], *sent = late_products(
        pieces, (gate, up, down), [each, each, each, 2 * each, each]
    )
    sent = [swapped(x) for x in sent]
    got[far, 1], got[last, 1], got[last, 0] = sent[0][:each], sent[0][each:], sent[1]
    last_terms = scattered(far, home_own, home_other, kept, got)
    home = lax.all_to_all(packed_sum(*last_terms, rows_x), "dev_0", 0, 0, tiled=True)
    return mixed_in(expert_ids.T, route_weights.T, home, hidden_state)


def solution(mesh):
    split = Mesh(
        mesh.devices.reshape(mesh.shape["groups"], 8, 8, 2), ("groups", "dev_0", "dev_1", "dev_2")
    )
    return jax.shard_map(
        layer,
        mesh=split,
        in_specs=(
            P(GROUPS_DEV, None),
            P(GROUPS_DEV, None),
            P(GROUPS_DEV, None),
            P(GROUPS_DEV, None, None),
            P(GROUPS_DEV),
            P(GROUPS_DEV, None),
            P("groups"),
            P(GROUPS_DEV, None),
            P(GROUPS_DEV, None),
            P(),
            P(None, DEV),
            P(None, DEV),
            P(DEV, None),
        ),
        out_specs=P(GROUPS_DEV, None),
        check_vma=False,
    )
```

```python
import functools
import math

import jax
import jax.numpy as jnp
from jax import lax
from jax.experimental import pallas as pl
from jax.experimental.pallas import tpu as pltpu
from jax.sharding import Mesh
from jax.sharding import PartitionSpec as P


QH = 48
KVH = 8
HD = 128
EXPERTS = 4
BLOCK = 16
MOST = 3
DEV = ("dev_0", "dev_1", "dev_2")
GROUPS_DEV = ("groups", "dev_0", "dev_1", "dev_2")


EPS = 1e-05
NEG = -1e30

CUT_K = 8
CUT_N = 4


def passed_along(value, axis, steps):
    count = lax.axis_size(axis)
    leading, last = (max(0, -steps), min(count, count - steps))
    return lax.ppermute(value, axis, [(source, source + steps) for source in range(leading, last)])


def shifted(value, axis, steps):
    count = lax.axis_size(axis)
    return lax.ppermute(value, axis, [(place, (place + steps) % count) for place in range(count)])


def swapped(value):
    return shifted(value, "dev_2", 1)


def passed_on(value):
    chips, cores = lax.axis_size("dev_1"), lax.axis_size("dev_2")
    pairs = []
    for chip in range(chips):
        for core in range(cores):
            pairs.append((chip * cores + core, (chip + 1 - 2 * core) % chips * cores + core))
    return lax.ppermute(value, ("dev_1", "dev_2"), pairs)


def gathered(own):
    other = swapped(own)
    far = lax.axis_size("dev_1") // 2
    came, theirs = {}, {}
    block = {0: own, 1: other}
    for step in range(1, far + 1):
        for part in (0, 1) if step < far else (0,):
            block[part] = passed_on(block[part])
            came[step, part] = block[part]
        for part in (0, 1) if step < far else (0,):
            theirs[step, part] = swapped(came[step, part])
    return other, came, theirs


def hop_kernel(parts, *refs):
    out = refs[-1]
    total = None
    for ref, (row, col) in zip(refs, parts):
        term = ref[row : row + out.shape[0], col : col + out.shape[1]].astype(jnp.float32)
        total = term if total is None else total + term
    out[...] = total.astype(out.dtype)


def hop_sum(rows, cols, *terms):
    vm = pl.BlockSpec(memory_space=pltpu.VMEM)
    return pl.pallas_call(
        functools.partial(hop_kernel, [at for _, at in terms]),
        out_shape=jax.ShapeDtypeStruct((rows, cols), jnp.bfloat16),
        in_specs=[vm] * len(terms),
        out_specs=vm,
        compiler_params=pltpu.CompilerParams(vmem_limit_bytes=8 * 1024 * 1024),
        name="hop_sum",
    )(*[x for x, _ in terms])


def scattered(far, each, own, other, kept, got):
    half = own.shape[1] // 2
    moving = {}
    for step in range(far, 0, -1):
        for part in (0, 1) if step < far else (1,):
            for side in (0, 1):
                terms = [(x, (row, side * half)) for x, row in (kept[step, part], got[step, part])]
                if (part, side) in moving:
                    terms.append((moving[part, side], (0, 0)))
                parcel = hop_sum(each, half, *terms)
                moving[part, side] = passed_on(parcel)
    return own, moving[1, 0], moving[1, 1], swapped(two_sum(other, moving[0, 0], moving[0, 1]))


def two_kernel(whole_ref, left_ref, right_ref, out_ref):
    half = left_ref.shape[1]
    for side, ref in enumerate((left_ref, right_ref)):
        cols = slice(side * half, (side + 1) * half)
        out_ref[:, cols] = (whole_ref[:, cols].astype(jnp.float32) + ref[...].astype(jnp.float32)).astype(out_ref.dtype)


def two_sum(whole, left, right):
    vm = pl.BlockSpec(memory_space=pltpu.VMEM)
    return pl.pallas_call(
        two_kernel,
        out_shape=jax.ShapeDtypeStruct(whole.shape, whole.dtype),
        in_specs=[vm] * 3,
        out_specs=vm,
        compiler_params=pltpu.CompilerParams(vmem_limit_bytes=8 * 1024 * 1024),
        name="two_sum",
    )(whole, left, right)


def multiplied(pieces, gate, up, down, outs, ready):
    depth = gate.shape[0] // CUT_K
    span = down.shape[1] // CUT_N
    gate_v = up_v = None
    for k in range(CUT_K):
        cols = pl.ds(k * depth, depth)
        x = jnp.concatenate([p[:, cols] for p in pieces], 0)
        ready(k)
        g = jnp.dot(x, gate[cols, :], preferred_element_type=jnp.float32)
        u = jnp.dot(x, up[cols, :], preferred_element_type=jnp.float32)
        gate_v = g if gate_v is None else gate_v + g
        up_v = u if up_v is None else up_v + u
    act = (gate_v / (1.0 + jnp.exp(-gate_v)) * up_v).astype(jnp.bfloat16)
    ready(CUT_K)
    for n in range(CUT_N):
        cols = pl.ds(n * span, span)
        part = jnp.dot(act, down[:, cols], preferred_element_type=jnp.float32).astype(jnp.bfloat16)
        at = 0
        for out in outs:
            rows = out.shape[0]
            out[:, cols] = part[at : at + rows]
            at += rows


def early_kernel(count, *refs):
    pieces, (gate_far, up_far, down_far) = refs[:count], refs[count : count + 3]
    outs, (gate, up, down, sems) = refs[count + 3 : -4], refs[-4:]
    depth = gate.shape[0] // CUT_K
    copies = []
    for k in range(CUT_K):
        rows = pl.ds(k * depth, depth)
        copies.append(
            (
                pltpu.make_async_copy(gate_far.at[rows], gate.at[rows], sems.at[2 * k]),
                pltpu.make_async_copy(up_far.at[rows], up.at[rows], sems.at[2 * k + 1]),
            )
        )
    copies.append((pltpu.make_async_copy(down_far, down, sems.at[2 * CUT_K]),))
    for group in copies:
        for copy in group:
            copy.start()

    def ready(k):
        for copy in copies[k]:
            copy.wait()

    multiplied(pieces, gate, up, down, outs, ready)


def late_kernel(count, *refs):
    multiplied(refs[:count], *refs[count : count + 3], refs[count + 3 :], lambda k: None)


def product_cost(rows, width, hidden):
    return pl.CostEstimate(flops=6 * rows * width * hidden, bytes_accessed=6 * width * hidden, transcendentals=rows * hidden)


def early_products(pieces, weights, sizes):
    width, hidden = weights[0].shape
    vm = pl.BlockSpec(memory_space=pltpu.VMEM)
    far = pl.BlockSpec(memory_space=pltpu.HBM)
    outs = [jax.ShapeDtypeStruct((s, width), jnp.bfloat16) for s in sizes]
    held = [pltpu.VMEM(w.shape, w.dtype) for w in weights]
    return pl.pallas_call(
        functools.partial(early_kernel, len(pieces)),
        out_shape=outs + held,
        in_specs=[vm] * len(pieces) + [far] * 3,
        out_specs=[vm] * (len(sizes) + 3),
        scratch_shapes=[pltpu.SemaphoreType.DMA((2 * CUT_K + 1,))],
        compiler_params=pltpu.CompilerParams(vmem_limit_bytes=24 * 1024 * 1024),
        cost_estimate=product_cost(sum(sizes), width, hidden),
        name="early",
    )(*pieces, *[pltpu.with_memory_space_constraint(w, pltpu.HBM) for w in weights])


def late_products(pieces, weights, sizes):
    width, hidden = weights[0].shape
    vm = pl.BlockSpec(memory_space=pltpu.VMEM)
    return pl.pallas_call(
        functools.partial(late_kernel, len(pieces)),
        out_shape=[jax.ShapeDtypeStruct((s, width), jnp.bfloat16) for s in sizes],
        in_specs=[vm] * (len(pieces) + 3),
        out_specs=[vm] * len(sizes),
        compiler_params=pltpu.CompilerParams(vmem_limit_bytes=24 * 1024 * 1024),
        cost_estimate=product_cost(sum(sizes), width, hidden),
        name="late",
    )(*pieces, *weights)


def slots_of(ids_ref, reqs, top):
    named = [ids_ref[k, t] for t in range(reqs) for k in range(top)]
    slots = []
    for i, one in enumerate(named):
        slot = jnp.int32(0)
        for earlier in named[:i]:
            slot = slot + (earlier == one).astype(jnp.int32)
        slots.append(slot)
    return named, slots


def attend_kernel(me_ref, *refs):
    next_ref = refs[0]
    far_refs, (hidden_ref, leaving_ref, turned, mixed, packed), near_refs = refs[1:10], refs[10:15], refs[15:24]
    copies = [pltpu.make_async_copy(f, n, refs[24].at[i]) for i, (f, n) in enumerate(zip(far_refs, near_refs))]
    for copy in copies:
        copy.start()
    lens_ref, ids_ref, counts_ref, query_ref, own_ref, cache_ref, fresh_ref, tokens_ref, gain_ref = near_refs
    reqs, width = tokens_ref.shape
    length = cache_ref.shape[1]
    span = fresh_ref.shape[0]
    group = QH // KVH
    rows = group * reqs
    half = KVH * HD
    scale = 1.0 / math.sqrt(HD)
    me = me_ref[0]
    f32 = jnp.float32
    for copy in copies:
        copy.wait()
    for h in range(QH):
        turned[h * reqs : (h + 1) * reqs, :] = query_ref[:, h * HD : (h + 1) * HD].astype(f32)
    counts = counts_ref[...].astype(f32)
    places = lax.broadcasted_iota(jnp.int32, counts.shape, 1)
    before = jnp.sum(jnp.where(places < me, counts, 0.0), 1, keepdims=True)
    taken = jnp.sum(jnp.where(places == me, counts, 0.0), 1, keepdims=True)
    first = (before - (me * (span // BLOCK)).astype(f32)) * BLOCK
    last = first + taken * BLOCK
    row_w = lax.broadcasted_iota(jnp.int32, (rows, 2 * span), 0) % reqs
    col_w = lax.broadcasted_iota(jnp.int32, (rows, 2 * span), 1).astype(f32)
    live_w = (row_w == 0) & (col_w >= first) & (col_w < last)
    row_c = lax.broadcasted_iota(jnp.int32, (rows, reqs * length), 0) % reqs
    col_c = lax.broadcasted_iota(jnp.int32, (rows, reqs * length), 1)
    live_c = (row_c < 0)
    for r in range(reqs):
        live_c = live_c | ((row_c == r) & (col_c >= r * length) & (col_c < r * length + lens_ref[r]))
    for g in range(KVH):
        k_at = slice(g * HD, (g + 1) * HD)
        v_at = slice(half + g * HD, half + (g + 1) * HD)
        q32 = turned[g * rows : (g + 1) * rows, :]
        q = q32.astype(jnp.bfloat16)
        contract = (((1,), (1,)), ((), ()))
        key_c = cache_ref[:, :, k_at].reshape(reqs * length, HD)
        key_w = jnp.concatenate([fresh_ref[:, k_at], next_ref[:, k_at]], 0)
        key_o = jnp.concatenate([own_ref[:, k_at].astype(f32)] * group, 0)
        val_o = jnp.concatenate([own_ref[:, v_at].astype(f32)] * group, 0)
        s_c = lax.dot_general(q, key_c, contract, preferred_element_type=f32) * scale
        s_w = lax.dot_general(q, key_w, contract, preferred_element_type=f32) * scale
        s_o = jnp.sum(q32 * key_o, 1, keepdims=True) * scale
        s_c = jnp.where(live_c, s_c, NEG)
        s_w = jnp.where(live_w, s_w, NEG)
        top = jnp.maximum(jnp.maximum(jnp.max(s_c, 1, keepdims=True), jnp.max(s_w, 1, keepdims=True)), s_o)
        e_c = jnp.exp(s_c - top)
        e_w = jnp.exp(s_w - top)
        e_o = jnp.exp(s_o - top)
        total = jnp.sum(e_c, 1, keepdims=True) + jnp.sum(e_w, 1, keepdims=True) + e_o
        over = 1.0 / total
        p_c = (e_c * over).astype(jnp.bfloat16)
        p_w = (e_w * over).astype(jnp.bfloat16)
        p_o = (e_o * over).astype(jnp.bfloat16).astype(f32)
        val_c = cache_ref[:, :, v_at].reshape(reqs * length, HD)
        val_w = jnp.concatenate([fresh_ref[:, v_at], next_ref[:, v_at]], 0)
        out = jnp.dot(p_c, val_c, preferred_element_type=f32) + jnp.dot(p_w, val_w, preferred_element_type=f32)
        mixed[g * rows : (g + 1) * rows, :] = out + p_o * val_o
    squares = jnp.zeros((reqs, HD), f32)
    for h in range(QH):
        cols = slice(h * HD, (h + 1) * HD)
        hidden = tokens_ref[:, cols].astype(f32) + mixed[h * reqs : (h + 1) * reqs, :]
        hidden_ref[:, cols] = hidden
        squares = squares + hidden * hidden
    norm = lax.rsqrt(jnp.sum(squares, 1, keepdims=True) / width + EPS)
    normed = (hidden_ref[...] * norm * gain_ref[...]).astype(jnp.bfloat16).astype(f32)
    named, slots = slots_of(ids_ref, reqs, ids_ref.shape[0])
    tall = leaving_ref.shape[0] // EXPERTS
    padded = MOST + 1
    cell = lax.broadcasted_iota(jnp.int32, (EXPERTS * padded, 1), 0)
    gone = jnp.zeros((EXPERTS * padded, width), f32)
    for t in range(reqs):
        takes = jnp.zeros((EXPERTS * padded, 1), f32)
        for k in range(ids_ref.shape[0]):
            i = t * ids_ref.shape[0] + k
            takes = takes + (cell == named[i] * padded + slots[i]).astype(f32)
        gone = gone + takes * normed[t : t + 1, :]
    for j in range(width // HD):
        packed[pl.ds(j, EXPERTS * padded, stride=width // HD), :] = gone[:, j * HD : (j + 1) * HD]
    cut = width // HD
    for x in range(leaving_ref.shape[0]):
        at = x // tall * padded * cut
        leaving_ref[x, :, :] = packed[at : at + MOST * cut, :].astype(jnp.bfloat16)


def attended(me, lens, ids, counts, query, own, cache, fresh, following, tokens, gain, places):
    reqs, width = tokens.shape
    sm = pl.BlockSpec(memory_space=pltpu.SMEM)
    vm = pl.BlockSpec(memory_space=pltpu.VMEM)
    far = (lens, ids, counts, query, own, cache, fresh, tokens, gain)
    far = [pltpu.with_memory_space_constraint(x, pltpu.HBM) for x in far]
    return pl.pallas_call(
        attend_kernel,
        out_shape=[jax.ShapeDtypeStruct((reqs, width), jnp.float32), jax.ShapeDtypeStruct((places, MOST * width // HD, HD), jnp.bfloat16)],
        in_specs=[sm, vm] + [pl.BlockSpec(memory_space=pltpu.HBM)] * len(far),
        out_specs=[vm, vm],
        scratch_shapes=[
            pltpu.VMEM((QH * reqs, HD), jnp.float32),
            pltpu.VMEM((QH * reqs, HD), jnp.float32),
            pltpu.VMEM((EXPERTS * (MOST + 1) * width // HD, HD), jnp.float32),
            *(pltpu.SMEM(x.shape, x.dtype) for x in far[:2]),
            *(pltpu.VMEM(x.shape, x.dtype) for x in far[2:]),
            pltpu.SemaphoreType.DMA((len(far),)),
        ],
        compiler_params=pltpu.CompilerParams(vmem_limit_bytes=16 * 1024 * 1024),
        cost_estimate=pl.CostEstimate(flops=8 * reqs * width * 392, bytes_accessed=2 * 1024 * 1024, transcendentals=0),
        name="attended",
    )(me, following, *far)


def unpack_kernel(came_ref, block_ref, spread):
    rows, width = block_ref.shape
    spread[...] = came_ref[...].astype(jnp.float32).reshape(spread.shape)
    for j in range(width // HD):
        block_ref[:, j * HD : (j + 1) * HD] = spread[pl.ds(j, rows, stride=width // HD), :].astype(jnp.bfloat16)


def unpacked(came):
    places, packed, lanes = came.shape
    vm = pl.BlockSpec(memory_space=pltpu.VMEM)
    return pl.pallas_call(
        unpack_kernel,
        out_shape=jax.ShapeDtypeStruct((places * MOST, packed // MOST * lanes), jnp.bfloat16),
        in_specs=[vm],
        out_specs=vm,
        scratch_shapes=[pltpu.VMEM((places * packed, lanes), jnp.float32)],
        compiler_params=pltpu.CompilerParams(vmem_limit_bytes=8 * 1024 * 1024),
        name="unpacked",
    )(came)


def pack_kernel(first_ref, left_ref, right_ref, third_ref, packed_ref, spread):
    rows, width = first_ref.shape
    f32 = jnp.float32
    half = left_ref.shape[1]
    for j in range(width // HD):
        cols = slice(j * HD, (j + 1) * HD)
        side = left_ref if j * HD < half else right_ref
        came = side[:, j * HD % half : j * HD % half + HD].astype(f32)
        total = first_ref[:, cols].astype(f32) + came + third_ref[:, cols].astype(f32)
        spread[pl.ds(j, rows, stride=width // HD), :] = total
    packed_ref[...] = spread[...].astype(jnp.bfloat16).reshape(packed_ref.shape)


def packed_sum(first, left, right, third, places):
    rows, width = first.shape
    vm = pl.BlockSpec(memory_space=pltpu.VMEM)
    return pl.pallas_call(
        pack_kernel,
        out_shape=jax.ShapeDtypeStruct((places, rows // places * width // HD, HD), jnp.bfloat16),
        in_specs=[vm] * 4,
        out_specs=vm,
        scratch_shapes=[pltpu.VMEM((rows * width // HD, HD), jnp.float32)],
        compiler_params=pltpu.CompilerParams(vmem_limit_bytes=8 * 1024 * 1024),
        name="packed_sum",
    )(first, left, right, third)


def mix_kernel(ids_ref, weights_ref, home_ref, hidden_ref, out_ref, spread):
    reqs, width = hidden_ref.shape
    tall = home_ref.shape[0] // EXPERTS
    cut = width // HD
    f32 = jnp.float32
    named, slots = slots_of(ids_ref, reqs, ids_ref.shape[0])
    sums = [jnp.zeros((cut, HD), f32) for _ in range(reqs)]
    for e in range(EXPERTS):
        for m in range(MOST):
            at = slice(m * cut, (m + 1) * cut)
            cell = home_ref[e * tall, at, :].astype(f32)
            for x in range(1, tall):
                cell = cell + home_ref[e * tall + x, at, :].astype(f32)
            for t in range(reqs):
                weight = jnp.float32(0.0)
                for k in range(ids_ref.shape[0]):
                    i = t * ids_ref.shape[0] + k
                    here = (named[i] == e) & (slots[i] == m)
                    weight = weight + jnp.where(here, weights_ref[k, t], 0.0)
                sums[t] = sums[t] + weight * cell
    for t in range(reqs):
        spread[t * cut : (t + 1) * cut, :] = sums[t]
    for j in range(cut):
        cols = slice(j * HD, (j + 1) * HD)
        moe = spread[pl.ds(j, reqs, stride=cut), :]
        out_ref[:, cols] = (hidden_ref[:, cols] + moe).astype(jnp.bfloat16)


def mixed_in(ids, weights, home, hidden):
    reqs, width = hidden.shape
    sm = pl.BlockSpec(memory_space=pltpu.SMEM)
    vm = pl.BlockSpec(memory_space=pltpu.VMEM)
    return pl.pallas_call(
        mix_kernel,
        out_shape=jax.ShapeDtypeStruct((reqs, width), jnp.bfloat16),
        in_specs=[sm, sm, vm, vm],
        out_specs=vm,
        scratch_shapes=[pltpu.VMEM((reqs * width // HD, HD), jnp.float32)],
        compiler_params=pltpu.CompilerParams(vmem_limit_bytes=8 * 1024 * 1024),
        name="mixed_in",
    )(ids, weights, home, hidden)


def layer(
    tokens,
    queries,
    token_kv,
    kv_cache,
    context_lengths,
    fresh_kv,
    block_counts,
    expert_ids,
    route_weights,
    norm_gain,
    w_gate,
    w_up,
    w_down,
):
    me = lax.axis_index(DEV)
    following = passed_along(fresh_kv, DEV, -1)
    rows_x = lax.axis_size("dev_0")
    me = lax.axis_index(DEV).astype(jnp.int32)[None]
    hidden_state, leaving = attended(
        me,
        context_lengths,
        expert_ids.T,
        block_counts[None],
        queries,
        token_kv,
        kv_cache,
        fresh_kv,
        following,
        tokens,
        norm_gain[None],
        rows_x,
    )
    own_block = unpacked(lax.all_to_all(leaving, "dev_0", 0, 0, tiled=True))
    other, came, theirs = gathered(own_block)
    far = lax.axis_size("dev_1") // 2
    each = rows_x * MOST
    near = range(far - 2, 0, -1)
    pieces = [own_block, other]
    for group in (theirs, came):
        for part in (0, 1):
            pieces += [group[step, part] for step in near]
    home_own, home_other, *groups, gate, up, down = early_products(
        pieces, (w_gate, w_up, w_down), [each, each] + [len(near) * each] * 4
    )
    last = far - 1
    pieces = [
        came[far, 0],
        theirs[last, 1],
        theirs[last, 0],
        theirs[far, 0],
        came[last, 1],
        came[last, 0],
    ]
    kept, got = {}, {}
    sent = [swapped(groups[2 + part]) for part in (0, 1)]
    for part in (0, 1):
        for i, step in enumerate(near):
            kept[step, part] = (groups[part], i * each)
            got[step, part] = (sent[part], i * each)
    *stay, sent_1, sent_0 = late_products(pieces, (gate, up, down), [each, each, each, 2 * each, each])
    kept[far, 1], kept[last, 1], kept[last, 0] = [(x, 0) for x in stay]
    first = swapped(sent_1)
    got[far, 1], got[last, 1], got[last, 0] = (first, 0), (first, each), (swapped(sent_0), 0)
    last_terms = scattered(far, each, home_own, home_other, kept, got)
    home = lax.all_to_all(packed_sum(*last_terms, rows_x), "dev_0", 0, 0, tiled=True)
    return mixed_in(expert_ids.T, route_weights.T, home, hidden_state)


def solution(mesh):
    split = Mesh(
        mesh.devices.reshape(mesh.shape["groups"], 8, 8, 2), ("groups", "dev_0", "dev_1", "dev_2")
    )
    return jax.shard_map(
        layer,
        mesh=split,
        in_specs=(
            P(GROUPS_DEV, None),
            P(GROUPS_DEV, None),
            P(GROUPS_DEV, None),
            P(GROUPS_DEV, None, None),
            P(GROUPS_DEV),
            P(GROUPS_DEV, None),
            P("groups"),
            P(GROUPS_DEV, None),
            P(GROUPS_DEV, None),
            P(),
            P(None, DEV),
            P(None, DEV),
            P(DEV, None),
        ),
        out_specs=P(GROUPS_DEV, None),
        check_vma=False,
    )
```

```python
import functools
import math

import jax
import jax.numpy as jnp
from jax import lax
from jax.experimental import pallas as pl
from jax.experimental.pallas import tpu as pltpu
from jax.sharding import Mesh
from jax.sharding import PartitionSpec as P


QH = 48
KVH = 8
HD = 128
EXPERTS = 4
BLOCK = 16
MOST = 3
DEV = ("dev_0", "dev_1", "dev_2")
GROUPS_DEV = ("groups", "dev_0", "dev_1", "dev_2")


EPS = 1e-05
NEG = -1e30

CUT_K = 8
CUT_N = 4


def passed_along(value, axis, steps):
    count = lax.axis_size(axis)
    leading, last = (max(0, -steps), min(count, count - steps))
    return lax.ppermute(value, axis, [(source, source + steps) for source in range(leading, last)])


def shifted(value, axis, steps):
    count = lax.axis_size(axis)
    return lax.ppermute(value, axis, [(place, (place + steps) % count) for place in range(count)])


def swapped(value):
    return shifted(value, "dev_2", 1)


def passed_on(value):
    chips, cores = lax.axis_size("dev_1"), lax.axis_size("dev_2")
    pairs = []
    for chip in range(chips):
        for core in range(cores):
            pairs.append((chip * cores + core, (chip + 1 - 2 * core) % chips * cores + core))
    return lax.ppermute(value, ("dev_1", "dev_2"), pairs)


def gathered(own):
    other = swapped(own)
    far = lax.axis_size("dev_1") // 2
    came, theirs = {}, {}
    block = {0: own, 1: other}
    for step in range(1, far + 1):
        for part in (0, 1) if step < far else (0,):
            block[part] = passed_on(block[part])
            came[step, part] = block[part]
        for part in (0, 1) if step < far else (0,):
            theirs[step, part] = swapped(came[step, part])
    return other, came, theirs


def hop_kernel(parts, *refs):
    out = refs[-1]
    total = None
    for ref, (row, col) in zip(refs, parts):
        term = ref[row : row + out.shape[0], col : col + out.shape[1]].astype(jnp.float32)
        total = term if total is None else total + term
    out[...] = total.astype(out.dtype)


def hop_sum(rows, cols, *terms):
    vm = pl.BlockSpec(memory_space=pltpu.VMEM)
    return pl.pallas_call(
        functools.partial(hop_kernel, [at for _, at in terms]),
        out_shape=jax.ShapeDtypeStruct((rows, cols), jnp.bfloat16),
        in_specs=[vm] * len(terms),
        out_specs=vm,
        compiler_params=pltpu.CompilerParams(vmem_limit_bytes=8 * 1024 * 1024),
        name="hop_sum",
    )(*[x for x, _ in terms])


def scattered(far, each, own, other, kept, got):
    half = own.shape[1] // 2
    moving = {}
    for step in range(far, 0, -1):
        for part in (0, 1) if step < far else (1,):
            for side in (0, 1):
                terms = [(x, (row, side * half)) for x, row in (kept[step, part], got[step, part])]
                if (part, side) in moving:
                    terms.append((moving[part, side], (0, 0)))
                parcel = hop_sum(each, half, *terms)
                moving[part, side] = passed_on(parcel)
    return own, moving[1, 0], moving[1, 1], swapped(two_sum(other, moving[0, 0], moving[0, 1]))


def two_kernel(whole_ref, left_ref, right_ref, out_ref):
    half = left_ref.shape[1]
    for side, ref in enumerate((left_ref, right_ref)):
        cols = slice(side * half, (side + 1) * half)
        out_ref[:, cols] = (whole_ref[:, cols].astype(jnp.float32) + ref[...].astype(jnp.float32)).astype(out_ref.dtype)


def two_sum(whole, left, right):
    vm = pl.BlockSpec(memory_space=pltpu.VMEM)
    return pl.pallas_call(
        two_kernel,
        out_shape=jax.ShapeDtypeStruct(whole.shape, whole.dtype),
        in_specs=[vm] * 3,
        out_specs=vm,
        compiler_params=pltpu.CompilerParams(vmem_limit_bytes=8 * 1024 * 1024),
        name="two_sum",
    )(whole, left, right)


def multiplied(pieces, gate, up, down, outs, ready):
    depth = gate.shape[0] // CUT_K
    span = down.shape[1] // CUT_N
    gate_v = up_v = None
    for k in range(CUT_K):
        cols = pl.ds(k * depth, depth)
        x = jnp.concatenate([p[:, cols] for p in pieces], 0)
        ready(k)
        g = jnp.dot(x, gate[cols, :], preferred_element_type=jnp.float32)
        u = jnp.dot(x, up[cols, :], preferred_element_type=jnp.float32)
        gate_v = g if gate_v is None else gate_v + g
        up_v = u if up_v is None else up_v + u
    act = (gate_v / (1.0 + jnp.exp(-gate_v)) * up_v).astype(jnp.bfloat16)
    ready(CUT_K)
    for n in range(CUT_N):
        cols = pl.ds(n * span, span)
        part = jnp.dot(act, down[:, cols], preferred_element_type=jnp.float32).astype(jnp.bfloat16)
        at = 0
        for out in outs:
            rows = out.shape[0]
            out[:, cols] = part[at : at + rows]
            at += rows


def early_kernel(count, *refs):
    pieces, (gate_far, up_far, down_far) = refs[:count], refs[count : count + 3]
    outs, (gate, up, down, sems) = refs[count + 3 : -4], refs[-4:]
    depth = gate.shape[0] // CUT_K
    copies = []
    for k in range(CUT_K):
        rows = pl.ds(k * depth, depth)
        copies.append(
            (
                pltpu.make_async_copy(gate_far.at[rows], gate.at[rows], sems.at[2 * k]),
                pltpu.make_async_copy(up_far.at[rows], up.at[rows], sems.at[2 * k + 1]),
            )
        )
    copies.append((pltpu.make_async_copy(down_far, down, sems.at[2 * CUT_K]),))
    for group in copies:
        for copy in group:
            copy.start()

    def ready(k):
        for copy in copies[k]:
            copy.wait()

    multiplied(pieces, gate, up, down, outs, ready)


def late_kernel(count, *refs):
    multiplied(refs[:count], *refs[count : count + 3], refs[count + 3 :], lambda k: None)


def product_cost(rows, width, hidden):
    return pl.CostEstimate(flops=6 * rows * width * hidden, bytes_accessed=6 * width * hidden, transcendentals=rows * hidden)


def early_products(pieces, weights, sizes):
    width, hidden = weights[0].shape
    vm = pl.BlockSpec(memory_space=pltpu.VMEM)
    far = pl.BlockSpec(memory_space=pltpu.HBM)
    outs = [jax.ShapeDtypeStruct((s, width), jnp.bfloat16) for s in sizes]
    held = [pltpu.VMEM(w.shape, w.dtype) for w in weights]
    return pl.pallas_call(
        functools.partial(early_kernel, len(pieces)),
        out_shape=outs + held,
        in_specs=[vm] * len(pieces) + [far] * 3,
        out_specs=[vm] * (len(sizes) + 3),
        scratch_shapes=[pltpu.SemaphoreType.DMA((2 * CUT_K + 1,))],
        compiler_params=pltpu.CompilerParams(vmem_limit_bytes=24 * 1024 * 1024),
        cost_estimate=product_cost(sum(sizes), width, hidden),
        name="early",
    )(*pieces, *[pltpu.with_memory_space_constraint(w, pltpu.HBM) for w in weights])


def late_products(pieces, weights, sizes):
    width, hidden = weights[0].shape
    vm = pl.BlockSpec(memory_space=pltpu.VMEM)
    return pl.pallas_call(
        functools.partial(late_kernel, len(pieces)),
        out_shape=[jax.ShapeDtypeStruct((s, width), jnp.bfloat16) for s in sizes],
        in_specs=[vm] * (len(pieces) + 3),
        out_specs=[vm] * len(sizes),
        compiler_params=pltpu.CompilerParams(vmem_limit_bytes=24 * 1024 * 1024),
        cost_estimate=product_cost(sum(sizes), width, hidden),
        name="late",
    )(*pieces, *weights)


def slots_of(ids_ref, reqs, top):
    named = [ids_ref[k, t] for t in range(reqs) for k in range(top)]
    slots = []
    for i, one in enumerate(named):
        slot = jnp.int32(0)
        for earlier in named[:i]:
            slot = slot + (earlier == one).astype(jnp.int32)
        slots.append(slot)
    return named, slots


def attend_kernel(me_ref, *refs):
    next_ref = refs[0]
    far_refs, (hidden_ref, leaving_ref, turned, mixed, packed), near_refs = refs[1:10], refs[10:15], refs[15:24]
    copies = [pltpu.make_async_copy(f, n, refs[24].at[i]) for i, (f, n) in enumerate(zip(far_refs, near_refs))]
    for copy in copies:
        copy.start()
    lens_ref, ids_ref, counts_ref, query_ref, own_ref, cache_ref, fresh_ref, tokens_ref, gain_ref = near_refs
    reqs, width = tokens_ref.shape
    length = cache_ref.shape[1]
    span = fresh_ref.shape[0]
    group = QH // KVH
    rows = group * reqs
    half = KVH * HD
    scale = 1.0 / math.sqrt(HD)
    me = me_ref[0]
    f32 = jnp.float32
    for copy in copies:
        copy.wait()
    for h in range(QH):
        turned[h * reqs : (h + 1) * reqs, :] = query_ref[:, h * HD : (h + 1) * HD].astype(f32)
    counts = counts_ref[...].astype(f32)
    places = lax.broadcasted_iota(jnp.int32, counts.shape, 1)
    before = jnp.sum(jnp.where(places < me, counts, 0.0), 1, keepdims=True)
    taken = jnp.sum(jnp.where(places == me, counts, 0.0), 1, keepdims=True)
    first = (before - (me * (span // BLOCK)).astype(f32)) * BLOCK
    last = first + taken * BLOCK
    row_w = lax.broadcasted_iota(jnp.int32, (rows, 2 * span), 0) % reqs
    col_w = lax.broadcasted_iota(jnp.int32, (rows, 2 * span), 1).astype(f32)
    live_w = (row_w == 0) & (col_w >= first) & (col_w < last)
    row_c = lax.broadcasted_iota(jnp.int32, (rows, reqs * length), 0) % reqs
    col_c = lax.broadcasted_iota(jnp.int32, (rows, reqs * length), 1)
    live_c = (row_c < 0)
    for r in range(reqs):
        live_c = live_c | ((row_c == r) & (col_c >= r * length) & (col_c < r * length + lens_ref[r]))
    for g in range(KVH):
        k_at = slice(g * HD, (g + 1) * HD)
        v_at = slice(half + g * HD, half + (g + 1) * HD)
        q32 = turned[g * rows : (g + 1) * rows, :]
        q = q32.astype(jnp.bfloat16)
        contract = (((1,), (1,)), ((), ()))
        key_c = cache_ref[:, :, k_at].reshape(reqs * length, HD)
        key_w = jnp.concatenate([fresh_ref[:, k_at], next_ref[:, k_at]], 0)
        key_o = jnp.concatenate([own_ref[:, k_at].astype(f32)] * group, 0)
        val_o = jnp.concatenate([own_ref[:, v_at].astype(f32)] * group, 0)
        s_c = lax.dot_general(q, key_c, contract, preferred_element_type=f32) * scale
        s_w = lax.dot_general(q, key_w, contract, preferred_element_type=f32) * scale
        s_o = jnp.sum(q32 * key_o, 1, keepdims=True) * scale
        s_c = jnp.where(live_c, s_c, NEG)
        s_w = jnp.where(live_w, s_w, NEG)
        top = jnp.maximum(jnp.maximum(jnp.max(s_c, 1, keepdims=True), jnp.max(s_w, 1, keepdims=True)), s_o)
        e_c = jnp.exp(s_c - top)
        e_w = jnp.exp(s_w - top)
        e_o = jnp.exp(s_o - top)
        total = jnp.sum(e_c, 1, keepdims=True) + jnp.sum(e_w, 1, keepdims=True) + e_o
        over = 1.0 / total
        p_c = (e_c * over).astype(jnp.bfloat16)
        p_w = (e_w * over).astype(jnp.bfloat16)
        p_o = (e_o * over).astype(jnp.bfloat16).astype(f32)
        val_c = cache_ref[:, :, v_at].reshape(reqs * length, HD)
        val_w = jnp.concatenate([fresh_ref[:, v_at], next_ref[:, v_at]], 0)
        out = jnp.dot(p_c, val_c, preferred_element_type=f32) + jnp.dot(p_w, val_w, preferred_element_type=f32)
        mixed[g * rows : (g + 1) * rows, :] = out + p_o * val_o
    squares = jnp.zeros((reqs, HD), f32)
    for h in range(QH):
        cols = slice(h * HD, (h + 1) * HD)
        hidden = tokens_ref[:, cols].astype(f32) + mixed[h * reqs : (h + 1) * reqs, :]
        hidden_ref[:, cols] = hidden
        squares = squares + hidden * hidden
    norm = lax.rsqrt(jnp.sum(squares, 1, keepdims=True) / width + EPS)
    normed = (hidden_ref[...] * norm * gain_ref[...]).astype(jnp.bfloat16).astype(f32)
    named, slots = slots_of(ids_ref, reqs, ids_ref.shape[0])
    tall = leaving_ref.shape[0] // EXPERTS
    padded = MOST + 1
    cell = lax.broadcasted_iota(jnp.int32, (EXPERTS * padded, 1), 0)
    gone = jnp.zeros((EXPERTS * padded, width), f32)
    for t in range(reqs):
        takes = jnp.zeros((EXPERTS * padded, 1), f32)
        for k in range(ids_ref.shape[0]):
            i = t * ids_ref.shape[0] + k
            takes = takes + (cell == named[i] * padded + slots[i]).astype(f32)
        gone = gone + takes * normed[t : t + 1, :]
    for j in range(width // HD):
        packed[pl.ds(j, EXPERTS * padded, stride=width // HD), :] = gone[:, j * HD : (j + 1) * HD]
    cut = width // HD
    for x in range(leaving_ref.shape[0]):
        at = x // tall * padded * cut
        leaving_ref[x, :, :] = packed[at : at + MOST * cut, :].astype(jnp.bfloat16)


def attended(me, lens, ids, counts, query, own, cache, fresh, following, tokens, gain, places):
    reqs, width = tokens.shape
    sm = pl.BlockSpec(memory_space=pltpu.SMEM)
    vm = pl.BlockSpec(memory_space=pltpu.VMEM)
    far = (lens, ids, counts, query, own, cache, fresh, tokens, gain)
    far = [pltpu.with_memory_space_constraint(x, pltpu.HBM) for x in far]
    return pl.pallas_call(
        attend_kernel,
        out_shape=[jax.ShapeDtypeStruct((reqs, width), jnp.float32), jax.ShapeDtypeStruct((places, MOST * width // HD, HD), jnp.bfloat16)],
        in_specs=[sm, vm] + [pl.BlockSpec(memory_space=pltpu.HBM)] * len(far),
        out_specs=[vm, vm],
        scratch_shapes=[
            pltpu.VMEM((QH * reqs, HD), jnp.float32),
            pltpu.VMEM((QH * reqs, HD), jnp.float32),
            pltpu.VMEM((EXPERTS * (MOST + 1) * width // HD, HD), jnp.float32),
            *(pltpu.SMEM(x.shape, x.dtype) for x in far[:2]),
            *(pltpu.VMEM(x.shape, x.dtype) for x in far[2:]),
            pltpu.SemaphoreType.DMA((len(far),)),
        ],
        compiler_params=pltpu.CompilerParams(vmem_limit_bytes=16 * 1024 * 1024),
        cost_estimate=pl.CostEstimate(flops=8 * reqs * width * 392, bytes_accessed=2 * 1024 * 1024, transcendentals=0),
        name="attended",
    )(me, following, *far)


def unpack_kernel(came_ref, block_ref, spread):
    rows, width = block_ref.shape
    spread[...] = came_ref[...].astype(jnp.float32).reshape(spread.shape)
    for j in range(width // HD):
        block_ref[:, j * HD : (j + 1) * HD] = spread[pl.ds(j, rows, stride=width // HD), :].astype(jnp.bfloat16)


def unpacked(came):
    places, packed, lanes = came.shape
    vm = pl.BlockSpec(memory_space=pltpu.VMEM)
    return pl.pallas_call(
        unpack_kernel,
        out_shape=jax.ShapeDtypeStruct((places * MOST, packed // MOST * lanes), jnp.bfloat16),
        in_specs=[vm],
        out_specs=vm,
        scratch_shapes=[pltpu.VMEM((places * packed, lanes), jnp.float32)],
        compiler_params=pltpu.CompilerParams(vmem_limit_bytes=8 * 1024 * 1024),
        name="unpacked",
    )(came)


def pack_kernel(first_ref, left_ref, right_ref, third_ref, packed_ref, spread):
    rows, width = first_ref.shape
    f32 = jnp.float32
    half = left_ref.shape[1]
    for j in range(width // HD):
        cols = slice(j * HD, (j + 1) * HD)
        side = left_ref if j * HD < half else right_ref
        came = side[:, j * HD % half : j * HD % half + HD].astype(f32)
        total = first_ref[:, cols].astype(f32) + came + third_ref[:, cols].astype(f32)
        spread[pl.ds(j, rows, stride=width // HD), :] = total
    packed_ref[...] = spread[...].astype(jnp.bfloat16).reshape(packed_ref.shape)


def packed_sum(first, left, right, third, places):
    rows, width = first.shape
    vm = pl.BlockSpec(memory_space=pltpu.VMEM)
    return pl.pallas_call(
        pack_kernel,
        out_shape=jax.ShapeDtypeStruct((places, rows // places * width // HD, HD), jnp.bfloat16),
        in_specs=[vm] * 4,
        out_specs=vm,
        scratch_shapes=[pltpu.VMEM((rows * width // HD, HD), jnp.float32)],
        compiler_params=pltpu.CompilerParams(vmem_limit_bytes=8 * 1024 * 1024),
        name="packed_sum",
    )(first, left, right, third)


def mix_kernel(ids_ref, weights_ref, home_ref, hidden_ref, out_ref, spread):
    reqs, width = hidden_ref.shape
    tall = home_ref.shape[0] // EXPERTS
    cut = width // HD
    f32 = jnp.float32
    named, slots = slots_of(ids_ref, reqs, ids_ref.shape[0])
    sums = [jnp.zeros((cut, HD), f32) for _ in range(reqs)]
    for e in range(EXPERTS):
        for m in range(MOST):
            at = slice(m * cut, (m + 1) * cut)
            cell = home_ref[e * tall, at, :].astype(f32)
            for x in range(1, tall):
                cell = cell + home_ref[e * tall + x, at, :].astype(f32)
            for t in range(reqs):
                weight = jnp.float32(0.0)
                for k in range(ids_ref.shape[0]):
                    i = t * ids_ref.shape[0] + k
                    here = (named[i] == e) & (slots[i] == m)
                    weight = weight + jnp.where(here, weights_ref[k, t], 0.0)
                sums[t] = sums[t] + weight * cell
    for t in range(reqs):
        spread[t * cut : (t + 1) * cut, :] = sums[t]
    for j in range(cut):
        cols = slice(j * HD, (j + 1) * HD)
        moe = spread[pl.ds(j, reqs, stride=cut), :]
        out_ref[:, cols] = (hidden_ref[:, cols] + moe).astype(jnp.bfloat16)


def mixed_in(ids, weights, home, hidden):
    reqs, width = hidden.shape
    sm = pl.BlockSpec(memory_space=pltpu.SMEM)
    vm = pl.BlockSpec(memory_space=pltpu.VMEM)
    return pl.pallas_call(
        mix_kernel,
        out_shape=jax.ShapeDtypeStruct((reqs, width), jnp.bfloat16),
        in_specs=[sm, sm, vm, vm],
        out_specs=vm,
        scratch_shapes=[pltpu.VMEM((reqs * width // HD, HD), jnp.float32)],
        compiler_params=pltpu.CompilerParams(vmem_limit_bytes=8 * 1024 * 1024),
        name="mixed_in",
    )(ids, weights, home, hidden)


def layer(
    tokens,
    queries,
    token_kv,
    kv_cache,
    context_lengths,
    fresh_kv,
    block_counts,
    expert_ids,
    route_weights,
    norm_gain,
    w_gate,
    w_up,
    w_down,
):
    me = lax.axis_index(DEV)
    following = passed_along(fresh_kv, DEV, -1)
    rows_x = lax.axis_size("dev_0")
    me = lax.axis_index(DEV).astype(jnp.int32)[None]
    hidden_state, leaving = attended(
        me,
        context_lengths,
        expert_ids.T,
        block_counts[None],
        queries,
        token_kv,
        kv_cache,
        fresh_kv,
        following,
        tokens,
        norm_gain[None],
        rows_x,
    )
    own_block = unpacked(lax.all_to_all(leaving, "dev_0", 0, 0, tiled=True))
    other, came, theirs = gathered(own_block)
    far = lax.axis_size("dev_1") // 2
    each = rows_x * MOST
    near = range(far - 2, 0, -1)
    pieces = [own_block, other]
    for group in (theirs, came):
        for part in (0, 1):
            pieces += [group[step, part] for step in near]
    home_own, home_other, *groups, gate, up, down = early_products(
        pieces, (w_gate, w_up, w_down), [each, each] + [len(near) * each] * 4
    )
    last = far - 1
    kept, got = {}, {}
    near_sent = [swapped(groups[2 + part]) for part in (0, 1)]
    for part in (0, 1):
        for i, step in enumerate(near):
            kept[step, part] = (groups[part], i * each)
            got[step, part] = (near_sent[part], i * each)
    pieces = [theirs[last, 0], theirs[last, 1], came[last, 0], came[last, 1]]
    results = late_products(pieces, (gate, up, down), [each] * 4)
    for part in (0, 1):
        kept[last, part] = (results[part], 0)
        got[last, part] = (swapped(results[2 + part]), 0)
    results = late_products([came[far, 0], theirs[far, 0]], (gate, up, down), [each] * 2)
    kept[far, 1] = (results[0], 0)
    got[far, 1] = (swapped(results[1]), 0)
    last_terms = scattered(far, each, home_own, home_other, kept, got)
    home = lax.all_to_all(packed_sum(*last_terms, rows_x), "dev_0", 0, 0, tiled=True)
    return mixed_in(expert_ids.T, route_weights.T, home, hidden_state)


def solution(mesh):
    split = Mesh(
        mesh.devices.reshape(mesh.shape["groups"], 8, 8, 2), ("groups", "dev_0", "dev_1", "dev_2")
    )
    return jax.shard_map(
        layer,
        mesh=split,
        in_specs=(
            P(GROUPS_DEV, None),
            P(GROUPS_DEV, None),
            P(GROUPS_DEV, None),
            P(GROUPS_DEV, None, None),
            P(GROUPS_DEV),
            P(GROUPS_DEV, None),
            P("groups"),
            P(GROUPS_DEV, None),
            P(GROUPS_DEV, None),
            P(),
            P(None, DEV),
            P(None, DEV),
            P(DEV, None),
        ),
        out_specs=P(GROUPS_DEV, None),
        check_vma=False,
    )
```

```python
import functools
import math

import jax
import jax.numpy as jnp
from jax import lax
from jax.experimental import pallas as pl
from jax.experimental.pallas import tpu as pltpu
from jax.sharding import Mesh
from jax.sharding import PartitionSpec as P


QH = 48
KVH = 8
HD = 128
EXPERTS = 4
BLOCK = 16
MOST = 3
DEV = ("dev_0", "dev_1", "dev_2")
GROUPS_DEV = ("groups", "dev_0", "dev_1", "dev_2")


EPS = 1e-05
NEG = -1e30

CUT_K = 8
CUT_N = 4


def passed_along(value, axis, steps):
    count = lax.axis_size(axis)
    leading, last = (max(0, -steps), min(count, count - steps))
    return lax.ppermute(value, axis, [(source, source + steps) for source in range(leading, last)])


def shifted(value, axis, steps):
    count = lax.axis_size(axis)
    return lax.ppermute(value, axis, [(place, (place + steps) % count) for place in range(count)])


def swapped(value):
    return shifted(value, "dev_2", 1)


def passed_on(value):
    chips, cores = lax.axis_size("dev_1"), lax.axis_size("dev_2")
    pairs = []
    for chip in range(chips):
        for core in range(cores):
            pairs.append((chip * cores + core, (chip + 1 - 2 * core) % chips * cores + core))
    return lax.ppermute(value, ("dev_1", "dev_2"), pairs)


def join_kernel(left_ref, right_ref, out_ref):
    half = left_ref.shape[1]
    out_ref[:, :half] = left_ref[...]
    out_ref[:, half:] = right_ref[...]


def joined(left, right):
    rows, half = left.shape
    vm = pl.BlockSpec(memory_space=pltpu.VMEM)
    return pl.pallas_call(
        join_kernel,
        out_shape=jax.ShapeDtypeStruct((rows, 2 * half), left.dtype),
        in_specs=[vm] * 2,
        out_specs=vm,
        compiler_params=pltpu.CompilerParams(vmem_limit_bytes=8 * 1024 * 1024),
        name="joined",
    )(left, right)


def gathered(own, left, right):
    other = swapped(own)
    far = lax.axis_size("dev_1") // 2
    came, theirs = {}, {}
    sides, whole = (left, right), other
    for step in range(1, far + 1):
        sides = [passed_on(x) for x in sides]
        came[step, 0] = joined(*sides)
        if step < far:
            whole = passed_on(whole)
            came[step, 1] = whole
        for part in (0, 1) if step < far else (0,):
            theirs[step, part] = swapped(came[step, part])
    return other, came, theirs


def hop_kernel(parts, *refs):
    out = refs[-1]
    total = None
    for ref, (row, col) in zip(refs, parts):
        term = ref[row : row + out.shape[0], col : col + out.shape[1]].astype(jnp.float32)
        total = term if total is None else total + term
    out[...] = total.astype(out.dtype)


def hop_sum(rows, cols, *terms):
    vm = pl.BlockSpec(memory_space=pltpu.VMEM)
    return pl.pallas_call(
        functools.partial(hop_kernel, [at for _, at in terms]),
        out_shape=jax.ShapeDtypeStruct((rows, cols), jnp.bfloat16),
        in_specs=[vm] * len(terms),
        out_specs=vm,
        compiler_params=pltpu.CompilerParams(vmem_limit_bytes=8 * 1024 * 1024),
        name="hop_sum",
    )(*[x for x, _ in terms])


def scattered(far, each, own, other, kept, got):
    half = own.shape[1] // 2
    moving = {}
    for step in range(far, 0, -1):
        for part in (0, 1) if step < far else (1,):
            for side in (0, 1):
                terms = [(x, (row, side * half)) for x, row in (kept[step, part], got[step, part])]
                if (part, side) in moving:
                    terms.append((moving[part, side], (0, 0)))
                parcel = hop_sum(each, half, *terms)
                moving[part, side] = passed_on(parcel)
    return own, moving[1, 0], moving[1, 1], swapped(two_sum(other, moving[0, 0], moving[0, 1]))


def two_kernel(whole_ref, left_ref, right_ref, out_ref):
    half = left_ref.shape[1]
    for side, ref in enumerate((left_ref, right_ref)):
        cols = slice(side * half, (side + 1) * half)
        out_ref[:, cols] = (whole_ref[:, cols].astype(jnp.float32) + ref[...].astype(jnp.float32)).astype(out_ref.dtype)


def two_sum(whole, left, right):
    vm = pl.BlockSpec(memory_space=pltpu.VMEM)
    return pl.pallas_call(
        two_kernel,
        out_shape=jax.ShapeDtypeStruct(whole.shape, whole.dtype),
        in_specs=[vm] * 3,
        out_specs=vm,
        compiler_params=pltpu.CompilerParams(vmem_limit_bytes=8 * 1024 * 1024),
        name="two_sum",
    )(whole, left, right)


def multiplied(pieces, gate, up, down, outs, ready):
    depth = gate.shape[0] // CUT_K
    span = down.shape[1] // CUT_N
    gate_v = up_v = None
    for k in range(CUT_K):
        cols = pl.ds(k * depth, depth)
        x = jnp.concatenate([p[:, cols] for p in pieces], 0)
        ready(k)
        g = jnp.dot(x, gate[cols, :], preferred_element_type=jnp.float32)
        u = jnp.dot(x, up[cols, :], preferred_element_type=jnp.float32)
        gate_v = g if gate_v is None else gate_v + g
        up_v = u if up_v is None else up_v + u
    act = (gate_v / (1.0 + jnp.exp(-gate_v)) * up_v).astype(jnp.bfloat16)
    ready(CUT_K)
    for n in range(CUT_N):
        cols = pl.ds(n * span, span)
        part = jnp.dot(act, down[:, cols], preferred_element_type=jnp.float32).astype(jnp.bfloat16)
        at = 0
        for out in outs:
            rows = out.shape[0]
            out[:, cols] = part[at : at + rows]
            at += rows


def early_kernel(count, *refs):
    pieces, (gate_far, up_far, down_far) = refs[:count], refs[count : count + 3]
    outs, (gate, up, down, sems) = refs[count + 3 : -4], refs[-4:]
    depth = gate.shape[0] // CUT_K
    copies = []
    for k in range(CUT_K):
        rows = pl.ds(k * depth, depth)
        copies.append(
            (
                pltpu.make_async_copy(gate_far.at[rows], gate.at[rows], sems.at[2 * k]),
                pltpu.make_async_copy(up_far.at[rows], up.at[rows], sems.at[2 * k + 1]),
            )
        )
    copies.append((pltpu.make_async_copy(down_far, down, sems.at[2 * CUT_K]),))
    for group in copies:
        for copy in group:
            copy.start()

    def ready(k):
        for copy in copies[k]:
            copy.wait()

    multiplied(pieces, gate, up, down, outs, ready)


def late_kernel(count, *refs):
    multiplied(refs[:count], *refs[count : count + 3], refs[count + 3 :], lambda k: None)


def product_cost(rows, width, hidden):
    return pl.CostEstimate(flops=6 * rows * width * hidden, bytes_accessed=6 * width * hidden, transcendentals=rows * hidden)


def early_products(pieces, weights, sizes):
    width, hidden = weights[0].shape
    vm = pl.BlockSpec(memory_space=pltpu.VMEM)
    far = pl.BlockSpec(memory_space=pltpu.HBM)
    outs = [jax.ShapeDtypeStruct((s, width), jnp.bfloat16) for s in sizes]
    held = [pltpu.VMEM(w.shape, w.dtype) for w in weights]
    return pl.pallas_call(
        functools.partial(early_kernel, len(pieces)),
        out_shape=outs + held,
        in_specs=[vm] * len(pieces) + [far] * 3,
        out_specs=[vm] * (len(sizes) + 3),
        scratch_shapes=[pltpu.SemaphoreType.DMA((2 * CUT_K + 1,))],
        compiler_params=pltpu.CompilerParams(vmem_limit_bytes=24 * 1024 * 1024),
        cost_estimate=product_cost(sum(sizes), width, hidden),
        name="early",
    )(*pieces, *[pltpu.with_memory_space_constraint(w, pltpu.HBM) for w in weights])


def late_products(pieces, weights, sizes):
    width, hidden = weights[0].shape
    vm = pl.BlockSpec(memory_space=pltpu.VMEM)
    return pl.pallas_call(
        functools.partial(late_kernel, len(pieces)),
        out_shape=[jax.ShapeDtypeStruct((s, width), jnp.bfloat16) for s in sizes],
        in_specs=[vm] * (len(pieces) + 3),
        out_specs=[vm] * len(sizes),
        compiler_params=pltpu.CompilerParams(vmem_limit_bytes=24 * 1024 * 1024),
        cost_estimate=product_cost(sum(sizes), width, hidden),
        name="late",
    )(*pieces, *weights)


def slots_of(ids_ref, reqs, top):
    named = [ids_ref[k, t] for t in range(reqs) for k in range(top)]
    slots = []
    for i, one in enumerate(named):
        slot = jnp.int32(0)
        for earlier in named[:i]:
            slot = slot + (earlier == one).astype(jnp.int32)
        slots.append(slot)
    return named, slots


def attend_kernel(me_ref, *refs):
    next_ref = refs[0]
    far_refs, (hidden_ref, leaving_ref, turned, mixed, packed), near_refs = refs[1:10], refs[10:15], refs[15:24]
    copies = [pltpu.make_async_copy(f, n, refs[24].at[i]) for i, (f, n) in enumerate(zip(far_refs, near_refs))]
    for copy in copies:
        copy.start()
    lens_ref, ids_ref, counts_ref, query_ref, own_ref, cache_ref, fresh_ref, tokens_ref, gain_ref = near_refs
    reqs, width = tokens_ref.shape
    length = cache_ref.shape[1]
    span = fresh_ref.shape[0]
    group = QH // KVH
    rows = group * reqs
    half = KVH * HD
    scale = 1.0 / math.sqrt(HD)
    me = me_ref[0]
    f32 = jnp.float32
    for copy in copies:
        copy.wait()
    for h in range(QH):
        turned[h * reqs : (h + 1) * reqs, :] = query_ref[:, h * HD : (h + 1) * HD].astype(f32)
    counts = counts_ref[...].astype(f32)
    places = lax.broadcasted_iota(jnp.int32, counts.shape, 1)
    before = jnp.sum(jnp.where(places < me, counts, 0.0), 1, keepdims=True)
    taken = jnp.sum(jnp.where(places == me, counts, 0.0), 1, keepdims=True)
    first = (before - (me * (span // BLOCK)).astype(f32)) * BLOCK
    last = first + taken * BLOCK
    row_w = lax.broadcasted_iota(jnp.int32, (rows, 2 * span), 0) % reqs
    col_w = lax.broadcasted_iota(jnp.int32, (rows, 2 * span), 1).astype(f32)
    live_w = (row_w == 0) & (col_w >= first) & (col_w < last)
    row_c = lax.broadcasted_iota(jnp.int32, (rows, reqs * length), 0) % reqs
    col_c = lax.broadcasted_iota(jnp.int32, (rows, reqs * length), 1)
    live_c = (row_c < 0)
    for r in range(reqs):
        live_c = live_c | ((row_c == r) & (col_c >= r * length) & (col_c < r * length + lens_ref[r]))
    for g in range(KVH):
        k_at = slice(g * HD, (g + 1) * HD)
        v_at = slice(half + g * HD, half + (g + 1) * HD)
        q32 = turned[g * rows : (g + 1) * rows, :]
        q = q32.astype(jnp.bfloat16)
        contract = (((1,), (1,)), ((), ()))
        key_c = cache_ref[:, :, k_at].reshape(reqs * length, HD)
        key_w = jnp.concatenate([fresh_ref[:, k_at], next_ref[:, k_at]], 0)
        key_o = jnp.concatenate([own_ref[:, k_at].astype(f32)] * group, 0)
        val_o = jnp.concatenate([own_ref[:, v_at].astype(f32)] * group, 0)
        s_c = lax.dot_general(q, key_c, contract, preferred_element_type=f32) * scale
        s_w = lax.dot_general(q, key_w, contract, preferred_element_type=f32) * scale
        s_o = jnp.sum(q32 * key_o, 1, keepdims=True) * scale
        s_c = jnp.where(live_c, s_c, NEG)
        s_w = jnp.where(live_w, s_w, NEG)
        top = jnp.maximum(jnp.maximum(jnp.max(s_c, 1, keepdims=True), jnp.max(s_w, 1, keepdims=True)), s_o)
        e_c = jnp.exp(s_c - top)
        e_w = jnp.exp(s_w - top)
        e_o = jnp.exp(s_o - top)
        total = jnp.sum(e_c, 1, keepdims=True) + jnp.sum(e_w, 1, keepdims=True) + e_o
        over = 1.0 / total
        p_c = (e_c * over).astype(jnp.bfloat16)
        p_w = (e_w * over).astype(jnp.bfloat16)
        p_o = (e_o * over).astype(jnp.bfloat16).astype(f32)
        val_c = cache_ref[:, :, v_at].reshape(reqs * length, HD)
        val_w = jnp.concatenate([fresh_ref[:, v_at], next_ref[:, v_at]], 0)
        out = jnp.dot(p_c, val_c, preferred_element_type=f32) + jnp.dot(p_w, val_w, preferred_element_type=f32)
        mixed[g * rows : (g + 1) * rows, :] = out + p_o * val_o
    squares = jnp.zeros((reqs, HD), f32)
    for h in range(QH):
        cols = slice(h * HD, (h + 1) * HD)
        hidden = tokens_ref[:, cols].astype(f32) + mixed[h * reqs : (h + 1) * reqs, :]
        hidden_ref[:, cols] = hidden
        squares = squares + hidden * hidden
    norm = lax.rsqrt(jnp.sum(squares, 1, keepdims=True) / width + EPS)
    normed = (hidden_ref[...] * norm * gain_ref[...]).astype(jnp.bfloat16).astype(f32)
    named, slots = slots_of(ids_ref, reqs, ids_ref.shape[0])
    tall = leaving_ref.shape[0] // EXPERTS
    padded = MOST + 1
    cell = lax.broadcasted_iota(jnp.int32, (EXPERTS * padded, 1), 0)
    gone = jnp.zeros((EXPERTS * padded, width), f32)
    for t in range(reqs):
        takes = jnp.zeros((EXPERTS * padded, 1), f32)
        for k in range(ids_ref.shape[0]):
            i = t * ids_ref.shape[0] + k
            takes = takes + (cell == named[i] * padded + slots[i]).astype(f32)
        gone = gone + takes * normed[t : t + 1, :]
    for j in range(width // HD):
        packed[pl.ds(j, EXPERTS * padded, stride=width // HD), :] = gone[:, j * HD : (j + 1) * HD]
    cut = width // HD
    for x in range(leaving_ref.shape[0]):
        at = x // tall * padded * cut
        leaving_ref[x, :, :] = packed[at : at + MOST * cut, :].astype(jnp.bfloat16)


def attended(me, lens, ids, counts, query, own, cache, fresh, following, tokens, gain, places):
    reqs, width = tokens.shape
    sm = pl.BlockSpec(memory_space=pltpu.SMEM)
    vm = pl.BlockSpec(memory_space=pltpu.VMEM)
    far = (lens, ids, counts, query, own, cache, fresh, tokens, gain)
    far = [pltpu.with_memory_space_constraint(x, pltpu.HBM) for x in far]
    return pl.pallas_call(
        attend_kernel,
        out_shape=[jax.ShapeDtypeStruct((reqs, width), jnp.float32), jax.ShapeDtypeStruct((places, MOST * width // HD, HD), jnp.bfloat16)],
        in_specs=[sm, vm] + [pl.BlockSpec(memory_space=pltpu.HBM)] * len(far),
        out_specs=[vm, vm],
        scratch_shapes=[
            pltpu.VMEM((QH * reqs, HD), jnp.float32),
            pltpu.VMEM((QH * reqs, HD), jnp.float32),
            pltpu.VMEM((EXPERTS * (MOST + 1) * width // HD, HD), jnp.float32),
            *(pltpu.SMEM(x.shape, x.dtype) for x in far[:2]),
            *(pltpu.VMEM(x.shape, x.dtype) for x in far[2:]),
            pltpu.SemaphoreType.DMA((len(far),)),
        ],
        compiler_params=pltpu.CompilerParams(vmem_limit_bytes=16 * 1024 * 1024),
        cost_estimate=pl.CostEstimate(flops=8 * reqs * width * 392, bytes_accessed=2 * 1024 * 1024, transcendentals=0),
        name="attended",
    )(me, following, *far)


def unpack_kernel(came_ref, block_ref, left_ref, right_ref, spread):
    rows, width = block_ref.shape
    half = width // 2
    spread[...] = came_ref[...].astype(jnp.float32).reshape(spread.shape)
    for j in range(width // HD):
        tile = spread[pl.ds(j, rows, stride=width // HD), :].astype(jnp.bfloat16)
        block_ref[:, j * HD : (j + 1) * HD] = tile
        side = left_ref if j * HD < half else right_ref
        side[:, j * HD % half : j * HD % half + HD] = tile


def unpacked(came):
    places, packed, lanes = came.shape
    vm = pl.BlockSpec(memory_space=pltpu.VMEM)
    return pl.pallas_call(
        unpack_kernel,
        out_shape=[
            jax.ShapeDtypeStruct((places * MOST, packed // MOST * lanes // cut), jnp.bfloat16) for cut in (1, 2, 2)
        ],
        in_specs=[vm],
        out_specs=[vm] * 3,
        scratch_shapes=[pltpu.VMEM((places * packed, lanes), jnp.float32)],
        compiler_params=pltpu.CompilerParams(vmem_limit_bytes=8 * 1024 * 1024),
        name="unpacked",
    )(came)


def pack_kernel(first_ref, left_ref, right_ref, third_ref, packed_ref, spread):
    rows, width = first_ref.shape
    f32 = jnp.float32
    half = left_ref.shape[1]
    for j in range(width // HD):
        cols = slice(j * HD, (j + 1) * HD)
        side = left_ref if j * HD < half else right_ref
        came = side[:, j * HD % half : j * HD % half + HD].astype(f32)
        total = first_ref[:, cols].astype(f32) + came + third_ref[:, cols].astype(f32)
        spread[pl.ds(j, rows, stride=width // HD), :] = total
    packed_ref[...] = spread[...].astype(jnp.bfloat16).reshape(packed_ref.shape)


def packed_sum(first, left, right, third, places):
    rows, width = first.shape
    vm = pl.BlockSpec(memory_space=pltpu.VMEM)
    return pl.pallas_call(
        pack_kernel,
        out_shape=jax.ShapeDtypeStruct((places, rows // places * width // HD, HD), jnp.bfloat16),
        in_specs=[vm] * 4,
        out_specs=vm,
        scratch_shapes=[pltpu.VMEM((rows * width // HD, HD), jnp.float32)],
        compiler_params=pltpu.CompilerParams(vmem_limit_bytes=8 * 1024 * 1024),
        name="packed_sum",
    )(first, left, right, third)


def mix_kernel(ids_ref, weights_ref, home_ref, hidden_ref, out_ref, spread):
    reqs, width = hidden_ref.shape
    tall = home_ref.shape[0] // EXPERTS
    cut = width // HD
    f32 = jnp.float32
    named, slots = slots_of(ids_ref, reqs, ids_ref.shape[0])
    sums = [jnp.zeros((cut, HD), f32) for _ in range(reqs)]
    for e in range(EXPERTS):
        for m in range(MOST):
            at = slice(m * cut, (m + 1) * cut)
            cell = home_ref[e * tall, at, :].astype(f32)
            for x in range(1, tall):
                cell = cell + home_ref[e * tall + x, at, :].astype(f32)
            for t in range(reqs):
                weight = jnp.float32(0.0)
                for k in range(ids_ref.shape[0]):
                    i = t * ids_ref.shape[0] + k
                    here = (named[i] == e) & (slots[i] == m)
                    weight = weight + jnp.where(here, weights_ref[k, t], 0.0)
                sums[t] = sums[t] + weight * cell
    for t in range(reqs):
        spread[t * cut : (t + 1) * cut, :] = sums[t]
    for j in range(cut):
        cols = slice(j * HD, (j + 1) * HD)
        moe = spread[pl.ds(j, reqs, stride=cut), :]
        out_ref[:, cols] = (hidden_ref[:, cols] + moe).astype(jnp.bfloat16)


def mixed_in(ids, weights, home, hidden):
    reqs, width = hidden.shape
    sm = pl.BlockSpec(memory_space=pltpu.SMEM)
    vm = pl.BlockSpec(memory_space=pltpu.VMEM)
    return pl.pallas_call(
        mix_kernel,
        out_shape=jax.ShapeDtypeStruct((reqs, width), jnp.bfloat16),
        in_specs=[sm, sm, vm, vm],
        out_specs=vm,
        scratch_shapes=[pltpu.VMEM((reqs * width // HD, HD), jnp.float32)],
        compiler_params=pltpu.CompilerParams(vmem_limit_bytes=8 * 1024 * 1024),
        name="mixed_in",
    )(ids, weights, home, hidden)


def layer(
    tokens,
    queries,
    token_kv,
    kv_cache,
    context_lengths,
    fresh_kv,
    block_counts,
    expert_ids,
    route_weights,
    norm_gain,
    w_gate,
    w_up,
    w_down,
):
    me = lax.axis_index(DEV)
    following = passed_along(fresh_kv, DEV, -1)
    rows_x = lax.axis_size("dev_0")
    me = lax.axis_index(DEV).astype(jnp.int32)[None]
    hidden_state, leaving = attended(
        me,
        context_lengths,
        expert_ids.T,
        block_counts[None],
        queries,
        token_kv,
        kv_cache,
        fresh_kv,
        following,
        tokens,
        norm_gain[None],
        rows_x,
    )
    own_block, *own_sides = unpacked(lax.all_to_all(leaving, "dev_0", 0, 0, tiled=True))
    other, came, theirs = gathered(own_block, *own_sides)
    far = lax.axis_size("dev_1") // 2
    each = rows_x * MOST
    near = range(far - 2, 0, -1)
    pieces = [own_block, other]
    for group in (theirs, came):
        for part in (0, 1):
            pieces += [group[step, part] for step in near]
    home_own, home_other, *groups, gate, up, down = early_products(
        pieces, (w_gate, w_up, w_down), [each, each] + [len(near) * each] * 4
    )
    last = far - 1
    pieces = [
        came[far, 0],
        theirs[last, 1],
        theirs[last, 0],
        theirs[far, 0],
        came[last, 1],
        came[last, 0],
    ]
    kept, got = {}, {}
    sent = [swapped(groups[2 + part]) for part in (0, 1)]
    for part in (0, 1):
        for i, step in enumerate(near):
            kept[step, part] = (groups[part], i * each)
            got[step, part] = (sent[part], i * each)
    *stay, sent_1, sent_0 = late_products(pieces, (gate, up, down), [each, each, each, 2 * each, each])
    kept[far, 1], kept[last, 1], kept[last, 0] = [(x, 0) for x in stay]
    first = swapped(sent_1)
    got[far, 1], got[last, 1], got[last, 0] = (first, 0), (first, each), (swapped(sent_0), 0)
    last_terms = scattered(far, each, home_own, home_other, kept, got)
    home = lax.all_to_all(packed_sum(*last_terms, rows_x), "dev_0", 0, 0, tiled=True)
    return mixed_in(expert_ids.T, route_weights.T, home, hidden_state)


def solution(mesh):
    split = Mesh(
        mesh.devices.reshape(mesh.shape["groups"], 8, 8, 2), ("groups", "dev_0", "dev_1", "dev_2")
    )
    return jax.shard_map(
        layer,
        mesh=split,
        in_specs=(
            P(GROUPS_DEV, None),
            P(GROUPS_DEV, None),
            P(GROUPS_DEV, None),
            P(GROUPS_DEV, None, None),
            P(GROUPS_DEV),
            P(GROUPS_DEV, None),
            P("groups"),
            P(GROUPS_DEV, None),
            P(GROUPS_DEV, None),
            P(),
            P(None, DEV),
            P(None, DEV),
            P(DEV, None),
        ),
        out_specs=P(GROUPS_DEV, None),
        check_vma=False,
    )
```

```python
import functools
import math

import jax
import jax.numpy as jnp
from jax import lax
from jax.experimental import pallas as pl
from jax.experimental.pallas import tpu as pltpu
from jax.sharding import Mesh
from jax.sharding import PartitionSpec as P


QH = 48
KVH = 8
HD = 128
EXPERTS = 4
BLOCK = 16
MOST = 3
DEV = ("dev_0", "dev_1", "dev_2")
GROUPS_DEV = ("groups", "dev_0", "dev_1", "dev_2")


EPS = 1e-05
NEG = -1e30

CUT_K = 8
CUT_N = 4


def passed_along(value, axis, steps):
    count = lax.axis_size(axis)
    leading, last = (max(0, -steps), min(count, count - steps))
    return lax.ppermute(value, axis, [(source, source + steps) for source in range(leading, last)])


def shifted(value, axis, steps):
    count = lax.axis_size(axis)
    return lax.ppermute(value, axis, [(place, (place + steps) % count) for place in range(count)])


def swapped(value):
    return shifted(value, "dev_2", 1)


def passed_on(value):
    chips, cores = lax.axis_size("dev_1"), lax.axis_size("dev_2")
    pairs = []
    for chip in range(chips):
        for core in range(cores):
            pairs.append((chip * cores + core, (chip + 1 - 2 * core) % chips * cores + core))
    return lax.ppermute(value, ("dev_1", "dev_2"), pairs)


def join_kernel(left_ref, right_ref, out_ref):
    half = left_ref.shape[1]
    out_ref[:, :half] = left_ref[...]
    out_ref[:, half:] = right_ref[...]


def joined(left, right):
    rows, half = left.shape
    vm = pl.BlockSpec(memory_space=pltpu.VMEM)
    return pl.pallas_call(
        join_kernel,
        out_shape=jax.ShapeDtypeStruct((rows, 2 * half), left.dtype),
        in_specs=[vm] * 2,
        out_specs=vm,
        compiler_params=pltpu.CompilerParams(vmem_limit_bytes=8 * 1024 * 1024),
        name="joined",
    )(left, right)


def gathered(own, left, right):
    other = swapped(own)
    far = lax.axis_size("dev_1") // 2
    came, theirs = {}, {}
    sides, whole = (left, right), other
    for step in range(1, far + 1):
        sides = [passed_on(x) for x in sides]
        came[step, 0] = joined(*sides)
        if step < far:
            whole = passed_on(whole)
            came[step, 1] = whole
        for part in (0, 1) if step < far else (0,):
            theirs[step, part] = swapped(came[step, part])
    return other, came, theirs


def hop_kernel(parts, *refs):
    out = refs[-1]
    total = None
    for ref, (row, col) in zip(refs, parts):
        term = ref[row : row + out.shape[0], col : col + out.shape[1]].astype(jnp.float32)
        total = term if total is None else total + term
    out[...] = total.astype(out.dtype)


def hop_sum(rows, cols, *terms):
    vm = pl.BlockSpec(memory_space=pltpu.VMEM)
    return pl.pallas_call(
        functools.partial(hop_kernel, [at for _, at in terms]),
        out_shape=jax.ShapeDtypeStruct((rows, cols), jnp.bfloat16),
        in_specs=[vm] * len(terms),
        out_specs=vm,
        compiler_params=pltpu.CompilerParams(vmem_limit_bytes=8 * 1024 * 1024),
        name="hop_sum",
    )(*[x for x, _ in terms])


def scattered(far, each, own, other, kept, got):
    half = own.shape[1] // 2
    moving = {}
    for step in range(far, 0, -1):
        for part in (0, 1) if step < far else (1,):
            for side in (0, 1):
                terms = [(x, (row, side * half)) for x, row in (kept[step, part], got[step, part])]
                if (part, side) in moving:
                    terms.append((moving[part, side], (0, 0)))
                parcel = hop_sum(each, half, *terms)
                moving[part, side] = passed_on(parcel)
    return own, moving[1, 0], moving[1, 1], swapped(two_sum(other, moving[0, 0], moving[0, 1]))


def two_kernel(whole_ref, left_ref, right_ref, out_ref):
    half = left_ref.shape[1]
    for side, ref in enumerate((left_ref, right_ref)):
        cols = slice(side * half, (side + 1) * half)
        out_ref[:, cols] = (whole_ref[:, cols].astype(jnp.float32) + ref[...].astype(jnp.float32)).astype(out_ref.dtype)


def two_sum(whole, left, right):
    vm = pl.BlockSpec(memory_space=pltpu.VMEM)
    return pl.pallas_call(
        two_kernel,
        out_shape=jax.ShapeDtypeStruct(whole.shape, whole.dtype),
        in_specs=[vm] * 3,
        out_specs=vm,
        compiler_params=pltpu.CompilerParams(vmem_limit_bytes=8 * 1024 * 1024),
        name="two_sum",
    )(whole, left, right)


def multiplied(pieces, gate, up, down, outs):
    depth = gate.shape[0] // CUT_K
    span = down.shape[1] // CUT_N
    gate_v = up_v = None
    for k in range(CUT_K):
        cols = pl.ds(k * depth, depth)
        x = jnp.concatenate([p[:, cols] for p in pieces], 0)
        g = jnp.dot(x, gate[cols, :], preferred_element_type=jnp.float32)
        u = jnp.dot(x, up[cols, :], preferred_element_type=jnp.float32)
        gate_v = g if gate_v is None else gate_v + g
        up_v = u if up_v is None else up_v + u
    act = (gate_v / (1.0 + jnp.exp(-gate_v)) * up_v).astype(jnp.bfloat16)
    for n in range(CUT_N):
        cols = pl.ds(n * span, span)
        part = jnp.dot(act, down[:, cols], preferred_element_type=jnp.float32).astype(jnp.bfloat16)
        at = 0
        for out in outs:
            rows = out.shape[0]
            out[:, cols] = part[at : at + rows]
            at += rows


def hold_kernel(*refs):
    count = len(refs) // 2
    copies = [pltpu.make_async_copy(refs[i], refs[count + i], refs[-1].at[i]) for i in range(count)]
    for copy in copies:
        copy.start()
    for copy in copies:
        copy.wait()


def held(weights):
    return pl.pallas_call(
        hold_kernel,
        out_shape=[pltpu.VMEM(w.shape, w.dtype) for w in weights],
        in_specs=[pl.BlockSpec(memory_space=pltpu.HBM)] * len(weights),
        out_specs=[pl.BlockSpec(memory_space=pltpu.VMEM)] * len(weights),
        scratch_shapes=[pltpu.SemaphoreType.DMA((len(weights),))],
        compiler_params=pltpu.CompilerParams(vmem_limit_bytes=16 * 1024 * 1024),
        cost_estimate=pl.CostEstimate(flops=1 << 20, bytes_accessed=2 * sum(w.size for w in weights), transcendentals=0),
        name="held",
    )(*[pltpu.with_memory_space_constraint(w, pltpu.HBM) for w in weights])


def product_kernel(count, *refs):
    multiplied(refs[:count], *refs[count : count + 3], refs[count + 3 :])


def product_cost(rows, width, hidden):
    return pl.CostEstimate(flops=6 * rows * width * hidden, bytes_accessed=6 * width * hidden, transcendentals=rows * hidden)


def products(pieces, weights, sizes):
    width, hidden = weights[0].shape
    vm = pl.BlockSpec(memory_space=pltpu.VMEM)
    return pl.pallas_call(
        functools.partial(product_kernel, len(pieces)),
        out_shape=[jax.ShapeDtypeStruct((s, width), jnp.bfloat16) for s in sizes],
        in_specs=[vm] * (len(pieces) + 3),
        out_specs=[vm] * len(sizes),
        compiler_params=pltpu.CompilerParams(vmem_limit_bytes=24 * 1024 * 1024),
        cost_estimate=product_cost(sum(sizes), width, hidden),
        name="products",
    )(*pieces, *weights)


def slots_of(ids_ref, reqs, top):
    named = [ids_ref[k, t] for t in range(reqs) for k in range(top)]
    slots = []
    for i, one in enumerate(named):
        slot = jnp.int32(0)
        for earlier in named[:i]:
            slot = slot + (earlier == one).astype(jnp.int32)
        slots.append(slot)
    return named, slots


def attend_kernel(me_ref, *refs):
    next_ref = refs[0]
    far_refs, (hidden_ref, leaving_ref, turned, mixed, packed), near_refs = refs[1:10], refs[10:15], refs[15:24]
    copies = [pltpu.make_async_copy(f, n, refs[24].at[i]) for i, (f, n) in enumerate(zip(far_refs, near_refs))]
    for copy in copies[5:7] + copies[:5] + copies[7:]:
        copy.start()
    lens_ref, ids_ref, counts_ref, query_ref, own_ref, cache_ref, fresh_ref, tokens_ref, gain_ref = near_refs
    reqs, width = tokens_ref.shape
    length = cache_ref.shape[1]
    span = fresh_ref.shape[0]
    group = QH // KVH
    rows = group * reqs
    half = KVH * HD
    scale = 1.0 / math.sqrt(HD)
    me = me_ref[0]
    f32 = jnp.float32
    for copy in copies[:5]:
        copy.wait()
    for h in range(QH):
        turned[h * reqs : (h + 1) * reqs, :] = query_ref[:, h * HD : (h + 1) * HD].astype(f32)
    counts = counts_ref[...].astype(f32)
    places = lax.broadcasted_iota(jnp.int32, counts.shape, 1)
    before = jnp.sum(jnp.where(places < me, counts, 0.0), 1, keepdims=True)
    taken = jnp.sum(jnp.where(places == me, counts, 0.0), 1, keepdims=True)
    first = (before - (me * (span // BLOCK)).astype(f32)) * BLOCK
    last = first + taken * BLOCK
    row_w = lax.broadcasted_iota(jnp.int32, (rows, 2 * span), 0) % reqs
    col_w = lax.broadcasted_iota(jnp.int32, (rows, 2 * span), 1).astype(f32)
    live_w = (row_w == 0) & (col_w >= first) & (col_w < last)
    row_c = lax.broadcasted_iota(jnp.int32, (rows, reqs * length), 0) % reqs
    col_c = lax.broadcasted_iota(jnp.int32, (rows, reqs * length), 1)
    live_c = (row_c < 0)
    for r in range(reqs):
        live_c = live_c | ((row_c == r) & (col_c >= r * length) & (col_c < r * length + lens_ref[r]))
    for copy in copies[5:7]:
        copy.wait()
    for g in range(KVH):
        k_at = slice(g * HD, (g + 1) * HD)
        v_at = slice(half + g * HD, half + (g + 1) * HD)
        q32 = turned[g * rows : (g + 1) * rows, :]
        q = q32.astype(jnp.bfloat16)
        contract = (((1,), (1,)), ((), ()))
        key_c = cache_ref[:, :, k_at].reshape(reqs * length, HD)
        key_w = jnp.concatenate([fresh_ref[:, k_at], next_ref[:, k_at]], 0)
        key_o = jnp.concatenate([own_ref[:, k_at].astype(f32)] * group, 0)
        val_o = jnp.concatenate([own_ref[:, v_at].astype(f32)] * group, 0)
        s_c = lax.dot_general(q, key_c, contract, preferred_element_type=f32) * scale
        s_w = lax.dot_general(q, key_w, contract, preferred_element_type=f32) * scale
        s_o = jnp.sum(q32 * key_o, 1, keepdims=True) * scale
        s_c = jnp.where(live_c, s_c, NEG)
        s_w = jnp.where(live_w, s_w, NEG)
        top = jnp.maximum(jnp.maximum(jnp.max(s_c, 1, keepdims=True), jnp.max(s_w, 1, keepdims=True)), s_o)
        e_c = jnp.exp(s_c - top)
        e_w = jnp.exp(s_w - top)
        e_o = jnp.exp(s_o - top)
        total = jnp.sum(e_c, 1, keepdims=True) + jnp.sum(e_w, 1, keepdims=True) + e_o
        over = 1.0 / total
        p_c = (e_c * over).astype(jnp.bfloat16)
        p_w = (e_w * over).astype(jnp.bfloat16)
        p_o = (e_o * over).astype(jnp.bfloat16).astype(f32)
        val_c = cache_ref[:, :, v_at].reshape(reqs * length, HD)
        val_w = jnp.concatenate([fresh_ref[:, v_at], next_ref[:, v_at]], 0)
        out = jnp.dot(p_c, val_c, preferred_element_type=f32) + jnp.dot(p_w, val_w, preferred_element_type=f32)
        mixed[g * rows : (g + 1) * rows, :] = out + p_o * val_o
    for copy in copies[7:]:
        copy.wait()
    squares = jnp.zeros((reqs, HD), f32)
    for h in range(QH):
        cols = slice(h * HD, (h + 1) * HD)
        hidden = tokens_ref[:, cols].astype(f32) + mixed[h * reqs : (h + 1) * reqs, :]
        hidden_ref[:, cols] = hidden
        squares = squares + hidden * hidden
    norm = lax.rsqrt(jnp.sum(squares, 1, keepdims=True) / width + EPS)
    normed = (hidden_ref[...] * norm * gain_ref[...]).astype(jnp.bfloat16).astype(f32)
    named, slots = slots_of(ids_ref, reqs, ids_ref.shape[0])
    tall = leaving_ref.shape[0] // EXPERTS
    padded = MOST + 1
    cell = lax.broadcasted_iota(jnp.int32, (EXPERTS * padded, 1), 0)
    gone = jnp.zeros((EXPERTS * padded, width), f32)
    for t in range(reqs):
        takes = jnp.zeros((EXPERTS * padded, 1), f32)
        for k in range(ids_ref.shape[0]):
            i = t * ids_ref.shape[0] + k
            takes = takes + (cell == named[i] * padded + slots[i]).astype(f32)
        gone = gone + takes * normed[t : t + 1, :]
    for j in range(width // HD):
        packed[pl.ds(j, EXPERTS * padded, stride=width // HD), :] = gone[:, j * HD : (j + 1) * HD]
    cut = width // HD
    for x in range(leaving_ref.shape[0]):
        at = x // tall * padded * cut
        leaving_ref[x, :, :] = packed[at : at + MOST * cut, :].astype(jnp.bfloat16)


def attended(me, lens, ids, counts, query, own, cache, fresh, following, tokens, gain, places):
    reqs, width = tokens.shape
    sm = pl.BlockSpec(memory_space=pltpu.SMEM)
    vm = pl.BlockSpec(memory_space=pltpu.VMEM)
    far = (lens, ids, counts, query, own, cache, fresh, tokens, gain)
    far = [pltpu.with_memory_space_constraint(x, pltpu.HBM) for x in far]
    return pl.pallas_call(
        attend_kernel,
        out_shape=[jax.ShapeDtypeStruct((reqs, width), jnp.float32), jax.ShapeDtypeStruct((places, MOST * width // HD, HD), jnp.bfloat16)],
        in_specs=[sm, vm] + [pl.BlockSpec(memory_space=pltpu.HBM)] * len(far),
        out_specs=[vm, vm],
        scratch_shapes=[
            pltpu.VMEM((QH * reqs, HD), jnp.float32),
            pltpu.VMEM((QH * reqs, HD), jnp.float32),
            pltpu.VMEM((EXPERTS * (MOST + 1) * width // HD, HD), jnp.float32),
            *(pltpu.SMEM(x.shape, x.dtype) for x in far[:2]),
            *(pltpu.VMEM(x.shape, x.dtype) for x in far[2:]),
            pltpu.SemaphoreType.DMA((len(far),)),
        ],
        compiler_params=pltpu.CompilerParams(vmem_limit_bytes=16 * 1024 * 1024),
        cost_estimate=pl.CostEstimate(flops=8 * reqs * width * 392, bytes_accessed=2 * 1024 * 1024, transcendentals=0),
        name="attended",
    )(me, following, *far)


def unpack_kernel(came_ref, block_ref, left_ref, right_ref, spread):
    rows, width = block_ref.shape
    half = width // 2
    spread[...] = came_ref[...].astype(jnp.float32).reshape(spread.shape)
    for j in range(width // HD):
        tile = spread[pl.ds(j, rows, stride=width // HD), :].astype(jnp.bfloat16)
        block_ref[:, j * HD : (j + 1) * HD] = tile
        side = left_ref if j * HD < half else right_ref
        side[:, j * HD % half : j * HD % half + HD] = tile


def unpacked(came):
    places, packed, lanes = came.shape
    vm = pl.BlockSpec(memory_space=pltpu.VMEM)
    return pl.pallas_call(
        unpack_kernel,
        out_shape=[
            jax.ShapeDtypeStruct((places * MOST, packed // MOST * lanes // cut), jnp.bfloat16) for cut in (1, 2, 2)
        ],
        in_specs=[vm],
        out_specs=[vm] * 3,
        scratch_shapes=[pltpu.VMEM((places * packed, lanes), jnp.float32)],
        compiler_params=pltpu.CompilerParams(vmem_limit_bytes=8 * 1024 * 1024),
        name="unpacked",
    )(came)


def pack_kernel(first_ref, left_ref, right_ref, third_ref, packed_ref, spread):
    rows, width = first_ref.shape
    f32 = jnp.float32
    half = left_ref.shape[1]
    for j in range(width // HD):
        cols = slice(j * HD, (j + 1) * HD)
        side = left_ref if j * HD < half else right_ref
        came = side[:, j * HD % half : j * HD % half + HD].astype(f32)
        total = first_ref[:, cols].astype(f32) + came + third_ref[:, cols].astype(f32)
        spread[pl.ds(j, rows, stride=width // HD), :] = total
    packed_ref[...] = spread[...].astype(jnp.bfloat16).reshape(packed_ref.shape)


def packed_sum(first, left, right, third, places):
    rows, width = first.shape
    vm = pl.BlockSpec(memory_space=pltpu.VMEM)
    return pl.pallas_call(
        pack_kernel,
        out_shape=jax.ShapeDtypeStruct((places, rows // places * width // HD, HD), jnp.bfloat16),
        in_specs=[vm] * 4,
        out_specs=vm,
        scratch_shapes=[pltpu.VMEM((rows * width // HD, HD), jnp.float32)],
        compiler_params=pltpu.CompilerParams(vmem_limit_bytes=8 * 1024 * 1024),
        name="packed_sum",
    )(first, left, right, third)


def mix_kernel(ids_ref, weights_ref, home_ref, hidden_ref, out_ref, spread):
    reqs, width = hidden_ref.shape
    tall = home_ref.shape[0] // EXPERTS
    cut = width // HD
    f32 = jnp.float32
    named, slots = slots_of(ids_ref, reqs, ids_ref.shape[0])
    sums = [jnp.zeros((cut, HD), f32) for _ in range(reqs)]
    for e in range(EXPERTS):
        for m in range(MOST):
            at = slice(m * cut, (m + 1) * cut)
            cell = home_ref[e * tall, at, :].astype(f32)
            for x in range(1, tall):
                cell = cell + home_ref[e * tall + x, at, :].astype(f32)
            for t in range(reqs):
                weight = jnp.float32(0.0)
                for k in range(ids_ref.shape[0]):
                    i = t * ids_ref.shape[0] + k
                    here = (named[i] == e) & (slots[i] == m)
                    weight = weight + jnp.where(here, weights_ref[k, t], 0.0)
                sums[t] = sums[t] + weight * cell
    for t in range(reqs):
        spread[t * cut : (t + 1) * cut, :] = sums[t]
    for j in range(cut):
        cols = slice(j * HD, (j + 1) * HD)
        moe = spread[pl.ds(j, reqs, stride=cut), :]
        out_ref[:, cols] = (hidden_ref[:, cols] + moe).astype(jnp.bfloat16)


def mixed_in(ids, weights, home, hidden):
    reqs, width = hidden.shape
    sm = pl.BlockSpec(memory_space=pltpu.SMEM)
    vm = pl.BlockSpec(memory_space=pltpu.VMEM)
    return pl.pallas_call(
        mix_kernel,
        out_shape=jax.ShapeDtypeStruct((reqs, width), jnp.bfloat16),
        in_specs=[sm, sm, vm, vm],
        out_specs=vm,
        scratch_shapes=[pltpu.VMEM((reqs * width // HD, HD), jnp.float32)],
        compiler_params=pltpu.CompilerParams(vmem_limit_bytes=8 * 1024 * 1024),
        name="mixed_in",
    )(ids, weights, home, hidden)


def layer(
    tokens,
    queries,
    token_kv,
    kv_cache,
    context_lengths,
    fresh_kv,
    block_counts,
    expert_ids,
    route_weights,
    norm_gain,
    w_gate,
    w_up,
    w_down,
):
    me = lax.axis_index(DEV)
    following = passed_along(fresh_kv, DEV, -1)
    rows_x = lax.axis_size("dev_0")
    me = lax.axis_index(DEV).astype(jnp.int32)[None]
    hidden_state, leaving = attended(
        me,
        context_lengths,
        expert_ids.T,
        block_counts[None],
        queries,
        token_kv,
        kv_cache,
        fresh_kv,
        following,
        tokens,
        norm_gain[None],
        rows_x,
    )
    own_block, *own_sides = unpacked(lax.all_to_all(leaving, "dev_0", 0, 0, tiled=True))
    other, came, theirs = gathered(own_block, *own_sides)
    far = lax.axis_size("dev_1") // 2
    each = rows_x * MOST
    near = range(far - 2, 0, -1)
    pieces = [own_block, other]
    for group in (theirs, came):
        for part in (0, 1):
            pieces += [group[step, part] for step in near]
    weights = held((w_gate, w_up, w_down))
    home_own, home_other, *groups = products(pieces, weights, [each, each] + [len(near) * each] * 4)
    last = far - 1
    pieces = [
        came[far, 0],
        theirs[last, 1],
        theirs[last, 0],
        theirs[far, 0],
        came[last, 1],
        came[last, 0],
    ]
    kept, got = {}, {}
    sent = [swapped(groups[2 + part]) for part in (0, 1)]
    for part in (0, 1):
        for i, step in enumerate(near):
            kept[step, part] = (groups[part], i * each)
            got[step, part] = (sent[part], i * each)
    *stay, sent_1, sent_0 = products(pieces, weights, [each, each, each, 2 * each, each])
    kept[far, 1], kept[last, 1], kept[last, 0] = [(x, 0) for x in stay]
    first = swapped(sent_1)
    got[far, 1], got[last, 1], got[last, 0] = (first, 0), (first, each), (swapped(sent_0), 0)
    last_terms = scattered(far, each, home_own, home_other, kept, got)
    home = lax.all_to_all(packed_sum(*last_terms, rows_x), "dev_0", 0, 0, tiled=True)
    return mixed_in(expert_ids.T, route_weights.T, home, hidden_state)


def solution(mesh):
    split = Mesh(
        mesh.devices.reshape(mesh.shape["groups"], 8, 8, 2), ("groups", "dev_0", "dev_1", "dev_2")
    )
    return jax.shard_map(
        layer,
        mesh=split,
        in_specs=(
            P(GROUPS_DEV, None),
            P(GROUPS_DEV, None),
            P(GROUPS_DEV, None),
            P(GROUPS_DEV, None, None),
            P(GROUPS_DEV),
            P(GROUPS_DEV, None),
            P("groups"),
            P(GROUPS_DEV, None),
            P(GROUPS_DEV, None),
            P(),
            P(None, DEV),
            P(None, DEV),
            P(DEV, None),
        ),
        out_specs=P(GROUPS_DEV, None),
        check_vma=False,
    )
```

```python
import functools
import math

import jax
import jax.numpy as jnp
from jax import lax
from jax.experimental import pallas as pl
from jax.experimental.pallas import tpu as pltpu
from jax.sharding import Mesh
from jax.sharding import PartitionSpec as P


QH = 48
KVH = 8
HD = 128
EXPERTS = 4
BLOCK = 16
MOST = 3
DEV = ("dev_0", "dev_1", "dev_2")
GROUPS_DEV = ("groups", "dev_0", "dev_1", "dev_2")


EPS = 1e-05
NEG = -1e30

CUT_K = 8
CUT_N = 4


def passed_along(value, axis, steps):
    count = lax.axis_size(axis)
    leading, last = (max(0, -steps), min(count, count - steps))
    return lax.ppermute(value, axis, [(source, source + steps) for source in range(leading, last)])


def shifted(value, axis, steps):
    count = lax.axis_size(axis)
    return lax.ppermute(value, axis, [(place, (place + steps) % count) for place in range(count)])


def swapped(value):
    return shifted(value, "dev_2", 1)


def passed_on(value):
    chips, cores = lax.axis_size("dev_1"), lax.axis_size("dev_2")
    pairs = []
    for chip in range(chips):
        for core in range(cores):
            pairs.append((chip * cores + core, (chip + 1 - 2 * core) % chips * cores + core))
    return lax.ppermute(value, ("dev_1", "dev_2"), pairs)


def join_kernel(left_ref, right_ref, out_ref):
    half = left_ref.shape[1]
    out_ref[:, :half] = left_ref[...]
    out_ref[:, half:] = right_ref[...]


def joined(left, right):
    rows, half = left.shape
    vm = pl.BlockSpec(memory_space=pltpu.VMEM)
    return pl.pallas_call(
        join_kernel,
        out_shape=jax.ShapeDtypeStruct((rows, 2 * half), left.dtype),
        in_specs=[vm] * 2,
        out_specs=vm,
        compiler_params=pltpu.CompilerParams(vmem_limit_bytes=8 * 1024 * 1024),
        name="joined",
    )(left, right)


def gathered(own, left, right):
    other = swapped(own)
    far = lax.axis_size("dev_1") // 2
    came, theirs = {}, {}
    sides, whole = (left, right), other
    for step in range(1, far + 1):
        sides = [passed_on(x) for x in sides]
        came[step, 0] = joined(*sides)
        if step < far:
            whole = passed_on(whole)
            came[step, 1] = whole
        for part in (0, 1) if step < far else (0,):
            theirs[step, part] = swapped(came[step, part])
    return other, came, theirs


def hop_kernel(parts, *refs):
    out = refs[-1]
    total = None
    for ref, (row, col) in zip(refs, parts):
        term = ref[row : row + out.shape[0], col : col + out.shape[1]].astype(jnp.float32)
        total = term if total is None else total + term
    out[...] = total.astype(out.dtype)


def hop_sum(rows, cols, *terms):
    vm = pl.BlockSpec(memory_space=pltpu.VMEM)
    return pl.pallas_call(
        functools.partial(hop_kernel, [at for _, at in terms]),
        out_shape=jax.ShapeDtypeStruct((rows, cols), jnp.bfloat16),
        in_specs=[vm] * len(terms),
        out_specs=vm,
        compiler_params=pltpu.CompilerParams(vmem_limit_bytes=8 * 1024 * 1024),
        name="hop_sum",
    )(*[x for x, _ in terms])


def scattered(far, each, own, other, kept, got):
    width = own.shape[1]
    half = width // 2
    moving = {}

    def hop(step, part, col, cols):
        terms = [(x, (row, col)) for x, row in (kept[step, part], got[step, part])]
        if (part, col) in moving:
            terms.append((moving[part, col], (0, 0)))
        parcel = hop_sum(each, cols, *terms)
        moving[part, col] = passed_on(parcel)

    for step in range(far, 0, -1):
        if step > 1:
            hop(step - 1, 0, 0, width)
        for side in (0, 1):
            hop(step, 1, side * half, half)
    leaving = hop_sum(each, width, (other, (0, 0)), (moving[0, 0], (0, 0)))
    return own, moving[1, 0], moving[1, half], swapped(leaving)


def multiplied(pieces, gate, up, down, outs, ready):
    depth = gate.shape[0] // CUT_K
    span = down.shape[1] // CUT_N
    gate_v = up_v = None
    for k in range(CUT_K):
        cols = pl.ds(k * depth, depth)
        x = jnp.concatenate([p[:, cols] for p in pieces], 0)
        ready(k)
        g = jnp.dot(x, gate[cols, :], preferred_element_type=jnp.float32)
        u = jnp.dot(x, up[cols, :], preferred_element_type=jnp.float32)
        gate_v = g if gate_v is None else gate_v + g
        up_v = u if up_v is None else up_v + u
    act = (gate_v / (1.0 + jnp.exp(-gate_v)) * up_v).astype(jnp.bfloat16)
    ready(CUT_K)
    for n in range(CUT_N):
        cols = pl.ds(n * span, span)
        part = jnp.dot(act, down[:, cols], preferred_element_type=jnp.float32).astype(jnp.bfloat16)
        at = 0
        for out in outs:
            rows = out.shape[0]
            out[:, cols] = part[at : at + rows]
            at += rows


def early_kernel(count, *refs):
    pieces, (gate_far, up_far, down_far) = refs[:count], refs[count : count + 3]
    outs, (gate, up, down, sems) = refs[count + 3 : -4], refs[-4:]
    depth = gate.shape[0] // CUT_K
    copies = []
    for k in range(CUT_K):
        rows = pl.ds(k * depth, depth)
        copies.append(
            (
                pltpu.make_async_copy(gate_far.at[rows], gate.at[rows], sems.at[2 * k]),
                pltpu.make_async_copy(up_far.at[rows], up.at[rows], sems.at[2 * k + 1]),
            )
        )
    copies.append((pltpu.make_async_copy(down_far, down, sems.at[2 * CUT_K]),))
    for group in copies:
        for copy in group:
            copy.start()

    def ready(k):
        for copy in copies[k]:
            copy.wait()

    multiplied(pieces, gate, up, down, outs, ready)


def late_kernel(count, *refs):
    multiplied(refs[:count], *refs[count : count + 3], refs[count + 3 :], lambda k: None)


def product_cost(rows, width, hidden):
    return pl.CostEstimate(flops=6 * rows * width * hidden, bytes_accessed=6 * width * hidden, transcendentals=rows * hidden)


def early_products(pieces, weights, sizes):
    width, hidden = weights[0].shape
    vm = pl.BlockSpec(memory_space=pltpu.VMEM)
    far = pl.BlockSpec(memory_space=pltpu.HBM)
    outs = [jax.ShapeDtypeStruct((s, width), jnp.bfloat16) for s in sizes]
    held = [pltpu.VMEM(w.shape, w.dtype) for w in weights]
    return pl.pallas_call(
        functools.partial(early_kernel, len(pieces)),
        out_shape=outs + held,
        in_specs=[vm] * len(pieces) + [far] * 3,
        out_specs=[vm] * (len(sizes) + 3),
        scratch_shapes=[pltpu.SemaphoreType.DMA((2 * CUT_K + 1,))],
        compiler_params=pltpu.CompilerParams(vmem_limit_bytes=24 * 1024 * 1024),
        cost_estimate=product_cost(sum(sizes), width, hidden),
        name="early",
    )(*pieces, *[pltpu.with_memory_space_constraint(w, pltpu.HBM) for w in weights])


def late_products(pieces, weights, sizes):
    width, hidden = weights[0].shape
    vm = pl.BlockSpec(memory_space=pltpu.VMEM)
    return pl.pallas_call(
        functools.partial(late_kernel, len(pieces)),
        out_shape=[jax.ShapeDtypeStruct((s, width), jnp.bfloat16) for s in sizes],
        in_specs=[vm] * (len(pieces) + 3),
        out_specs=[vm] * len(sizes),
        compiler_params=pltpu.CompilerParams(vmem_limit_bytes=24 * 1024 * 1024),
        cost_estimate=product_cost(sum(sizes), width, hidden),
        name="late",
    )(*pieces, *weights)


def slots_of(ids_ref, reqs, top):
    named = [ids_ref[k, t] for t in range(reqs) for k in range(top)]
    slots = []
    for i, one in enumerate(named):
        slot = jnp.int32(0)
        for earlier in named[:i]:
            slot = slot + (earlier == one).astype(jnp.int32)
        slots.append(slot)
    return named, slots


def attend_kernel(me_ref, *refs):
    next_ref = refs[0]
    far_refs, (hidden_ref, leaving_ref, turned, mixed, packed), near_refs = refs[1:10], refs[10:15], refs[15:24]
    copies = [pltpu.make_async_copy(f, n, refs[24].at[i]) for i, (f, n) in enumerate(zip(far_refs, near_refs))]
    for copy in copies:
        copy.start()
    lens_ref, ids_ref, counts_ref, query_ref, own_ref, cache_ref, fresh_ref, tokens_ref, gain_ref = near_refs
    reqs, width = tokens_ref.shape
    length = cache_ref.shape[1]
    span = fresh_ref.shape[0]
    group = QH // KVH
    rows = group * reqs
    half = KVH * HD
    scale = 1.0 / math.sqrt(HD)
    me = me_ref[0]
    f32 = jnp.float32
    for copy in copies:
        copy.wait()
    for h in range(QH):
        turned[h * reqs : (h + 1) * reqs, :] = query_ref[:, h * HD : (h + 1) * HD].astype(f32)
    counts = counts_ref[...].astype(f32)
    places = lax.broadcasted_iota(jnp.int32, counts.shape, 1)
    before = jnp.sum(jnp.where(places < me, counts, 0.0), 1, keepdims=True)
    taken = jnp.sum(jnp.where(places == me, counts, 0.0), 1, keepdims=True)
    first = (before - (me * (span // BLOCK)).astype(f32)) * BLOCK
    last = first + taken * BLOCK
    row_w = lax.broadcasted_iota(jnp.int32, (rows, 2 * span), 0) % reqs
    col_w = lax.broadcasted_iota(jnp.int32, (rows, 2 * span), 1).astype(f32)
    live_w = (row_w == 0) & (col_w >= first) & (col_w < last)
    row_c = lax.broadcasted_iota(jnp.int32, (rows, reqs * length), 0) % reqs
    col_c = lax.broadcasted_iota(jnp.int32, (rows, reqs * length), 1)
    live_c = (row_c < 0)
    for r in range(reqs):
        live_c = live_c | ((row_c == r) & (col_c >= r * length) & (col_c < r * length + lens_ref[r]))
    for g in range(KVH):
        k_at = slice(g * HD, (g + 1) * HD)
        v_at = slice(half + g * HD, half + (g + 1) * HD)
        q32 = turned[g * rows : (g + 1) * rows, :]
        q = q32.astype(jnp.bfloat16)
        contract = (((1,), (1,)), ((), ()))
        key_c = cache_ref[:, :, k_at].reshape(reqs * length, HD)
        key_w = jnp.concatenate([fresh_ref[:, k_at], next_ref[:, k_at]], 0)
        key_o = jnp.concatenate([own_ref[:, k_at].astype(f32)] * group, 0)
        val_o = jnp.concatenate([own_ref[:, v_at].astype(f32)] * group, 0)
        s_c = lax.dot_general(q, key_c, contract, preferred_element_type=f32) * scale
        s_w = lax.dot_general(q, key_w, contract, preferred_element_type=f32) * scale
        s_o = jnp.sum(q32 * key_o, 1, keepdims=True) * scale
        s_c = jnp.where(live_c, s_c, NEG)
        s_w = jnp.where(live_w, s_w, NEG)
        top = jnp.maximum(jnp.maximum(jnp.max(s_c, 1, keepdims=True), jnp.max(s_w, 1, keepdims=True)), s_o)
        e_c = jnp.exp(s_c - top)
        e_w = jnp.exp(s_w - top)
        e_o = jnp.exp(s_o - top)
        total = jnp.sum(e_c, 1, keepdims=True) + jnp.sum(e_w, 1, keepdims=True) + e_o
        over = 1.0 / total
        p_c = (e_c * over).astype(jnp.bfloat16)
        p_w = (e_w * over).astype(jnp.bfloat16)
        p_o = (e_o * over).astype(jnp.bfloat16).astype(f32)
        val_c = cache_ref[:, :, v_at].reshape(reqs * length, HD)
        val_w = jnp.concatenate([fresh_ref[:, v_at], next_ref[:, v_at]], 0)
        out = jnp.dot(p_c, val_c, preferred_element_type=f32) + jnp.dot(p_w, val_w, preferred_element_type=f32)
        mixed[g * rows : (g + 1) * rows, :] = out + p_o * val_o
    squares = jnp.zeros((reqs, HD), f32)
    for h in range(QH):
        cols = slice(h * HD, (h + 1) * HD)
        hidden = tokens_ref[:, cols].astype(f32) + mixed[h * reqs : (h + 1) * reqs, :]
        hidden_ref[:, cols] = hidden
        squares = squares + hidden * hidden
    norm = lax.rsqrt(jnp.sum(squares, 1, keepdims=True) / width + EPS)
    normed = (hidden_ref[...] * norm * gain_ref[...]).astype(jnp.bfloat16).astype(f32)
    named, slots = slots_of(ids_ref, reqs, ids_ref.shape[0])
    tall = leaving_ref.shape[0] // EXPERTS
    padded = MOST + 1
    cell = lax.broadcasted_iota(jnp.int32, (EXPERTS * padded, 1), 0)
    gone = jnp.zeros((EXPERTS * padded, width), f32)
    for t in range(reqs):
        takes = jnp.zeros((EXPERTS * padded, 1), f32)
        for k in range(ids_ref.shape[0]):
            i = t * ids_ref.shape[0] + k
            takes = takes + (cell == named[i] * padded + slots[i]).astype(f32)
        gone = gone + takes * normed[t : t + 1, :]
    for j in range(width // HD):
        packed[pl.ds(j, EXPERTS * padded, stride=width // HD), :] = gone[:, j * HD : (j + 1) * HD]
    cut = width // HD
    for x in range(leaving_ref.shape[0]):
        at = x // tall * padded * cut
        leaving_ref[x, :, :] = packed[at : at + MOST * cut, :].astype(jnp.bfloat16)


def attended(me, lens, ids, counts, query, own, cache, fresh, following, tokens, gain, places):
    reqs, width = tokens.shape
    sm = pl.BlockSpec(memory_space=pltpu.SMEM)
    vm = pl.BlockSpec(memory_space=pltpu.VMEM)
    far = (lens, ids, counts, query, own, cache, fresh, tokens, gain)
    far = [pltpu.with_memory_space_constraint(x, pltpu.HBM) for x in far]
    return pl.pallas_call(
        attend_kernel,
        out_shape=[jax.ShapeDtypeStruct((reqs, width), jnp.float32), jax.ShapeDtypeStruct((places, MOST * width // HD, HD), jnp.bfloat16)],
        in_specs=[sm, vm] + [pl.BlockSpec(memory_space=pltpu.HBM)] * len(far),
        out_specs=[vm, vm],
        scratch_shapes=[
            pltpu.VMEM((QH * reqs, HD), jnp.float32),
            pltpu.VMEM((QH * reqs, HD), jnp.float32),
            pltpu.VMEM((EXPERTS * (MOST + 1) * width // HD, HD), jnp.float32),
            *(pltpu.SMEM(x.shape, x.dtype) for x in far[:2]),
            *(pltpu.VMEM(x.shape, x.dtype) for x in far[2:]),
            pltpu.SemaphoreType.DMA((len(far),)),
        ],
        compiler_params=pltpu.CompilerParams(vmem_limit_bytes=16 * 1024 * 1024),
        cost_estimate=pl.CostEstimate(flops=8 * reqs * width * 392, bytes_accessed=2 * 1024 * 1024, transcendentals=0),
        name="attended",
    )(me, following, *far)


def unpack_kernel(came_ref, block_ref, left_ref, right_ref, spread):
    rows, width = block_ref.shape
    half = width // 2
    spread[...] = came_ref[...].astype(jnp.float32).reshape(spread.shape)
    for j in range(width // HD):
        tile = spread[pl.ds(j, rows, stride=width // HD), :].astype(jnp.bfloat16)
        block_ref[:, j * HD : (j + 1) * HD] = tile
        side = left_ref if j * HD < half else right_ref
        side[:, j * HD % half : j * HD % half + HD] = tile


def unpacked(came):
    places, packed, lanes = came.shape
    vm = pl.BlockSpec(memory_space=pltpu.VMEM)
    return pl.pallas_call(
        unpack_kernel,
        out_shape=[
            jax.ShapeDtypeStruct((places * MOST, packed // MOST * lanes // cut), jnp.bfloat16) for cut in (1, 2, 2)
        ],
        in_specs=[vm],
        out_specs=[vm] * 3,
        scratch_shapes=[pltpu.VMEM((places * packed, lanes), jnp.float32)],
        compiler_params=pltpu.CompilerParams(vmem_limit_bytes=8 * 1024 * 1024),
        name="unpacked",
    )(came)


def pack_kernel(first_ref, left_ref, right_ref, third_ref, packed_ref, spread):
    rows, width = first_ref.shape
    f32 = jnp.float32
    half = left_ref.shape[1]
    for j in range(width // HD):
        cols = slice(j * HD, (j + 1) * HD)
        side = left_ref if j * HD < half else right_ref
        came = side[:, j * HD % half : j * HD % half + HD].astype(f32)
        total = first_ref[:, cols].astype(f32) + came + third_ref[:, cols].astype(f32)
        spread[pl.ds(j, rows, stride=width // HD), :] = total
    packed_ref[...] = spread[...].astype(jnp.bfloat16).reshape(packed_ref.shape)


def packed_sum(first, left, right, third, places):
    rows, width = first.shape
    vm = pl.BlockSpec(memory_space=pltpu.VMEM)
    return pl.pallas_call(
        pack_kernel,
        out_shape=jax.ShapeDtypeStruct((places, rows // places * width // HD, HD), jnp.bfloat16),
        in_specs=[vm] * 4,
        out_specs=vm,
        scratch_shapes=[pltpu.VMEM((rows * width // HD, HD), jnp.float32)],
        compiler_params=pltpu.CompilerParams(vmem_limit_bytes=8 * 1024 * 1024),
        name="packed_sum",
    )(first, left, right, third)


def mix_kernel(ids_ref, weights_ref, home_ref, hidden_ref, out_ref, spread):
    reqs, width = hidden_ref.shape
    tall = home_ref.shape[0] // EXPERTS
    cut = width // HD
    f32 = jnp.float32
    named, slots = slots_of(ids_ref, reqs, ids_ref.shape[0])
    sums = [jnp.zeros((cut, HD), f32) for _ in range(reqs)]
    for e in range(EXPERTS):
        for m in range(MOST):
            at = slice(m * cut, (m + 1) * cut)
            cell = home_ref[e * tall, at, :].astype(f32)
            for x in range(1, tall):
                cell = cell + home_ref[e * tall + x, at, :].astype(f32)
            for t in range(reqs):
                weight = jnp.float32(0.0)
                for k in range(ids_ref.shape[0]):
                    i = t * ids_ref.shape[0] + k
                    here = (named[i] == e) & (slots[i] == m)
                    weight = weight + jnp.where(here, weights_ref[k, t], 0.0)
                sums[t] = sums[t] + weight * cell
    for t in range(reqs):
        spread[t * cut : (t + 1) * cut, :] = sums[t]
    for j in range(cut):
        cols = slice(j * HD, (j + 1) * HD)
        moe = spread[pl.ds(j, reqs, stride=cut), :]
        out_ref[:, cols] = (hidden_ref[:, cols] + moe).astype(jnp.bfloat16)


def mixed_in(ids, weights, home, hidden):
    reqs, width = hidden.shape
    sm = pl.BlockSpec(memory_space=pltpu.SMEM)
    vm = pl.BlockSpec(memory_space=pltpu.VMEM)
    return pl.pallas_call(
        mix_kernel,
        out_shape=jax.ShapeDtypeStruct((reqs, width), jnp.bfloat16),
        in_specs=[sm, sm, vm, vm],
        out_specs=vm,
        scratch_shapes=[pltpu.VMEM((reqs * width // HD, HD), jnp.float32)],
        compiler_params=pltpu.CompilerParams(vmem_limit_bytes=8 * 1024 * 1024),
        name="mixed_in",
    )(ids, weights, home, hidden)


def layer(
    tokens,
    queries,
    token_kv,
    kv_cache,
    context_lengths,
    fresh_kv,
    block_counts,
    expert_ids,
    route_weights,
    norm_gain,
    w_gate,
    w_up,
    w_down,
):
    me = lax.axis_index(DEV)
    following = passed_along(fresh_kv, DEV, -1)
    rows_x = lax.axis_size("dev_0")
    me = lax.axis_index(DEV).astype(jnp.int32)[None]
    hidden_state, leaving = attended(
        me,
        context_lengths,
        expert_ids.T,
        block_counts[None],
        queries,
        token_kv,
        kv_cache,
        fresh_kv,
        following,
        tokens,
        norm_gain[None],
        rows_x,
    )
    own_block, *own_sides = unpacked(lax.all_to_all(leaving, "dev_0", 0, 0, tiled=True))
    other, came, theirs = gathered(own_block, *own_sides)
    far = lax.axis_size("dev_1") // 2
    each = rows_x * MOST
    near = range(far - 2, 0, -1)
    pieces = [own_block, other]
    for group in (theirs, came):
        for part in (0, 1):
            pieces += [group[step, part] for step in near]
    home_own, home_other, *groups, gate, up, down = early_products(
        pieces, (w_gate, w_up, w_down), [each, each] + [len(near) * each] * 4
    )
    last = far - 1
    pieces = [
        came[far, 0],
        theirs[last, 1],
        theirs[last, 0],
        theirs[far, 0],
        came[last, 1],
        came[last, 0],
    ]
    kept, got = {}, {}
    sent = [swapped(groups[2 + part]) for part in (0, 1)]
    for part in (0, 1):
        for i, step in enumerate(near):
            kept[step, part] = (groups[part], i * each)
            got[step, part] = (sent[part], i * each)
    *stay, sent_1, sent_0 = late_products(pieces, (gate, up, down), [each, each, each, 2 * each, each])
    kept[far, 1], kept[last, 1], kept[last, 0] = [(x, 0) for x in stay]
    first = swapped(sent_1)
    got[far, 1], got[last, 1], got[last, 0] = (first, 0), (first, each), (swapped(sent_0), 0)
    last_terms = scattered(far, each, home_own, home_other, kept, got)
    home = lax.all_to_all(packed_sum(*last_terms, rows_x), "dev_0", 0, 0, tiled=True)
    return mixed_in(expert_ids.T, route_weights.T, home, hidden_state)


def solution(mesh):
    split = Mesh(
        mesh.devices.reshape(mesh.shape["groups"], 8, 8, 2), ("groups", "dev_0", "dev_1", "dev_2")
    )
    return jax.shard_map(
        layer,
        mesh=split,
        in_specs=(
            P(GROUPS_DEV, None),
            P(GROUPS_DEV, None),
            P(GROUPS_DEV, None),
            P(GROUPS_DEV, None, None),
            P(GROUPS_DEV),
            P(GROUPS_DEV, None),
            P("groups"),
            P(GROUPS_DEV, None),
            P(GROUPS_DEV, None),
            P(),
            P(None, DEV),
            P(None, DEV),
            P(DEV, None),
        ),
        out_specs=P(GROUPS_DEV, None),
        check_vma=False,
    )
```

```python
import functools
import math

import jax
import jax.numpy as jnp
from jax import lax
from jax.experimental import pallas as pl
from jax.experimental.pallas import tpu as pltpu
from jax.sharding import Mesh
from jax.sharding import PartitionSpec as P


QH = 48
KVH = 8
HD = 128
EXPERTS = 4
BLOCK = 16
MOST = 3
DEV = ("dev_0", "dev_1", "dev_2")
GROUPS_DEV = ("groups", "dev_0", "dev_1", "dev_2")


EPS = 1e-05
NEG = -1e30

CUT_K = 8
CUT_N = 4


def passed_along(value, axis, steps):
    count = lax.axis_size(axis)
    leading, last = (max(0, -steps), min(count, count - steps))
    return lax.ppermute(value, axis, [(source, source + steps) for source in range(leading, last)])


def shifted(value, axis, steps):
    count = lax.axis_size(axis)
    return lax.ppermute(value, axis, [(place, (place + steps) % count) for place in range(count)])


def swapped(value):
    return shifted(value, "dev_2", 1)


def passed_on(value):
    chips, cores = lax.axis_size("dev_1"), lax.axis_size("dev_2")
    pairs = []
    for chip in range(chips):
        for core in range(cores):
            pairs.append((chip * cores + core, (chip + 1 - 2 * core) % chips * cores + core))
    return lax.ppermute(value, ("dev_1", "dev_2"), pairs)


def join_kernel(*refs):
    out = refs[-1]
    rows, half = refs[0].shape
    for i, ref in enumerate(refs[:-1]):
        row, col = i // 2 * rows, i % 2 * half
        out[row : row + rows, col : col + half] = ref[...]


def joined(*sides):
    rows, half = sides[0].shape
    vm = pl.BlockSpec(memory_space=pltpu.VMEM)
    return pl.pallas_call(
        join_kernel,
        out_shape=jax.ShapeDtypeStruct((len(sides) // 2 * rows, 2 * half), sides[0].dtype),
        in_specs=[vm] * len(sides),
        out_specs=vm,
        compiler_params=pltpu.CompilerParams(vmem_limit_bytes=8 * 1024 * 1024),
        name="joined",
    )(*sides)


def gathered(left, right):
    far = lax.axis_size("dev_1") // 2
    sides = {0: [left, right], 1: [swapped(x) for x in (left, right)]}
    other = joined(*sides[1])
    came, theirs = {}, {}
    for step in range(1, far + 1):
        parts = (1, 0) if step < far else (0,)
        for part in reversed(parts):
            sides[part] = [passed_on(x) for x in sides[part]]
        came[step] = joined(*[x for part in parts for x in sides[part]])
        theirs[step] = swapped(came[step])
    return other, came, theirs


def hop_kernel(parts, *refs):
    out = refs[-1]
    total = None
    for ref, (row, col) in zip(refs, parts):
        term = ref[row : row + out.shape[0], col : col + out.shape[1]].astype(jnp.float32)
        total = term if total is None else total + term
    out[...] = total.astype(out.dtype)


def hop_sum(rows, cols, *terms):
    vm = pl.BlockSpec(memory_space=pltpu.VMEM)
    return pl.pallas_call(
        functools.partial(hop_kernel, [at for _, at in terms]),
        out_shape=jax.ShapeDtypeStruct((rows, cols), jnp.bfloat16),
        in_specs=[vm] * len(terms),
        out_specs=vm,
        compiler_params=pltpu.CompilerParams(vmem_limit_bytes=8 * 1024 * 1024),
        name="hop_sum",
    )(*[x for x, _ in terms])


def scattered(far, each, own, other, kept, got):
    half = own.shape[1] // 2
    moving = {}
    for step in range(far, 0, -1):
        for part in (0, 1) if step < far else (1,):
            for side in (0, 1):
                terms = [(x, (row, side * half)) for x, row in (kept[step, part], got[step, part])]
                if (part, side) in moving:
                    terms.append((moving[part, side], (0, 0)))
                parcel = hop_sum(each, half, *terms)
                moving[part, side] = passed_on(parcel)
    return own, moving[1, 0], moving[1, 1], swapped(two_sum(other, moving[0, 0], moving[0, 1]))


def two_kernel(whole_ref, left_ref, right_ref, out_ref):
    half = left_ref.shape[1]
    for side, ref in enumerate((left_ref, right_ref)):
        cols = slice(side * half, (side + 1) * half)
        out_ref[:, cols] = (whole_ref[:, cols].astype(jnp.float32) + ref[...].astype(jnp.float32)).astype(out_ref.dtype)


def two_sum(whole, left, right):
    vm = pl.BlockSpec(memory_space=pltpu.VMEM)
    return pl.pallas_call(
        two_kernel,
        out_shape=jax.ShapeDtypeStruct(whole.shape, whole.dtype),
        in_specs=[vm] * 3,
        out_specs=vm,
        compiler_params=pltpu.CompilerParams(vmem_limit_bytes=8 * 1024 * 1024),
        name="two_sum",
    )(whole, left, right)


def multiplied(pieces, gate, up, down, outs, ready):
    depth = gate.shape[0] // CUT_K
    span = down.shape[1] // CUT_N
    gate_v = up_v = None
    for k in range(CUT_K):
        cols = pl.ds(k * depth, depth)
        x = jnp.concatenate([p[:, cols] for p in pieces], 0)
        ready(k)
        g = jnp.dot(x, gate[cols, :], preferred_element_type=jnp.float32)
        u = jnp.dot(x, up[cols, :], preferred_element_type=jnp.float32)
        gate_v = g if gate_v is None else gate_v + g
        up_v = u if up_v is None else up_v + u
    act = (gate_v / (1.0 + jnp.exp(-gate_v)) * up_v).astype(jnp.bfloat16)
    ready(CUT_K)
    for n in range(CUT_N):
        cols = pl.ds(n * span, span)
        part = jnp.dot(act, down[:, cols], preferred_element_type=jnp.float32).astype(jnp.bfloat16)
        at = 0
        for out in outs:
            rows = out.shape[0]
            out[:, cols] = part[at : at + rows]
            at += rows


def early_kernel(count, *refs):
    pieces, (gate_far, up_far, down_far) = refs[:count], refs[count : count + 3]
    outs, (gate, up, down, sems) = refs[count + 3 : -4], refs[-4:]
    depth = gate.shape[0] // CUT_K
    copies = []
    for k in range(CUT_K):
        rows = pl.ds(k * depth, depth)
        copies.append(
            (
                pltpu.make_async_copy(gate_far.at[rows], gate.at[rows], sems.at[2 * k]),
                pltpu.make_async_copy(up_far.at[rows], up.at[rows], sems.at[2 * k + 1]),
            )
        )
    copies.append((pltpu.make_async_copy(down_far, down, sems.at[2 * CUT_K]),))
    for group in copies:
        for copy in group:
            copy.start()

    def ready(k):
        for copy in copies[k]:
            copy.wait()

    multiplied(pieces, gate, up, down, outs, ready)


def late_kernel(count, *refs):
    multiplied(refs[:count], *refs[count : count + 3], refs[count + 3 :], lambda k: None)


def product_cost(rows, width, hidden):
    return pl.CostEstimate(flops=6 * rows * width * hidden, bytes_accessed=6 * width * hidden, transcendentals=rows * hidden)


def early_products(pieces, weights, sizes):
    width, hidden = weights[0].shape
    vm = pl.BlockSpec(memory_space=pltpu.VMEM)
    far = pl.BlockSpec(memory_space=pltpu.HBM)
    outs = [jax.ShapeDtypeStruct((s, width), jnp.bfloat16) for s in sizes]
    held = [pltpu.VMEM(w.shape, w.dtype) for w in weights]
    return pl.pallas_call(
        functools.partial(early_kernel, len(pieces)),
        out_shape=outs + held,
        in_specs=[vm] * len(pieces) + [far] * 3,
        out_specs=[vm] * (len(sizes) + 3),
        scratch_shapes=[pltpu.SemaphoreType.DMA((2 * CUT_K + 1,))],
        compiler_params=pltpu.CompilerParams(vmem_limit_bytes=24 * 1024 * 1024),
        cost_estimate=product_cost(sum(sizes), width, hidden),
        name="early",
    )(*pieces, *[pltpu.with_memory_space_constraint(w, pltpu.HBM) for w in weights])


def late_products(pieces, weights, sizes):
    width, hidden = weights[0].shape
    vm = pl.BlockSpec(memory_space=pltpu.VMEM)
    return pl.pallas_call(
        functools.partial(late_kernel, len(pieces)),
        out_shape=[jax.ShapeDtypeStruct((s, width), jnp.bfloat16) for s in sizes],
        in_specs=[vm] * (len(pieces) + 3),
        out_specs=[vm] * len(sizes),
        compiler_params=pltpu.CompilerParams(vmem_limit_bytes=24 * 1024 * 1024),
        cost_estimate=product_cost(sum(sizes), width, hidden),
        name="late",
    )(*pieces, *weights)


def slots_of(ids_ref, reqs, top):
    named = [ids_ref[k, t] for t in range(reqs) for k in range(top)]
    slots = []
    for i, one in enumerate(named):
        slot = jnp.int32(0)
        for earlier in named[:i]:
            slot = slot + (earlier == one).astype(jnp.int32)
        slots.append(slot)
    return named, slots


def attend_kernel(me_ref, *refs):
    next_ref = refs[0]
    far_refs, (hidden_ref, leaving_ref, turned, mixed, packed), near_refs = refs[1:10], refs[10:15], refs[15:24]
    copies = [pltpu.make_async_copy(f, n, refs[24].at[i]) for i, (f, n) in enumerate(zip(far_refs, near_refs))]
    for copy in copies:
        copy.start()
    lens_ref, ids_ref, counts_ref, query_ref, own_ref, cache_ref, fresh_ref, tokens_ref, gain_ref = near_refs
    reqs, width = tokens_ref.shape
    length = cache_ref.shape[1]
    span = fresh_ref.shape[0]
    group = QH // KVH
    rows = group * reqs
    half = KVH * HD
    scale = 1.0 / math.sqrt(HD)
    me = me_ref[0]
    f32 = jnp.float32
    for copy in copies:
        copy.wait()
    for h in range(QH):
        turned[h * reqs : (h + 1) * reqs, :] = query_ref[:, h * HD : (h + 1) * HD].astype(f32)
    counts = counts_ref[...].astype(f32)
    places = lax.broadcasted_iota(jnp.int32, counts.shape, 1)
    before = jnp.sum(jnp.where(places < me, counts, 0.0), 1, keepdims=True)
    taken = jnp.sum(jnp.where(places == me, counts, 0.0), 1, keepdims=True)
    first = (before - (me * (span // BLOCK)).astype(f32)) * BLOCK
    last = first + taken * BLOCK
    row_w = lax.broadcasted_iota(jnp.int32, (rows, 2 * span), 0) % reqs
    col_w = lax.broadcasted_iota(jnp.int32, (rows, 2 * span), 1).astype(f32)
    live_w = (row_w == 0) & (col_w >= first) & (col_w < last)
    row_c = lax.broadcasted_iota(jnp.int32, (rows, reqs * length), 0) % reqs
    col_c = lax.broadcasted_iota(jnp.int32, (rows, reqs * length), 1)
    live_c = (row_c < 0)
    for r in range(reqs):
        live_c = live_c | ((row_c == r) & (col_c >= r * length) & (col_c < r * length + lens_ref[r]))
    for g in range(KVH):
        k_at = slice(g * HD, (g + 1) * HD)
        v_at = slice(half + g * HD, half + (g + 1) * HD)
        q32 = turned[g * rows : (g + 1) * rows, :]
        q = q32.astype(jnp.bfloat16)
        contract = (((1,), (1,)), ((), ()))
        key_c = cache_ref[:, :, k_at].reshape(reqs * length, HD)
        key_w = jnp.concatenate([fresh_ref[:, k_at], next_ref[:, k_at]], 0)
        key_o = jnp.concatenate([own_ref[:, k_at].astype(f32)] * group, 0)
        val_o = jnp.concatenate([own_ref[:, v_at].astype(f32)] * group, 0)
        s_c = lax.dot_general(q, key_c, contract, preferred_element_type=f32) * scale
        s_w = lax.dot_general(q, key_w, contract, preferred_element_type=f32) * scale
        s_o = jnp.sum(q32 * key_o, 1, keepdims=True) * scale
        s_c = jnp.where(live_c, s_c, NEG)
        s_w = jnp.where(live_w, s_w, NEG)
        top = jnp.maximum(jnp.maximum(jnp.max(s_c, 1, keepdims=True), jnp.max(s_w, 1, keepdims=True)), s_o)
        e_c = jnp.exp(s_c - top)
        e_w = jnp.exp(s_w - top)
        e_o = jnp.exp(s_o - top)
        total = jnp.sum(e_c, 1, keepdims=True) + jnp.sum(e_w, 1, keepdims=True) + e_o
        over = 1.0 / total
        p_c = (e_c * over).astype(jnp.bfloat16)
        p_w = (e_w * over).astype(jnp.bfloat16)
        p_o = (e_o * over).astype(jnp.bfloat16).astype(f32)
        val_c = cache_ref[:, :, v_at].reshape(reqs * length, HD)
        val_w = jnp.concatenate([fresh_ref[:, v_at], next_ref[:, v_at]], 0)
        out = jnp.dot(p_c, val_c, preferred_element_type=f32) + jnp.dot(p_w, val_w, preferred_element_type=f32)
        mixed[g * rows : (g + 1) * rows, :] = out + p_o * val_o
    squares = jnp.zeros((reqs, HD), f32)
    for h in range(QH):
        cols = slice(h * HD, (h + 1) * HD)
        hidden = tokens_ref[:, cols].astype(f32) + mixed[h * reqs : (h + 1) * reqs, :]
        hidden_ref[:, cols] = hidden
        squares = squares + hidden * hidden
    norm = lax.rsqrt(jnp.sum(squares, 1, keepdims=True) / width + EPS)
    normed = (hidden_ref[...] * norm * gain_ref[...]).astype(jnp.bfloat16).astype(f32)
    named, slots = slots_of(ids_ref, reqs, ids_ref.shape[0])
    tall = leaving_ref.shape[0] // EXPERTS
    padded = MOST + 1
    cell = lax.broadcasted_iota(jnp.int32, (EXPERTS * padded, 1), 0)
    gone = jnp.zeros((EXPERTS * padded, width), f32)
    for t in range(reqs):
        takes = jnp.zeros((EXPERTS * padded, 1), f32)
        for k in range(ids_ref.shape[0]):
            i = t * ids_ref.shape[0] + k
            takes = takes + (cell == named[i] * padded + slots[i]).astype(f32)
        gone = gone + takes * normed[t : t + 1, :]
    for j in range(width // HD):
        packed[pl.ds(j, EXPERTS * padded, stride=width // HD), :] = gone[:, j * HD : (j + 1) * HD]
    cut = width // HD
    for x in range(leaving_ref.shape[0]):
        at = x // tall * padded * cut
        leaving_ref[x, :, :] = packed[at : at + MOST * cut, :].astype(jnp.bfloat16)


def attended(me, lens, ids, counts, query, own, cache, fresh, following, tokens, gain, places):
    reqs, width = tokens.shape
    sm = pl.BlockSpec(memory_space=pltpu.SMEM)
    vm = pl.BlockSpec(memory_space=pltpu.VMEM)
    far = (lens, ids, counts, query, own, cache, fresh, tokens, gain)
    far = [pltpu.with_memory_space_constraint(x, pltpu.HBM) for x in far]
    return pl.pallas_call(
        attend_kernel,
        out_shape=[jax.ShapeDtypeStruct((reqs, width), jnp.float32), jax.ShapeDtypeStruct((places, MOST * width // HD, HD), jnp.bfloat16)],
        in_specs=[sm, vm] + [pl.BlockSpec(memory_space=pltpu.HBM)] * len(far),
        out_specs=[vm, vm],
        scratch_shapes=[
            pltpu.VMEM((QH * reqs, HD), jnp.float32),
            pltpu.VMEM((QH * reqs, HD), jnp.float32),
            pltpu.VMEM((EXPERTS * (MOST + 1) * width // HD, HD), jnp.float32),
            *(pltpu.SMEM(x.shape, x.dtype) for x in far[:2]),
            *(pltpu.VMEM(x.shape, x.dtype) for x in far[2:]),
            pltpu.SemaphoreType.DMA((len(far),)),
        ],
        compiler_params=pltpu.CompilerParams(vmem_limit_bytes=16 * 1024 * 1024),
        cost_estimate=pl.CostEstimate(flops=8 * reqs * width * 392, bytes_accessed=2 * 1024 * 1024, transcendentals=0),
        name="attended",
    )(me, following, *far)


def unpack_kernel(came_ref, block_ref, left_ref, right_ref, spread):
    rows, width = block_ref.shape
    half = width // 2
    spread[...] = came_ref[...].astype(jnp.float32).reshape(spread.shape)
    for j in range(width // HD):
        tile = spread[pl.ds(j, rows, stride=width // HD), :].astype(jnp.bfloat16)
        block_ref[:, j * HD : (j + 1) * HD] = tile
        side = left_ref if j * HD < half else right_ref
        side[:, j * HD % half : j * HD % half + HD] = tile


def unpacked(came):
    places, packed, lanes = came.shape
    vm = pl.BlockSpec(memory_space=pltpu.VMEM)
    return pl.pallas_call(
        unpack_kernel,
        out_shape=[
            jax.ShapeDtypeStruct((places * MOST, packed // MOST * lanes // cut), jnp.bfloat16) for cut in (1, 2, 2)
        ],
        in_specs=[vm],
        out_specs=[vm] * 3,
        scratch_shapes=[pltpu.VMEM((places * packed, lanes), jnp.float32)],
        compiler_params=pltpu.CompilerParams(vmem_limit_bytes=8 * 1024 * 1024),
        name="unpacked",
    )(came)


def pack_kernel(first_ref, left_ref, right_ref, third_ref, packed_ref, spread):
    rows, width = first_ref.shape
    f32 = jnp.float32
    half = left_ref.shape[1]
    for j in range(width // HD):
        cols = slice(j * HD, (j + 1) * HD)
        side = left_ref if j * HD < half else right_ref
        came = side[:, j * HD % half : j * HD % half + HD].astype(f32)
        total = first_ref[:, cols].astype(f32) + came + third_ref[:, cols].astype(f32)
        spread[pl.ds(j, rows, stride=width // HD), :] = total
    packed_ref[...] = spread[...].astype(jnp.bfloat16).reshape(packed_ref.shape)


def packed_sum(first, left, right, third, places):
    rows, width = first.shape
    vm = pl.BlockSpec(memory_space=pltpu.VMEM)
    return pl.pallas_call(
        pack_kernel,
        out_shape=jax.ShapeDtypeStruct((places, rows // places * width // HD, HD), jnp.bfloat16),
        in_specs=[vm] * 4,
        out_specs=vm,
        scratch_shapes=[pltpu.VMEM((rows * width // HD, HD), jnp.float32)],
        compiler_params=pltpu.CompilerParams(vmem_limit_bytes=8 * 1024 * 1024),
        name="packed_sum",
    )(first, left, right, third)


def mix_kernel(ids_ref, weights_ref, home_ref, hidden_ref, out_ref, spread):
    reqs, width = hidden_ref.shape
    tall = home_ref.shape[0] // EXPERTS
    cut = width // HD
    f32 = jnp.float32
    named, slots = slots_of(ids_ref, reqs, ids_ref.shape[0])
    sums = [jnp.zeros((cut, HD), f32) for _ in range(reqs)]
    for e in range(EXPERTS):
        for m in range(MOST):
            at = slice(m * cut, (m + 1) * cut)
            cell = home_ref[e * tall, at, :].astype(f32)
            for x in range(1, tall):
                cell = cell + home_ref[e * tall + x, at, :].astype(f32)
            for t in range(reqs):
                weight = jnp.float32(0.0)
                for k in range(ids_ref.shape[0]):
                    i = t * ids_ref.shape[0] + k
                    here = (named[i] == e) & (slots[i] == m)
                    weight = weight + jnp.where(here, weights_ref[k, t], 0.0)
                sums[t] = sums[t] + weight * cell
    for t in range(reqs):
        spread[t * cut : (t + 1) * cut, :] = sums[t]
    for j in range(cut):
        cols = slice(j * HD, (j + 1) * HD)
        moe = spread[pl.ds(j, reqs, stride=cut), :]
        out_ref[:, cols] = (hidden_ref[:, cols] + moe).astype(jnp.bfloat16)


def mixed_in(ids, weights, home, hidden):
    reqs, width = hidden.shape
    sm = pl.BlockSpec(memory_space=pltpu.SMEM)
    vm = pl.BlockSpec(memory_space=pltpu.VMEM)
    return pl.pallas_call(
        mix_kernel,
        out_shape=jax.ShapeDtypeStruct((reqs, width), jnp.bfloat16),
        in_specs=[sm, sm, vm, vm],
        out_specs=vm,
        scratch_shapes=[pltpu.VMEM((reqs * width // HD, HD), jnp.float32)],
        compiler_params=pltpu.CompilerParams(vmem_limit_bytes=8 * 1024 * 1024),
        name="mixed_in",
    )(ids, weights, home, hidden)


def layer(
    tokens,
    queries,
    token_kv,
    kv_cache,
    context_lengths,
    fresh_kv,
    block_counts,
    expert_ids,
    route_weights,
    norm_gain,
    w_gate,
    w_up,
    w_down,
):
    me = lax.axis_index(DEV)
    following = passed_along(fresh_kv, DEV, -1)
    rows_x = lax.axis_size("dev_0")
    me = lax.axis_index(DEV).astype(jnp.int32)[None]
    hidden_state, leaving = attended(
        me,
        context_lengths,
        expert_ids.T,
        block_counts[None],
        queries,
        token_kv,
        kv_cache,
        fresh_kv,
        following,
        tokens,
        norm_gain[None],
        rows_x,
    )
    own_block, *own_sides = unpacked(lax.all_to_all(leaving, "dev_0", 0, 0, tiled=True))
    other, came, theirs = gathered(*own_sides)
    far = lax.axis_size("dev_1") // 2
    each = rows_x * MOST
    last = far - 1
    near = range(far - 2, 0, -1)
    pieces = [own_block, other] + [group[step] for group in (theirs, came) for step in near]
    home_own, home_other, *near_kept, near_sent, gate, up, down = early_products(
        pieces, (w_gate, w_up, w_down), [each, each] + [2 * each] * len(near) + [2 * len(near) * each]
    )
    kept, got = {}, {}
    near_got = swapped(near_sent)
    for i, step in enumerate(near):
        for part in (0, 1):
            row = (1 - part) * each
            kept[step, part] = (near_kept[i], row)
            got[step, part] = (near_got, 2 * i * each + row)
    far_kept, last_kept, sent = late_products(
        [came[far], theirs[last], theirs[far], came[last]], (gate, up, down), [each, 2 * each, 3 * each]
    )
    kept[far, 1], kept[last, 1], kept[last, 0] = (far_kept, 0), (last_kept, 0), (last_kept, each)
    first = swapped(sent)
    got[far, 1], got[last, 1], got[last, 0] = (first, 0), (first, each), (first, 2 * each)
    last_terms = scattered(far, each, home_own, home_other, kept, got)
    home = lax.all_to_all(packed_sum(*last_terms, rows_x), "dev_0", 0, 0, tiled=True)
    return mixed_in(expert_ids.T, route_weights.T, home, hidden_state)


def solution(mesh):
    split = Mesh(
        mesh.devices.reshape(mesh.shape["groups"], 8, 8, 2), ("groups", "dev_0", "dev_1", "dev_2")
    )
    return jax.shard_map(
        layer,
        mesh=split,
        in_specs=(
            P(GROUPS_DEV, None),
            P(GROUPS_DEV, None),
            P(GROUPS_DEV, None),
            P(GROUPS_DEV, None, None),
            P(GROUPS_DEV),
            P(GROUPS_DEV, None),
            P("groups"),
            P(GROUPS_DEV, None),
            P(GROUPS_DEV, None),
            P(),
            P(None, DEV),
            P(None, DEV),
            P(DEV, None),
        ),
        out_specs=P(GROUPS_DEV, None),
        check_vma=False,
    )
```
